32 devices in a mesh: dp: 2 (over x), tp: 4 (over z), sp: 4 (over y, core).
Axes of the slice: x: 2, y: 2, z: 4, core: 2. Of those that a mesh axis runs over, the one named last changes fastest.
Arguments:
- k_cache: bfloat16 [4, 16, 4, 8192, 64], P(None, 'dp', 'tp', 'sp'), parts along dimension 1
- v_cache: bfloat16 [4, 16, 4, 8192, 64], P(None, 'dp', 'tp', 'sp'), parts along dimension 1
- lengths: int32 [16], P('dp'), parts along dimension 0
- hidden: bfloat16 [16, 2048], P(('dp', 'sp')), parts along dimension 0
- ln_gain: bfloat16 [4, 2048], replicated
- w_query: bfloat16 [4, 2048, 2048], P(None, None, 'tp')
- w_key: bfloat16 [4, 2048, 256], P(None, None, 'tp')
- w_value: bfloat16 [4, 2048, 256], P(None, None, 'tp')
- w_out: bfloat16 [4, 2048, 2048], P(None, 'tp')
- w_gate: bfloat16 [4, 2048, 5632], P(None, None, 'tp')
- w_up: bfloat16 [4, 2048, 5632], P(None, None, 'tp')
- w_down: bfloat16 [4, 5632, 2048], P(None, 'tp')
Outputs:
- output 1: bfloat16 [16, 2048], P(('dp', 'sp')), parts along dimension 0
- output 2: bfloat16 [3, 16, 4, 4096, 64], P(None, ('dp', 'sp'), 'tp'), parts along dimension 1
- output 3: bfloat16 [3, 16, 4, 4096, 64], P(None, ('dp', 'sp'), 'tp'), parts along dimension 1
- output 4: bfloat16 [16, 4, 8192, 64], P(('dp', 'sp'), 'tp'), parts along dimension 0
- output 5: bfloat16 [16, 4, 8192, 64], P(('dp', 'sp'), 'tp'), parts along dimension 0
There are 2 independent parts. The reference program is written for one: setup_inputs(seed, part) draws one part's arguments, and reference() takes and returns one part's arrays. A program takes and returns all parts, laid end to end along the dimension named above; an argument that names none is the same for every part.
All inputs are finite; a program needn't handle non-finite values.
Results may differ from the reference program's by a relative error of at most 0.02.
Values are sent between devices in bfloat16 or wider.
A program may use at most 1 GiB of HBM per device.

```python
import jax
import jax.numpy as jnp
from jax import lax

N_ROWS = 8
SEQ_LEN = 8192
MODEL_DIM = 2048
N_HEADS = 32
KV_HEADS = 4
HEAD_DIM = 64
FFN_DIM = 5632
WINDOW = 4096
ROPE_BASE = 50000
N_LAYERS = 4
NORM_EPS = 1e-5


def scaled_normal(key_in, shape, fan_in, spread=1.0):
    return (jax.random.normal(key_in, shape, jnp.float32) * (spread * fan_in ** -0.5)).astype(jnp.bfloat16)


def draw_lengths(len_key):
    key_lo, key_hi = jax.random.split(len_key)
    lengths = jax.random.randint(key_lo, (N_ROWS,), WINDOW + 1, SEQ_LEN, jnp.int32)
    order = jax.random.permutation(key_hi, N_ROWS)
    lengths = lengths.at[order[0]].set(SEQ_LEN - 1)
    return lengths.at[order[1]].set(WINDOW + 1)


def setup_inputs(seed: int = 0, part: int = 0) -> dict:
    base_key = jax.random.key(seed)
    part_key = jax.random.fold_in(base_key, part)
    part_keys = jax.random.split(part_key, 3)
    cache_shape = (N_LAYERS, N_ROWS, KV_HEADS, SEQ_LEN, HEAD_DIM)
    k_cache = (2.5 * jax.random.normal(part_keys[0], cache_shape, jnp.float32)).astype(jnp.bfloat16)
    v_cache = jax.random.normal(part_keys[1], cache_shape, jnp.float32).astype(jnp.bfloat16)
    hidden = jax.random.normal(part_keys[2], (N_ROWS, MODEL_DIM), jnp.float32).astype(jnp.bfloat16)
    lengths = draw_lengths(jax.random.fold_in(part_key, 3))
    shared = jax.random.split(jax.random.fold_in(base_key, 1000), 8)
    q_width = N_HEADS * HEAD_DIM
    kv_width = KV_HEADS * HEAD_DIM
    ln_gain = jax.random.uniform(shared[0], (N_LAYERS, MODEL_DIM), jnp.float32, 0.5, 1.5).astype(jnp.bfloat16)
    return {
        "k_cache": k_cache,
        "v_cache": v_cache,
        "lengths": lengths,
        "hidden": hidden,
        "ln_gain": ln_gain,
        "w_query": scaled_normal(shared[1], (N_LAYERS, MODEL_DIM, q_width), MODEL_DIM),
        "w_key": scaled_normal(shared[2], (N_LAYERS, MODEL_DIM, kv_width), MODEL_DIM, 8.0),
        "w_value": scaled_normal(shared[3], (N_LAYERS, MODEL_DIM, kv_width), MODEL_DIM, 2.0),
        "w_out": scaled_normal(shared[4], (N_LAYERS, q_width, MODEL_DIM), q_width),
        "w_gate": scaled_normal(shared[5], (N_LAYERS, MODEL_DIM, FFN_DIM), MODEL_DIM),
        "w_up": scaled_normal(shared[6], (N_LAYERS, MODEL_DIM, FFN_DIM), MODEL_DIM),
        "w_down": scaled_normal(shared[7], (N_LAYERS, FFN_DIM, MODEL_DIM), FFN_DIM),
    }


def layer_norm(rows_in, gain):
    rows32 = rows_in.astype(jnp.float32)
    centered = rows32 - rows32.mean(axis=-1, keepdims=True)
    variance = (centered * centered).mean(axis=-1, keepdims=True)
    scaled = centered * lax.rsqrt(variance + NORM_EPS)
    return (scaled * gain.astype(jnp.float32)).astype(jnp.bfloat16)


def rotary(proj, positions, n_groups):
    half_dim = HEAD_DIM // 2
    inv_freq = 1.0 / (ROPE_BASE ** (jnp.arange(half_dim, dtype=jnp.float32) * 2.0 / HEAD_DIM))
    angles = positions.astype(jnp.float32)[:, None] * inv_freq[None, :]
    cosine = jnp.cos(angles)[:, None, :]
    sine = jnp.sin(angles)[:, None, :]
    heads = proj.reshape(proj.shape[0], n_groups, HEAD_DIM)
    first = heads[..., :half_dim]
    second = heads[..., half_dim:]
    turned = jnp.concatenate([first * cosine - second * sine, second * cosine + first * sine], axis=-1)
    return turned.reshape(proj.shape)


def attend(query, keys, values, key_valid):
    group_size = N_HEADS // KV_HEADS

    def one_row(row):
        q_row, k_row, v_row, ok_row = row
        grouped = q_row.reshape(KV_HEADS, group_size, HEAD_DIM).astype(jnp.float32)
        scores = jnp.einsum("kgd,ksd->kgs", grouped, k_row.astype(jnp.float32)) * HEAD_DIM ** -0.5
        scores = jnp.where(ok_row[None, None, :], scores, -1e30)
        weights = jax.nn.softmax(scores, axis=-1).astype(jnp.bfloat16)
        mixed = jnp.einsum("kgs,ksd->kgd", weights.astype(jnp.float32), v_row.astype(jnp.float32))
        return mixed.astype(jnp.bfloat16).reshape(N_HEADS * HEAD_DIM)

    return lax.map(one_row, (query, keys, values, key_valid))


def reference(k_cache, v_cache, lengths, hidden, ln_gain, w_query, w_key, w_value, w_out, w_gate, w_up, w_down):
    slot_ids = jnp.arange(WINDOW, dtype=jnp.int32)
    slot_pos = lengths[:, None] - (lengths[:, None] - slot_ids[None, :]) % WINDOW
    seq_ids = jnp.arange(SEQ_LEN, dtype=jnp.int32)
    window_valid = jnp.ones((N_ROWS, WINDOW), dtype=jnp.bool_)
    global_valid = seq_ids[None, :] <= lengths[:, None]
    before_new = (seq_ids[None, :] < lengths[:, None])[:, None, :, None]
    at_new = (seq_ids[None, :] == lengths[:, None])[:, None, :, None]
    slot_new = (slot_pos == lengths[:, None])[:, None, :, None]
    slot_index = slot_pos[:, None, :, None]
    residual = hidden
    windows_k = []
    windows_v = []
    for layer in range(N_LAYERS):
        sliding = layer < N_LAYERS - 1
        normed = layer_norm(residual, ln_gain[layer])
        query = jnp.dot(normed, w_query[layer], preferred_element_type=jnp.float32)
        key_new = jnp.dot(normed, w_key[layer], preferred_element_type=jnp.float32)
        value_new = jnp.dot(normed, w_value[layer], preferred_element_type=jnp.float32)
        if sliding:
            query = rotary(query, lengths, N_HEADS)
            key_new = rotary(key_new, lengths, KV_HEADS)
        query = query.astype(jnp.bfloat16).reshape(N_ROWS, N_HEADS, HEAD_DIM)
        key_new = key_new.astype(jnp.bfloat16).reshape(N_ROWS, KV_HEADS, 1, HEAD_DIM)
        value_new = value_new.astype(jnp.bfloat16).reshape(N_ROWS, KV_HEADS, 1, HEAD_DIM)
        if sliding:
            keys = jnp.where(slot_new, key_new, jnp.take_along_axis(k_cache[layer], slot_index, axis=2))
            values = jnp.where(slot_new, value_new, jnp.take_along_axis(v_cache[layer], slot_index, axis=2))
            windows_k.append(keys)
            windows_v.append(values)
            key_valid = window_valid
        else:
            keys = jnp.where(at_new, key_new, jnp.where(before_new, k_cache[layer], 0))
            values = jnp.where(at_new, value_new, jnp.where(before_new, v_cache[layer], 0))
            key_valid = global_valid
        mixed = attend(query, keys, values, key_valid)
        attn_out = jnp.dot(mixed, w_out[layer], preferred_element_type=jnp.float32)
        gate_proj = jnp.dot(normed, w_gate[layer], preferred_element_type=jnp.float32)
        up_proj = jnp.dot(normed, w_up[layer], preferred_element_type=jnp.float32)
        activated = (jax.nn.silu(gate_proj) * up_proj).astype(jnp.bfloat16)
        mlp_out = jnp.dot(activated, w_down[layer], preferred_element_type=jnp.float32)
        residual = (residual.astype(jnp.float32) + attn_out + mlp_out).astype(jnp.bfloat16)
    return residual, jnp.stack(windows_k), jnp.stack(windows_v), keys, values
```

```python
import jax
import jax.numpy as jnp
from jax import lax
from jax.sharding import PartitionSpec as P

WINDOW = 4096
ROPE_BASE = 50000
NORM_EPS = 1e-5


def layer_norm(rows_in, gain):
    rows32 = rows_in.astype(jnp.float32)
    centered = rows32 - rows32.mean(axis=-1, keepdims=True)
    variance = (centered * centered).mean(axis=-1, keepdims=True)
    scaled = centered * lax.rsqrt(variance + NORM_EPS)
    return (scaled * gain.astype(jnp.float32)).astype(jnp.bfloat16)


def rotary(proj, positions, head_dim):
    half_dim = head_dim // 2
    inv_freq = 1.0 / (ROPE_BASE ** (jnp.arange(half_dim, dtype=jnp.float32) * 2.0 / head_dim))
    angles = positions.astype(jnp.float32)[:, None] * inv_freq[None, :]
    cosine = jnp.cos(angles)[:, None, :]
    sine = jnp.sin(angles)[:, None, :]
    heads = proj.reshape(proj.shape[0], -1, head_dim)
    first = heads[..., :half_dim]
    second = heads[..., half_dim:]
    turned = jnp.concatenate([first * cosine - second * sine, second * cosine + first * sine], axis=-1)
    return turned.reshape(proj.shape)


def project(normed, w_query_l, w_key_l, w_value_l, positions, head_dim, sliding):
    n_rows = normed.shape[0]
    query = jnp.dot(normed, w_query_l, preferred_element_type=jnp.float32)
    key_new = jnp.dot(normed, w_key_l, preferred_element_type=jnp.float32)
    value_new = jnp.dot(normed, w_value_l, preferred_element_type=jnp.float32)
    if sliding:
        query = rotary(query, positions, head_dim)
        key_new = rotary(key_new, positions, head_dim)
    query = query.astype(jnp.bfloat16).reshape(n_rows, -1, head_dim)
    return query, key_new.astype(jnp.bfloat16), value_new.astype(jnp.bfloat16)


def mlp_part(normed, w_gate_l, w_up_l, w_down_l):
    gate_proj = jnp.dot(normed, w_gate_l, preferred_element_type=jnp.float32)
    up_proj = jnp.dot(normed, w_up_l, preferred_element_type=jnp.float32)
    activated = (jax.nn.silu(gate_proj) * up_proj).astype(jnp.bfloat16)
    return jnp.dot(activated, w_down_l, preferred_element_type=jnp.float32)


def attend_t(query, keys_t, values_t, key_valid):
    head_dim = query.shape[-1]
    scores = jnp.einsum("bgd,bds->bgs", query, keys_t, preferred_element_type=jnp.float32) * head_dim ** -0.5
    if key_valid is not None:
        scores = jnp.where(key_valid[:, None, :], scores, -1e30)
    weights = jax.nn.softmax(scores, axis=-1).astype(jnp.bfloat16)
    mixed = jnp.einsum("bgs,bds->bgd", weights, values_t, preferred_element_type=jnp.float32)
    return mixed.astype(jnp.bfloat16).reshape(query.shape[0], -1)


def solution(mesh):
    cache_spec = P(None, "dp", "tp", "sp", None)
    row_spec = P(("dp", "sp"), None)
    col_spec = P(None, None, "tp")
    inner_spec = P(None, "tp", None)
    window_spec = P(None, ("dp", "sp"), "tp", None, None)
    global_spec = P(("dp", "sp"), "tp", None, None)
    in_specs = (cache_spec, cache_spec, P("dp"), row_spec, P(None, None), col_spec, col_spec, col_spec, inner_spec, col_spec, col_spec, inner_spec)
    out_specs = (row_spec, window_spec, window_spec, global_spec, global_spec)
    n_dev = mesh.shape["sp"]

    def device_step(k_cache, v_cache, lengths, hidden, ln_gain, w_query, w_key, w_value, w_out, w_gate, w_up, w_down):
        n_layers = w_query.shape[0]
        rows_dev = hidden.shape[0]
        head_dim = k_cache.shape[-1]
        me = lax.axis_index("sp")
        my_lengths = lax.dynamic_slice_in_dim(lengths, me * rows_dev, rows_dev)
        my_off = my_lengths - WINDOW
        core = me % 2
        upper = me >= 2
        k_t = k_cache[:, :, 0].swapaxes(-1, -2)
        v_t = v_cache[:, :, 0].swapaxes(-1, -2)
        half_len = k_t.shape[-1]

        def rows_of(layer, owner):
            k_rows = lax.dynamic_slice_in_dim(k_t[layer], owner * rows_dev, rows_dev)
            v_rows = lax.dynamic_slice_in_dim(v_t[layer], owner * rows_dev, rows_dev)
            return jnp.stack([k_rows, v_rows])

        moved = []
        for layer in range(n_layers):
            got = [rows_of(layer, me)]
            for flip in (1, 2, 3):
                pairs = [(i, i ^ flip) for i in range(n_dev)]
                got.append(lax.ppermute(rows_of(layer, me ^ flip), "sp", pairs))
            moved.append(got)
        residual = hidden
        windows_k = []
        windows_v = []
        for layer in range(n_layers):
            sliding = layer < n_layers - 1
            normed = layer_norm(residual, ln_gain[layer])
            query, key_new, value_new = project(normed, w_query[layer], w_key[layer], w_value[layer], my_lengths, head_dim, sliding)
            mlp_out = mlp_part(normed, w_gate[layer], w_up[layer], w_down[layer])
            own, partner, across, diagonal = moved[layer]
            if sliding:
                slot = jnp.arange(WINDOW, dtype=jnp.int32).reshape(2, half_len)
                edge = my_off[None, :, None, None]

                def half_of(near, far, half):
                    ids = slot[half][None, None, None, :]
                    from_upper = jnp.where(upper, near, far)
                    from_lower = jnp.where(upper, far, near)
                    return jnp.where(ids < edge, from_upper, from_lower)

                mine = half_of(own, across, core)
                other = half_of(partner, diagonal, 1 - core)
                both = jnp.concatenate([jnp.where(core == 0, mine, other), jnp.where(core == 0, other, mine)], axis=-1)
                is_new = jnp.arange(WINDOW, dtype=jnp.int32)[None, None, :] == my_off[:, None, None]
                keys = jnp.where(is_new, key_new[:, :, None], both[0])
                values = jnp.where(is_new, value_new[:, :, None], both[1])
                key_valid = None
            else:
                near = jnp.concatenate([jnp.where(core == 0, own, partner), jnp.where(core == 0, partner, own)], axis=-1)
                far = jnp.concatenate([jnp.where(core == 0, across, diagonal), jnp.where(core == 0, diagonal, across)], axis=-1)
                both = jnp.concatenate([jnp.where(upper, far, near), jnp.where(upper, near, far)], axis=-1)
                slot = jnp.arange(2 * WINDOW, dtype=jnp.int32)[None, None, :]
                edge = my_lengths[:, None, None]
                keys = jnp.where(slot == edge, key_new[:, :, None], jnp.where(slot < edge, both[0], 0))
                values = jnp.where(slot == edge, value_new[:, :, None], jnp.where(slot < edge, both[1], 0))
                key_valid = jnp.arange(2 * WINDOW, dtype=jnp.int32)[None, :] <= my_lengths[:, None]
            if sliding:
                windows_k.append(keys)
                windows_v.append(values)
            mixed = attend_t(query, keys, values, key_valid)
            attn_out = jnp.dot(mixed, w_out[layer], preferred_element_type=jnp.float32)
            total = lax.psum(attn_out + mlp_out, "tp")
            residual = (residual.astype(jnp.float32) + total).astype(jnp.bfloat16)

        def back(rows_t):
            return rows_t.swapaxes(-1, -2)

        win_k = back(jnp.stack(windows_k))[:, :, None]
        win_v = back(jnp.stack(windows_v))[:, :, None]
        return residual, win_k, win_v, back(keys)[:, None], back(values)[:, None]

    return jax.shard_map(device_step, mesh=mesh, in_specs=in_specs, out_specs=out_specs, check_vma=False)
```

```python
import functools

import jax
import jax.numpy as jnp
from jax import lax
from jax.experimental import pallas as pl
from jax.experimental.pallas import tpu as pltpu
from jax.sharding import PartitionSpec as P

WINDOW = 4096
ROPE_BASE = 50000
NORM_EPS = 1e-5


PAD = 16
K_STEPS = 4
N_STEPS = 4
MESH_ID = pl.DeviceIdType.MESH


def project_kernel(sliding, h_ref, gain_ref, cq_ref, sq_ref, ck_ref, sk_ref, wq_ref, wk_ref, wv_ref, wg_ref, wu_ref, wd_ref,
                   q_out, k_out, v_out, mlp_out, u_ref, q_acc, k_acc, v_acc, g_acc, up_acc, act_ref):
    step = pl.program_id(0)
    n_rows = h_ref.shape[0]
    width = wq_ref.shape[1]
    dim = wk_ref.shape[1]
    heads = wq_ref.shape[2] // dim

    @pl.when(step == 0)
    def _():
        rows32 = h_ref[...]
        centered = rows32 - jnp.mean(rows32, axis=-1, keepdims=True)
        variance = jnp.mean(centered * centered, axis=-1, keepdims=True)
        scaled = centered * lax.rsqrt(variance + NORM_EPS)
        normed = scaled * gain_ref[...].astype(jnp.float32)
        padded = jnp.concatenate([normed, jnp.zeros((PAD - n_rows, normed.shape[1]), jnp.float32)], axis=0).astype(jnp.bfloat16)
        for part in range(K_STEPS):
            u_ref[part] = padded[:, part * width:(part + 1) * width]
        q_acc[...] = jnp.zeros_like(q_acc)
        k_acc[...] = jnp.zeros_like(k_acc)
        v_acc[...] = jnp.zeros_like(v_acc)
        g_acc[...] = jnp.zeros_like(g_acc)
        up_acc[...] = jnp.zeros_like(up_acc)

    @pl.when(step < K_STEPS)
    def _():
        part = u_ref[jnp.minimum(step, K_STEPS - 1)]
        nt = (((1,), (1,)), ((), ()))
        q_acc[...] += jnp.dot(part, wq_ref[0], preferred_element_type=jnp.float32)
        k_acc[...] += lax.dot_general(wk_ref[0], part, nt, preferred_element_type=jnp.float32)
        v_acc[...] += lax.dot_general(wv_ref[0], part, nt, preferred_element_type=jnp.float32)
        g_acc[...] += jnp.dot(part, wg_ref[0], preferred_element_type=jnp.float32)
        up_acc[...] += jnp.dot(part, wu_ref[0], preferred_element_type=jnp.float32)

    @pl.when(step == K_STEPS - 1)
    def _():
        gate = g_acc[...]
        act_ref[...] = (gate * jax.nn.sigmoid(gate) * up_acc[...]).astype(jnp.bfloat16)
        query = q_acc[:8]
        k_t = k_acc[...]
        if sliding:
            lane = lax.broadcasted_iota(jnp.int32, query.shape, 1)
            wide = query.shape[1]
            swapped = jnp.where(lane % dim < dim // 2, pltpu.roll(query, wide - dim // 2, 1), pltpu.roll(query, dim // 2, 1))
            query = query * cq_ref[...] + swapped * sq_ref[...]
            first = k_t[:dim // 2]
            second = k_t[dim // 2:]
            cosine = ck_ref[...]
            sine = sk_ref[...]
            k_t = jnp.concatenate([first * cosine - second * sine, second * cosine + first * sine], axis=0)
        k_out[...] = k_t.astype(jnp.bfloat16)
        v_out[...] = v_acc[...].astype(jnp.bfloat16)
        spread = [jnp.broadcast_to(query[r:r + 1], (heads, query.shape[1])) for r in range(n_rows)]
        spread = jnp.concatenate(spread, axis=0)
        row = lax.broadcasted_iota(jnp.int32, spread.shape, 0)
        lane = lax.broadcasted_iota(jnp.int32, spread.shape, 1)
        masked = jnp.where(lane // dim == row % heads, spread, 0.0).astype(jnp.bfloat16)
        pick_row = lax.broadcasted_iota(jnp.int32, (query.shape[1], dim), 0)
        pick_col = lax.broadcasted_iota(jnp.int32, (query.shape[1], dim), 1)
        pick = jnp.where(pick_row % dim == pick_col, 1.0, 0.0).astype(jnp.bfloat16)
        q_out[...] = jnp.dot(masked, pick, preferred_element_type=jnp.float32).astype(jnp.bfloat16)

    @pl.when(step >= K_STEPS)
    def _():
        part = jnp.dot(act_ref[...], wd_ref[0], preferred_element_type=jnp.float32)
        mlp_out[...] = part[:mlp_out.shape[0]]


def project_call(layer, sliding, h, gain, tables, w_query, wk_t, wv_t, w_gate, w_up, w_down):
    n_rows, model = h.shape
    q_width = w_query.shape[2]
    dim = wk_t.shape[1]
    hidden = w_gate.shape[2]
    k_len = model // K_STEPS
    n_len = model // N_STEPS
    last_k = K_STEPS - 1
    whole = lambda shape: pl.BlockSpec(shape, lambda i: (0,) * len(shape))
    by_k = lambda shape: pl.BlockSpec(shape, lambda i: (layer, jnp.minimum(i, last_k), 0))
    by_kt = pl.BlockSpec((1, dim, k_len), lambda i: (layer, 0, jnp.minimum(i, last_k)))
    heads = q_width // dim
    out_shape = (
        jax.ShapeDtypeStruct((n_rows * heads, dim), jnp.bfloat16),
        jax.ShapeDtypeStruct((dim, PAD), jnp.bfloat16),
        jax.ShapeDtypeStruct((dim, PAD), jnp.bfloat16),
        jax.ShapeDtypeStruct((n_rows, model), jnp.float32),
    )
    weight_bytes = 2 * (model * q_width + 2 * dim * model + 3 * model * hidden)
    return pl.pallas_call(
        functools.partial(project_kernel, sliding),
        grid=(K_STEPS + N_STEPS,),
        in_specs=[
            whole((n_rows, model)), pl.BlockSpec((1, model), lambda i: (0, 0)),
            whole(tables[0].shape), whole(tables[1].shape), whole(tables[2].shape), whole(tables[3].shape),
            by_k((1, k_len, q_width)), by_kt, by_kt, by_k((1, k_len, hidden)), by_k((1, k_len, hidden)),
            pl.BlockSpec((1, hidden, n_len), lambda i: (layer, 0, jnp.maximum(i - K_STEPS, 0))),
        ],
        out_specs=(
            whole((n_rows * heads, dim)), whole((dim, PAD)), whole((dim, PAD)),
            pl.BlockSpec((n_rows, n_len), lambda i: (0, jnp.maximum(i - K_STEPS, 0))),
        ),
        out_shape=out_shape,
        scratch_shapes=[
            pltpu.VMEM((K_STEPS, PAD, k_len), jnp.bfloat16),
            pltpu.VMEM((PAD, q_width), jnp.float32),
            pltpu.VMEM((dim, PAD), jnp.float32),
            pltpu.VMEM((dim, PAD), jnp.float32),
            pltpu.VMEM((PAD, hidden), jnp.float32),
            pltpu.VMEM((PAD, hidden), jnp.float32),
            pltpu.VMEM((PAD, hidden), jnp.bfloat16),
        ],
        compiler_params=pltpu.CompilerParams(dimension_semantics=("arbitrary",), vmem_limit_bytes=40 * 2 ** 20),
        cost_estimate=pl.CostEstimate(flops=PAD * weight_bytes, bytes_accessed=weight_bytes, transcendentals=0),
        name="project_%d" % layer,
    )(h, gain, *tables, w_query, wk_t, wv_t, w_gate, w_up, w_down)


def rotary_tables(positions, dim, heads):
    half = dim // 2
    inv_freq = 1.0 / (ROPE_BASE ** (jnp.arange(half, dtype=jnp.float32) * 2.0 / dim))
    angles = positions.astype(jnp.float32)[:, None] * inv_freq[None, :]
    cosine = jnp.cos(angles)
    sine = jnp.sin(angles)
    n_rows = positions.shape[0]
    cq = jnp.pad(jnp.tile(jnp.concatenate([cosine, cosine], axis=1), (1, heads)), ((0, 8 - n_rows), (0, 0)))
    sq = jnp.pad(jnp.tile(jnp.concatenate([-sine, sine], axis=1), (1, heads)), ((0, 8 - n_rows), (0, 0)))
    ck = jnp.pad(cosine.T, ((0, 0), (0, PAD - n_rows)))
    sk = jnp.pad(sine.T, ((0, 0), (0, PAD - n_rows)))
    return cq, sq, ck, sk


def sum_kernel(n_tp, part_ref, resid_ref, out_ref, slots, send_sem, recv_sem):
    me = lax.axis_index("tp")
    barrier = pltpu.get_barrier_semaphore()
    for flip in range(1, n_tp):
        pl.semaphore_signal(barrier, inc=1, device_id={"tp": me ^ flip}, device_id_type=MESH_ID)
    pl.semaphore_wait(barrier, n_tp - 1)
    copies = []
    for flip in range(1, n_tp):
        copy = pltpu.make_async_remote_copy(
            src_ref=part_ref, dst_ref=slots.at[me], send_sem=send_sem.at[flip - 1], recv_sem=recv_sem.at[flip - 1],
            device_id={"tp": me ^ flip}, device_id_type=MESH_ID)
        copy.start()
        copies.append(copy)
    slots[me] = part_ref[...]
    for copy in copies:
        copy.wait()
    total = slots[0]
    for index in range(1, n_tp):
        total = total + slots[index]
    out_ref[...] = (resid_ref[...] + total).astype(jnp.bfloat16).astype(jnp.float32)


def sum_call(part, resid, n_tp):
    return pl.pallas_call(
        functools.partial(sum_kernel, n_tp),
        out_shape=jax.ShapeDtypeStruct(part.shape, jnp.float32),
        in_specs=[pl.BlockSpec(memory_space=pltpu.VMEM)] * 2,
        out_specs=pl.BlockSpec(memory_space=pltpu.VMEM),
        scratch_shapes=[
            pltpu.VMEM((n_tp,) + part.shape, jnp.float32),
            pltpu.SemaphoreType.DMA((n_tp - 1,)),
            pltpu.SemaphoreType.DMA((n_tp - 1,)),
        ],
        compiler_params=pltpu.CompilerParams(collective_id=0, has_side_effects=True),
        name="sum_tp",
    )(part, resid)


def attend_t(query, keys_t, values_t, key_valid):
    head_dim = query.shape[-1]
    scores = jnp.einsum("bgd,bds->bgs", query, keys_t, preferred_element_type=jnp.float32) * head_dim ** -0.5
    if key_valid is not None:
        scores = jnp.where(key_valid[:, None, :], scores, -1e30)
    weights = jax.nn.softmax(scores, axis=-1).astype(jnp.bfloat16)
    mixed = jnp.einsum("bgs,bds->bgd", weights, values_t, preferred_element_type=jnp.float32)
    return mixed.astype(jnp.bfloat16).reshape(query.shape[0], -1)


def solution(mesh):
    cache_spec = P(None, "dp", "tp", "sp", None)
    row_spec = P(("dp", "sp"), None)
    col_spec = P(None, None, "tp")
    inner_spec = P(None, "tp", None)
    window_spec = P(None, ("dp", "sp"), "tp", None, None)
    global_spec = P(("dp", "sp"), "tp", None, None)
    in_specs = (cache_spec, cache_spec, P("dp"), row_spec, P(None, None), col_spec, col_spec, col_spec, inner_spec, col_spec, col_spec, inner_spec)
    out_specs = (row_spec, window_spec, window_spec, global_spec, global_spec)
    n_dev = mesh.shape["sp"]

    def device_step(k_cache, v_cache, lengths, hidden, ln_gain, w_query, w_key, w_value, w_out, w_gate, w_up, w_down):
        n_layers = w_query.shape[0]
        rows_dev = hidden.shape[0]
        head_dim = k_cache.shape[-1]
        me = lax.axis_index("sp")
        my_lengths = lax.dynamic_slice_in_dim(lengths, me * rows_dev, rows_dev)
        my_off = my_lengths - WINDOW
        core = me % 2
        upper = me >= 2
        k_rows_t = k_cache[:, :, 0].swapaxes(-1, -2)
        v_t = v_cache[:, :, 0].swapaxes(-1, -2)
        half_len = k_rows_t.shape[-1]

        def rows_of(layer, owner):
            k_rows = lax.dynamic_slice_in_dim(k_rows_t[layer], owner * rows_dev, rows_dev)
            v_rows = lax.dynamic_slice_in_dim(v_t[layer], owner * rows_dev, rows_dev)
            return jnp.stack([k_rows, v_rows])

        moved = []
        for layer in range(n_layers):
            got = [rows_of(layer, me)]
            for flip in (1, 2, 3):
                pairs = [(i, i ^ flip) for i in range(n_dev)]
                got.append(lax.ppermute(rows_of(layer, me ^ flip), "sp", pairs))
            moved.append(got)
        residual = hidden.astype(jnp.float32)
        tables = rotary_tables(my_lengths, head_dim, w_query.shape[2] // head_dim)
        wk_t = w_key.swapaxes(1, 2)
        wv_t = w_value.swapaxes(1, 2)
        windows_k = []
        windows_v = []
        for layer in range(n_layers):
            sliding = layer < n_layers - 1
            query, k_t, v_t_new, mlp_out = project_call(layer, sliding, residual, ln_gain[layer:layer + 1], tables, w_query, wk_t, wv_t, w_gate, w_up, w_down)
            query = query.reshape(rows_dev, -1, head_dim)
            key_new = k_t[:, :rows_dev].T
            value_new = v_t_new[:, :rows_dev].T
            own, partner, across, diagonal = moved[layer]
            if sliding:
                slot = jnp.arange(WINDOW, dtype=jnp.int32).reshape(2, half_len)
                edge = my_off[None, :, None, None]

                def half_of(near, far, half):
                    ids = slot[half][None, None, None, :]
                    from_upper = jnp.where(upper, near, far)
                    from_lower = jnp.where(upper, far, near)
                    return jnp.where(ids < edge, from_upper, from_lower)

                mine = half_of(own, across, core)
                other = half_of(partner, diagonal, 1 - core)
                both = jnp.concatenate([jnp.where(core == 0, mine, other), jnp.where(core == 0, other, mine)], axis=-1)
                is_new = jnp.arange(WINDOW, dtype=jnp.int32)[None, None, :] == my_off[:, None, None]
                keys = jnp.where(is_new, key_new[:, :, None], both[0])
                values = jnp.where(is_new, value_new[:, :, None], both[1])
                key_valid = None
            else:
                near = jnp.concatenate([jnp.where(core == 0, own, partner), jnp.where(core == 0, partner, own)], axis=-1)
                far = jnp.concatenate([jnp.where(core == 0, across, diagonal), jnp.where(core == 0, diagonal, across)], axis=-1)
                both = jnp.concatenate([jnp.where(upper, far, near), jnp.where(upper, near, far)], axis=-1)
                slot = jnp.arange(2 * WINDOW, dtype=jnp.int32)[None, None, :]
                edge = my_lengths[:, None, None]
                keys = jnp.where(slot == edge, key_new[:, :, None], jnp.where(slot < edge, both[0], 0))
                values = jnp.where(slot == edge, value_new[:, :, None], jnp.where(slot < edge, both[1], 0))
                key_valid = jnp.arange(2 * WINDOW, dtype=jnp.int32)[None, :] <= my_lengths[:, None]
            if sliding:
                windows_k.append(keys)
                windows_v.append(values)
            mixed = attend_t(query, keys, values, key_valid)
            attn_out = jnp.dot(mixed, w_out[layer], preferred_element_type=jnp.float32)
            residual = sum_call(attn_out + mlp_out, residual, mesh.shape["tp"])

        def back(rows_t):
            return rows_t.swapaxes(-1, -2)

        win_k = back(jnp.stack(windows_k))[:, :, None]
        win_v = back(jnp.stack(windows_v))[:, :, None]
        return residual.astype(jnp.bfloat16), win_k, win_v, back(keys)[:, None], back(values)[:, None]

    return jax.shard_map(device_step, mesh=mesh, in_specs=in_specs, out_specs=out_specs, check_vma=False)
```

```python
import functools

import jax
import jax.numpy as jnp
from jax import lax
from jax.experimental import pallas as pl
from jax.experimental.pallas import tpu as pltpu
from jax.sharding import PartitionSpec as P

WINDOW = 4096
ROPE_BASE = 50000
NORM_EPS = 1e-5


PAD = 16
K_STEPS = 4
N_STEPS = 4
MESH_ID = pl.DeviceIdType.MESH


def project_kernel(sliding, h_ref, gain_ref, cq_ref, sq_ref, ck_ref, sk_ref, wq_ref, wk_ref, wv_ref, wg_ref, wu_ref, wd_ref,
                   q_out, k_out, v_out, mlp_out, u_ref, q_acc, k_acc, v_acc, g_acc, up_acc, act_ref):
    step = pl.program_id(0)
    n_rows = h_ref.shape[0]
    width = wq_ref.shape[1]
    dim = wk_ref.shape[1]
    heads = wq_ref.shape[2] // dim

    @pl.when(step == 0)
    def _():
        rows32 = h_ref[...]
        centered = rows32 - jnp.mean(rows32, axis=-1, keepdims=True)
        variance = jnp.mean(centered * centered, axis=-1, keepdims=True)
        scaled = centered * lax.rsqrt(variance + NORM_EPS)
        normed = scaled * gain_ref[...].astype(jnp.float32)
        padded = jnp.concatenate([normed, jnp.zeros((PAD - n_rows, normed.shape[1]), jnp.float32)], axis=0).astype(jnp.bfloat16)
        for part in range(K_STEPS):
            u_ref[part] = padded[:, part * width:(part + 1) * width]
        q_acc[...] = jnp.zeros_like(q_acc)
        k_acc[...] = jnp.zeros_like(k_acc)
        v_acc[...] = jnp.zeros_like(v_acc)
        g_acc[...] = jnp.zeros_like(g_acc)
        up_acc[...] = jnp.zeros_like(up_acc)

    @pl.when(step < K_STEPS)
    def _():
        part = u_ref[jnp.minimum(step, K_STEPS - 1)]
        nt = (((1,), (1,)), ((), ()))
        q_acc[...] += jnp.dot(part, wq_ref[0], preferred_element_type=jnp.float32)
        k_acc[...] += lax.dot_general(wk_ref[0], part, nt, preferred_element_type=jnp.float32)
        v_acc[...] += lax.dot_general(wv_ref[0], part, nt, preferred_element_type=jnp.float32)
        g_acc[...] += jnp.dot(part, wg_ref[0], preferred_element_type=jnp.float32)
        up_acc[...] += jnp.dot(part, wu_ref[0], preferred_element_type=jnp.float32)

    @pl.when(step == K_STEPS - 1)
    def _():
        gate = g_acc[...]
        act_ref[...] = (gate * jax.nn.sigmoid(gate) * up_acc[...]).astype(jnp.bfloat16)
        query = q_acc[:8]
        k_t = k_acc[...]
        if sliding:
            lane = lax.broadcasted_iota(jnp.int32, query.shape, 1)
            wide = query.shape[1]
            swapped = jnp.where(lane % dim < dim // 2, pltpu.roll(query, wide - dim // 2, 1), pltpu.roll(query, dim // 2, 1))
            query = query * cq_ref[...] + swapped * sq_ref[...]
            first = k_t[:dim // 2]
            second = k_t[dim // 2:]
            cosine = ck_ref[...]
            sine = sk_ref[...]
            k_t = jnp.concatenate([first * cosine - second * sine, second * cosine + first * sine], axis=0)
        k_out[...] = k_t.astype(jnp.bfloat16)
        v_out[...] = v_acc[...].astype(jnp.bfloat16)
        spread = [jnp.broadcast_to(query[r:r + 1], (heads, query.shape[1])) for r in range(n_rows)]
        spread = jnp.concatenate(spread, axis=0)
        row = lax.broadcasted_iota(jnp.int32, spread.shape, 0)
        lane = lax.broadcasted_iota(jnp.int32, spread.shape, 1)
        masked = jnp.where(lane // dim == row % heads, spread, 0.0).astype(jnp.bfloat16)
        pick_row = lax.broadcasted_iota(jnp.int32, (query.shape[1], dim), 0)
        pick_col = lax.broadcasted_iota(jnp.int32, (query.shape[1], dim), 1)
        pick = jnp.where(pick_row % dim == pick_col, 1.0, 0.0).astype(jnp.bfloat16)
        q_out[...] = jnp.dot(masked, pick, preferred_element_type=jnp.float32).astype(jnp.bfloat16)

    @pl.when(step >= K_STEPS)
    def _():
        part = jnp.dot(act_ref[...], wd_ref[0], preferred_element_type=jnp.float32)
        mlp_out[...] = part[:mlp_out.shape[0]]


def project_call(layer, sliding, h, gain, tables, w_query, wk_t, wv_t, w_gate, w_up, w_down):
    n_rows, model = h.shape
    q_width = w_query.shape[2]
    dim = wk_t.shape[1]
    hidden = w_gate.shape[2]
    k_len = model // K_STEPS
    n_len = model // N_STEPS
    last_k = K_STEPS - 1
    whole = lambda shape: pl.BlockSpec(shape, lambda i: (0,) * len(shape))
    by_k = lambda shape: pl.BlockSpec(shape, lambda i: (layer, jnp.minimum(i, last_k), 0))
    by_kt = pl.BlockSpec((1, dim, k_len), lambda i: (layer, 0, jnp.minimum(i, last_k)))
    heads = q_width // dim
    out_shape = (
        jax.ShapeDtypeStruct((n_rows * heads, dim), jnp.bfloat16),
        jax.ShapeDtypeStruct((dim, PAD), jnp.bfloat16),
        jax.ShapeDtypeStruct((dim, PAD), jnp.bfloat16),
        jax.ShapeDtypeStruct((n_rows, model), jnp.float32),
    )
    weight_bytes = 2 * (model * q_width + 2 * dim * model + 3 * model * hidden)
    return pl.pallas_call(
        functools.partial(project_kernel, sliding),
        grid=(K_STEPS + N_STEPS,),
        in_specs=[
            whole((n_rows, model)), pl.BlockSpec((1, model), lambda i: (0, 0)),
            whole(tables[0].shape), whole(tables[1].shape), whole(tables[2].shape), whole(tables[3].shape),
            by_k((1, k_len, q_width)), by_kt, by_kt, by_k((1, k_len, hidden)), by_k((1, k_len, hidden)),
            pl.BlockSpec((1, hidden, n_len), lambda i: (layer, 0, jnp.maximum(i - K_STEPS, 0))),
        ],
        out_specs=(
            whole((n_rows * heads, dim)), whole((dim, PAD)), whole((dim, PAD)),
            pl.BlockSpec((n_rows, n_len), lambda i: (0, jnp.maximum(i - K_STEPS, 0))),
        ),
        out_shape=out_shape,
        scratch_shapes=[
            pltpu.VMEM((K_STEPS, PAD, k_len), jnp.bfloat16),
            pltpu.VMEM((PAD, q_width), jnp.float32),
            pltpu.VMEM((dim, PAD), jnp.float32),
            pltpu.VMEM((dim, PAD), jnp.float32),
            pltpu.VMEM((PAD, hidden), jnp.float32),
            pltpu.VMEM((PAD, hidden), jnp.float32),
            pltpu.VMEM((PAD, hidden), jnp.bfloat16),
        ],
        compiler_params=pltpu.CompilerParams(dimension_semantics=("arbitrary",), vmem_limit_bytes=40 * 2 ** 20),
        cost_estimate=pl.CostEstimate(flops=PAD * weight_bytes, bytes_accessed=weight_bytes, transcendentals=0),
        name="project_%d" % layer,
    )(h, gain, *tables, w_query, wk_t, wv_t, w_gate, w_up, w_down)


def rotary_tables(positions, dim, heads):
    half = dim // 2
    inv_freq = 1.0 / (ROPE_BASE ** (jnp.arange(half, dtype=jnp.float32) * 2.0 / dim))
    angles = positions.astype(jnp.float32)[:, None] * inv_freq[None, :]
    cosine = jnp.cos(angles)
    sine = jnp.sin(angles)
    n_rows = positions.shape[0]
    cq = jnp.pad(jnp.tile(jnp.concatenate([cosine, cosine], axis=1), (1, heads)), ((0, 8 - n_rows), (0, 0)))
    sq = jnp.pad(jnp.tile(jnp.concatenate([-sine, sine], axis=1), (1, heads)), ((0, 8 - n_rows), (0, 0)))
    ck = jnp.pad(cosine.T, ((0, 0), (0, PAD - n_rows)))
    sk = jnp.pad(sine.T, ((0, 0), (0, PAD - n_rows)))
    return cq, sq, ck, sk


def sum_kernel(n_tp, part_ref, resid_ref, out_ref, slots, send_sem, recv_sem):
    me = lax.axis_index("tp")
    barrier = pltpu.get_barrier_semaphore()
    for flip in range(1, n_tp):
        pl.semaphore_signal(barrier, inc=1, device_id={"tp": me ^ flip}, device_id_type=MESH_ID)
    pl.semaphore_wait(barrier, n_tp - 1)
    copies = []
    for flip in range(1, n_tp):
        copy = pltpu.make_async_remote_copy(
            src_ref=part_ref, dst_ref=slots.at[me], send_sem=send_sem.at[flip - 1], recv_sem=recv_sem.at[flip - 1],
            device_id={"tp": me ^ flip}, device_id_type=MESH_ID)
        copy.start()
        copies.append(copy)
    slots[me] = part_ref[...]
    for copy in copies:
        copy.wait()
    total = slots[0]
    for index in range(1, n_tp):
        total = total + slots[index]
    out_ref[...] = (resid_ref[...] + total).astype(jnp.bfloat16).astype(jnp.float32)


def sum_call(part, resid, n_tp):
    return pl.pallas_call(
        functools.partial(sum_kernel, n_tp),
        out_shape=jax.ShapeDtypeStruct(part.shape, jnp.float32),
        in_specs=[pl.BlockSpec(memory_space=pltpu.VMEM)] * 2,
        out_specs=pl.BlockSpec(memory_space=pltpu.VMEM),
        scratch_shapes=[
            pltpu.VMEM((n_tp,) + part.shape, jnp.float32),
            pltpu.SemaphoreType.DMA((n_tp - 1,)),
            pltpu.SemaphoreType.DMA((n_tp - 1,)),
        ],
        compiler_params=pltpu.CompilerParams(collective_id=0, has_side_effects=True),
        name="sum_tp",
    )(part, resid)


LANES = 128
HALF_UNITS = 16
CHIP_ROWS = 4
MAX_UNITS = CHIP_ROWS * HALF_UNITS
HEAVY_LEVELS = (32, 40, 44, 48, 52, 56, 60, 64)
LIGHT_LEVELS = (8, 16, 20, 24, 28, 32, 36, 40, 44, 48, 56, 64)


def unit_table(offsets):
    half = jnp.arange(2, dtype=jnp.int32)[None, :] * HALF_UNITS
    edge = offsets[:, None]
    upper_end = jnp.clip((edge + LANES - 1) // LANES, half, half + HALF_UNITS)
    lower_start = jnp.clip((edge + 1) // LANES, half, half + HALF_UNITS)
    from_upper = jnp.arange(offsets.shape[0], dtype=jnp.int32)[:, None] < CHIP_ROWS
    start = jnp.where(from_upper, half, lower_start)
    count = jnp.where(from_upper, upper_end - half, half + HALF_UNITS - lower_start)
    by_chip = count.reshape(2, CHIP_ROWS, 2)
    ends = jnp.cumsum(by_chip, axis=1)
    base = (ends - by_chip).reshape(count.shape)
    return start, count, base, ends[:, -1]


def pack_kernel(info_ref, k_ref, v_ref, out_ref):
    for row in range(CHIP_ROWS):
        first = info_ref[1 + 3 * row]
        count = info_ref[2 + 3 * row]
        base = info_ref[3 + 3 * row]
        for unit in range(HALF_UNITS):
            @pl.when(jnp.logical_and(unit >= first, unit < first + count))
            def _():
                place = base + unit - first
                cols = pl.ds(unit * LANES, LANES)
                out_ref[0, 0, place] = k_ref[0, row, :, cols]
                out_ref[0, 1, place] = v_ref[0, row, :, cols]


def pack_call(info, k_t, v_t, n_layers):
    dim, half_len = k_t.shape[2:]
    block = pl.BlockSpec((1, CHIP_ROWS, dim, half_len), lambda l, info: (l, info[0], 0, 0))
    return pl.pallas_call(
        pack_kernel,
        grid_spec=pltpu.PrefetchScalarGridSpec(
            num_scalar_prefetch=1, grid=(n_layers,), in_specs=[block, block],
            out_specs=pl.BlockSpec((1, 2, MAX_UNITS, dim, LANES), lambda l, info: (l, 0, 0, 0, 0))),
        out_shape=jax.ShapeDtypeStruct((n_layers, 2, MAX_UNITS, dim, LANES), k_t.dtype),
        compiler_params=pltpu.CompilerParams(dimension_semantics=("arbitrary",), vmem_limit_bytes=60 * 2 ** 20),
        name="pack_units",
    )(info, k_t, v_t)


def send_kernel(heavy, n_units, packed_ref, k_ref, v_ref, *rest):
    if heavy:
        got_ref, partner_ref, send_sem, recv_sem, fsend_sem, frecv_sem, psend_sem, precv_sem = rest
        phase = 0
    else:
        _, got_ref, send_sem, recv_sem, fsend_sem, frecv_sem = rest
        phase = 1
    me = lax.axis_index("sp")
    middle = jnp.logical_or(me == 1, me == 2)
    sender = middle if heavy else jnp.logical_not(middle)
    across = (me + 2) % 4
    partner = me + 1 - 2 * (me % 2)
    n_layers = packed_ref.shape[0]
    barrier = pltpu.get_barrier_semaphore()
    for peer in (across, partner):
        pl.semaphore_signal(barrier, inc=1, device_id={"sp": peer}, device_id_type=MESH_ID)
    pl.semaphore_wait(barrier, 2)
    direct = []
    onward = []
    for layer in range(n_layers):
        for kind in range(2):
            index = layer * 2 + kind
            part = pl.ds(0, n_units)
            target = got_ref.at[phase, layer, kind, part]
            direct.append(pltpu.make_async_remote_copy(
                src_ref=packed_ref.at[layer, kind, part], dst_ref=target, send_sem=send_sem.at[index], recv_sem=recv_sem.at[index],
                device_id={"sp": across}, device_id_type=MESH_ID))
            onward.append(pltpu.make_async_remote_copy(
                src_ref=target, dst_ref=target, send_sem=fsend_sem.at[index], recv_sem=frecv_sem.at[index],
                device_id={"sp": partner}, device_id_type=MESH_ID))

    @pl.when(sender)
    def _():
        for copy in direct:
            copy.start()

    shares = []
    if heavy:
        rows = partner_ref.shape[2]
        for kind, source in enumerate((k_ref, v_ref)):
            for layer in range(source.shape[0]):
                index = layer * 2 + kind
                shares.append(pltpu.make_async_remote_copy(
                    src_ref=source.at[layer, pl.ds(rows * partner, rows)], dst_ref=partner_ref.at[kind, layer],
                    send_sem=psend_sem.at[index], recv_sem=precv_sem.at[index],
                    device_id={"sp": partner}, device_id_type=MESH_ID))
        for copy in shares:
            copy.start()

    @pl.when(jnp.logical_not(sender))
    def _():
        for near, far in zip(direct, onward):
            near.wait_recv()
            far.start()
        for far in onward:
            far.wait_send()

    @pl.when(sender)
    def _():
        for near, far in zip(direct, onward):
            near.wait_send()
            far.wait_recv()

    for copy in shares:
        copy.wait()


def send_call(heavy, n_units, slot, packed, k_t, v_t, got=None):
    n_layers = packed.shape[0]
    n_copies = 2 * n_layers
    anywhere = pl.BlockSpec(memory_space=pl.ANY)
    got_shape = jax.ShapeDtypeStruct((2,) + packed.shape, packed.dtype)
    sems = [pltpu.SemaphoreType.DMA((n_copies,)) for _ in range(4)]
    if heavy:
        args = (packed, k_t, v_t)
        rows = k_t.shape[1] // 4
        out_shape = (got_shape, jax.ShapeDtypeStruct((2, k_t.shape[0], rows) + k_t.shape[2:], k_t.dtype))
        sems += [pltpu.SemaphoreType.DMA((2 * k_t.shape[0],)) for _ in range(2)]
        aliases = {}
        out_specs = (anywhere, anywhere)
    else:
        args = (packed, k_t, v_t, got)
        out_shape = got_shape
        aliases = {3: 0}
        out_specs = anywhere
    return pl.pallas_call(
        functools.partial(send_kernel, heavy, n_units),
        out_shape=out_shape, in_specs=[anywhere] * len(args), out_specs=out_specs, scratch_shapes=sems,
        input_output_aliases=aliases,
        compiler_params=pltpu.CompilerParams(collective_id=slot, has_side_effects=True),
        name="send_%s_%d" % ("heavy" if heavy else "light", n_units),
    )(*args)


def attend_kernel(sliding, n_in, *refs):
    info_ref = refs[0]
    q_ref, kn_ref, vn_ref, wo_ref, mlp_ref, own_k, own_v, par_k, par_v = refs[1:10]
    extra = refs[10:10 + n_in]
    out_ref, keys_ref, values_ref, mixed_ref = refs[-4:]
    row = pl.program_id(0)
    n_rows = pl.num_programs(0)
    edge = info_ref[4 + row]
    core = info_ref[0]
    chip = info_ref[1]
    heads, dim = q_ref.shape
    n_units = keys_ref.shape[-1] // LANES
    column = lax.broadcasted_iota(jnp.int32, (dim, PAD), 1)

    def new_column(ref):
        picked = jnp.sum(jnp.where(column == row, ref[...].astype(jnp.float32), 0.0), axis=1, keepdims=True)
        return jnp.broadcast_to(picked, (dim, LANES))

    k_new = new_column(kn_ref)
    v_new = new_column(vn_ref)
    lane = lax.broadcasted_iota(jnp.int32, (dim, LANES), 1)
    for unit in range(n_units):
        fold = unit % (2 * HALF_UNITS)
        half = fold // HALF_UNITS
        cols = pl.ds((fold % HALF_UNITS) * LANES, LANES)
        slot = lane + unit * LANES
        in_own = core == half
        if sliding:
            keep_local = jnp.logical_xor(slot < edge, chip == 0)
            place = jnp.clip(info_ref[16 + 2 * row + half] + unit - info_ref[8 + 2 * row + half], 0, MAX_UNITS - 1)
        for kind, (own, par, new, dest) in enumerate(((own_k, par_k, k_new, keys_ref), (own_v, par_v, v_new, values_ref))):
            mine = own[0, 0, :, cols].astype(jnp.float32)
            other = par[0, 0, 0, :, cols].astype(jnp.float32)
            local = jnp.where(in_own, mine, other)
            if sliding:
                remote = extra[2 * half + kind][0, 0, 0, place].astype(jnp.float32)
                merged = jnp.where(keep_local, local, remote)
                merged = jnp.where(slot == edge, new, merged)
                dest[0, 0, :, pl.ds(unit * LANES, LANES)] = merged.astype(dest.dtype)
            else:
                acr = extra[0][kind, 0, :, cols].astype(jnp.float32)
                dia = extra[1][kind, 0, :, cols].astype(jnp.float32)
                remote = jnp.where(in_own, acr, dia)
                merged = jnp.where(chip == unit // (2 * HALF_UNITS), local, remote)
                merged = jnp.where(slot < edge, merged, 0.0)
                merged = jnp.where(slot == edge, new, merged)
                dest[0, :, pl.ds(unit * LANES, LANES)] = merged.astype(dest.dtype)
    keys = keys_ref[0, 0] if sliding else keys_ref[0]
    values = values_ref[0, 0] if sliding else values_ref[0]
    scores = jnp.dot(q_ref[...], keys, preferred_element_type=jnp.float32) * dim ** -0.5
    if not sliding:
        position = lax.broadcasted_iota(jnp.int32, scores.shape, 1)
        scores = jnp.where(position <= edge, scores, -1e30)
    top = jnp.max(scores, axis=-1, keepdims=True)
    raised = jnp.exp(scores - top)
    weights = (raised / jnp.sum(raised, axis=-1, keepdims=True)).astype(jnp.bfloat16)
    mixed = lax.dot_general(weights, values, (((1,), (1,)), ((), ())), preferred_element_type=jnp.float32)
    mixed_ref[row] = mixed

    @pl.when(row == n_rows - 1)
    def _():
        both = jnp.concatenate([mixed_ref[0], mixed_ref[1]], axis=0).astype(jnp.bfloat16)
        width = wo_ref.shape[1]
        pick_row = lax.broadcasted_iota(jnp.int32, (dim, width), 0)
        pick_col = lax.broadcasted_iota(jnp.int32, (dim, width), 1)
        pick = jnp.where(pick_col % dim == pick_row, 1.0, 0.0).astype(jnp.bfloat16)
        spread = jnp.dot(both, pick, preferred_element_type=jnp.float32)
        at_row = lax.broadcasted_iota(jnp.int32, spread.shape, 0)
        at_col = lax.broadcasted_iota(jnp.int32, spread.shape, 1)
        spread = jnp.where(at_col // dim == at_row % heads, spread, 0.0).astype(jnp.bfloat16)
        product = jnp.dot(spread, wo_ref[0], preferred_element_type=jnp.float32)
        first = jnp.sum(product[:heads], axis=0, keepdims=True)
        second = jnp.sum(product[heads:], axis=0, keepdims=True)
        out_ref[...] = jnp.concatenate([first, second], axis=0) + mlp_ref[...]


def attend_call(layer, sliding, info, query, k_new, v_new, w_out, mlp, k_t, v_t, partner, extra, held):
    n_rows = mlp.shape[0]
    dim = query.shape[1]
    heads = query.shape[0] // n_rows
    half_len = k_t.shape[-1]
    model = mlp.shape[1]
    whole = lambda shape: pl.BlockSpec(shape, lambda r, info: (0,) * len(shape))
    own = pl.BlockSpec((1, 1, dim, half_len), lambda r, info: (layer, info[2] + r, 0, 0))
    shared = lambda kind: pl.BlockSpec((1, 1, 1, dim, half_len), lambda r, info: (kind, layer, r, 0, 0))
    in_specs = [
        pl.BlockSpec((heads, dim), lambda r, info: (r, 0)), whole(k_new.shape), whole(v_new.shape),
        pl.BlockSpec((1,) + w_out.shape[1:], lambda r, info: (layer, 0, 0)), whole(mlp.shape),
        own, own, shared(0), shared(1),
    ]
    args = [query, k_new, v_new, w_out, mlp, k_t, v_t, partner, partner]
    if sliding:
        for half in range(2):
            for kind in range(2):
                in_specs.append(pl.BlockSpec(
                    (1, 1, 1, MAX_UNITS, dim, LANES),
                    functools.partial(lambda r, info, half, kind: (info[6 + half], layer, kind, 0, 0, 0), half=half, kind=kind)))
                args.append(extra)
        total = 2 * half_len
        n_kept = 3
        out_block = pl.BlockSpec((1, 1, dim, total), lambda r, info: (layer, r, 0, 0))
        kept_shape = jax.ShapeDtypeStruct((n_kept, n_rows, dim, total), k_t.dtype)
    else:
        for part in extra:
            in_specs.append(pl.BlockSpec((2, 1, dim, half_len), lambda r, info: (0, r, 0, 0)))
            args.append(part)
        total = 4 * half_len
        out_block = pl.BlockSpec((1, dim, total), lambda r, info: (r, 0, 0))
        kept_shape = jax.ShapeDtypeStruct((n_rows, dim, total), k_t.dtype)
    n_in = len(args) - 9
    aliases = {}
    if held is not None:
        for place, array in enumerate(held):
            aliases[1 + len(args)] = 1 + place
            in_specs.append(pl.BlockSpec(memory_space=pl.ANY))
            args.append(array)
    flops = 4 * n_rows * heads * dim * total + 32 * w_out.shape[1] * model
    return pl.pallas_call(
        functools.partial(attend_kernel, sliding, n_in),
        grid_spec=pltpu.PrefetchScalarGridSpec(
            num_scalar_prefetch=1, grid=(n_rows,), in_specs=in_specs,
            out_specs=(whole((n_rows, model)), out_block, out_block),
            scratch_shapes=[pltpu.VMEM((n_rows, heads, dim), jnp.float32)]),
        out_shape=(jax.ShapeDtypeStruct((n_rows, model), jnp.float32), kept_shape, kept_shape),
        input_output_aliases=aliases,
        compiler_params=pltpu.CompilerParams(dimension_semantics=("arbitrary",), vmem_limit_bytes=60 * 2 ** 20),
        cost_estimate=pl.CostEstimate(flops=flops * 8, bytes_accessed=2 ** 23, transcendentals=0),
        name="attend_%d" % layer,
    )(info, *args)


def solution(mesh):
    cache_spec = P(None, "dp", "tp", "sp", None)
    row_spec = P(("dp", "sp"), None)
    col_spec = P(None, None, "tp")
    inner_spec = P(None, "tp", None)
    window_spec = P(None, ("dp", "sp"), "tp", None, None)
    global_spec = P(("dp", "sp"), "tp", None, None)
    in_specs = (cache_spec, cache_spec, P("dp"), row_spec, P(None, None), col_spec, col_spec, col_spec, inner_spec, col_spec, col_spec, inner_spec)
    out_specs = (row_spec, window_spec, window_spec, global_spec, global_spec)

    def device_step(k_cache, v_cache, lengths, hidden, ln_gain, w_query, w_key, w_value, w_out, w_gate, w_up, w_down):
        n_layers = w_query.shape[0]
        rows_dev = hidden.shape[0]
        head_dim = k_cache.shape[-1]
        n_tp = mesh.shape["tp"]
        me = lax.axis_index("sp")
        core = me % 2
        chip = me // 2
        my_lengths = lax.dynamic_slice_in_dim(lengths, me * rows_dev, rows_dev)
        k_t = k_cache[:, :, 0].swapaxes(-1, -2)
        v_t = v_cache[:, :, 0].swapaxes(-1, -2)
        start, count, base, totals = unit_table(lengths - WINDOW)
        other_lengths = lax.ppermute(lengths, "dp", [(0, 1), (1, 0)])
        other_totals = unit_table(other_lengths - WINDOW)[3]
        most = jnp.maximum(totals, other_totals)
        heavy_need = jnp.maximum(most[0, 0], most[1, 1])
        light_need = jnp.maximum(most[0, 1], most[1, 0])
        heavy_index = jnp.sum(heavy_need > jnp.array(HEAVY_LEVELS, jnp.int32)).astype(jnp.int32)
        light_index = jnp.sum(light_need > jnp.array(LIGHT_LEVELS, jnp.int32)).astype(jnp.int32)

        table = jnp.stack([start, count, base], axis=-1)
        sent = lax.dynamic_slice(table, ((1 - chip) * CHIP_ROWS, core, 0), (CHIP_ROWS, 1, 3))[:, 0]
        sent = sent - jnp.array([1, 0, 0], jnp.int32) * (core * HALF_UNITS)
        pack_info = jnp.concatenate([(1 - chip)[None], sent.reshape(-1)]).astype(jnp.int32)
        mine = lax.dynamic_slice_in_dim(table, me * rows_dev, rows_dev)
        window_info = jnp.concatenate([
            jnp.stack([core, chip, me * rows_dev, me]), my_lengths - WINDOW, jnp.stack([chip, 1 - chip]),
            mine[:, :, 0].reshape(-1), jnp.zeros((4,), jnp.int32), mine[:, :, 2].reshape(-1)]).astype(jnp.int32)
        global_info = jnp.concatenate([jnp.stack([core, chip, me * rows_dev, me]), my_lengths]).astype(jnp.int32)

        packed = pack_call(pack_info, k_t, v_t, n_layers - 1)
        heavy_calls = [functools.partial(send_call, True, n, 1 + i) for i, n in enumerate(HEAVY_LEVELS)]
        light_calls = [functools.partial(send_call, False, n, 1 + len(HEAVY_LEVELS) + i) for i, n in enumerate(LIGHT_LEVELS)]
        got, partner = lax.switch(heavy_index, heavy_calls, packed, k_t, v_t)
        got = lax.switch(light_index, light_calls, packed, k_t, v_t, got)

        got, k_last, v_last = lax.optimization_barrier((got, k_t[n_layers - 1], v_t[n_layers - 1]))
        far = []
        for flip in (2, 3):
            owner = me ^ flip
            rows = jnp.stack([lax.dynamic_slice_in_dim(part, owner * rows_dev, rows_dev) for part in (k_last, v_last)])
            far.append(lax.ppermute(rows, "sp", [(i, i ^ flip) for i in range(4)]))

        residual = hidden.astype(jnp.float32)
        tables = rotary_tables(my_lengths, head_dim, w_query.shape[2] // head_dim)
        wk_t = w_key.swapaxes(1, 2)
        wv_t = w_value.swapaxes(1, 2)
        held = None
        for layer in range(n_layers):
            sliding = layer < n_layers - 1
            query, k_new, v_new, mlp = project_call(layer, sliding, residual, ln_gain[layer:layer + 1], tables, w_query, wk_t, wv_t, w_gate, w_up, w_down)
            if sliding:
                part, *held = attend_call(layer, True, window_info, query, k_new, v_new, w_out, mlp, k_t, v_t, partner, got, held)
            else:
                part, *kept = attend_call(layer, False, global_info, query, k_new, v_new, w_out, mlp, k_t, v_t, partner, far, None)
            residual = sum_call(part, residual, n_tp)

        def back(rows_t):
            return rows_t.swapaxes(-1, -2)

        return (residual.astype(jnp.bfloat16), back(held[0])[:, :, None], back(held[1])[:, :, None],
                back(kept[0])[:, None], back(kept[1])[:, None])

    return jax.shard_map(device_step, mesh=mesh, in_specs=in_specs, out_specs=out_specs, check_vma=False)
```

```python
import functools

import jax
import jax.numpy as jnp
from jax import lax
from jax.experimental import pallas as pl
from jax.experimental.pallas import tpu as pltpu
from jax.sharding import PartitionSpec as P

WINDOW = 4096
ROPE_BASE = 50000
NORM_EPS = 1e-5


PAD = 16
K_STEPS = 4
N_STEPS = 4
MESH_ID = pl.DeviceIdType.MESH


VMEM_GRANT = 58 * 2 ** 20


def layer_kernel(layer, sliding, n_far, *refs):
    info_ref, h_ref, gain_ref, cq_ref, sq_ref, ck_ref, sk_ref, wq_ref, wk_ref, wv_ref, wg_ref, wu_ref, wd_ref = refs[:13]
    wo_hbm, k_hbm, v_hbm, partner_hbm = refs[13:17]
    far = refs[17:17 + n_far]
    (out_ref, keys_hbm, values_hbm, u_ref, q_acc, k_acc, v_acc, g_acc, up_acc, act_ref, q_ref, kn_ref, vn_ref, mlp_ref,
     wo_ref, keys_ref, values_ref, units_ref, spread_ref, in_sem, out_sem) = refs[-21:]
    step = pl.program_id(0)
    n_rows = h_ref.shape[0]
    width = wq_ref.shape[1]
    dim = wk_ref.shape[1]
    q_width = wq_ref.shape[2]
    heads = q_width // dim
    half_len = k_hbm.shape[-1]
    me = info_ref[3]
    chip = info_ref[1]
    first_row = info_ref[2]
    buffers = (keys_ref, values_ref)

    def cache_copies(index):
        found = []
        pieces = 2 if sliding else 4
        for kind, (source, buffer) in enumerate(zip((k_hbm, v_hbm), buffers)):
            for piece in range(pieces):
                place = pl.ds(piece * half_len, half_len)
                who = piece ^ (index % 2) if sliding else piece ^ index
                if who == 0:
                    origin = source.at[layer, pl.ds(first_row, n_rows)]
                elif who == 1:
                    origin = partner_hbm.at[kind, layer]
                else:
                    origin = far[who - 2].at[kind]
                found.append(pltpu.make_async_copy(origin, buffer.at[:, :, place], in_sem.at[kind * 4 + piece]))
        return found

    def unit_copies():
        found = []
        if sliding:
            for half in range(2):
                for kind in range(2):
                    found.append(pltpu.make_async_copy(
                        far[0].at[info_ref[6 + half], layer, kind], units_ref.at[half, kind], in_sem.at[8 + half * 2 + kind]))
        return found

    def wo_copy():
        return pltpu.make_async_copy(wo_hbm.at[layer], wo_ref, in_sem.at[12])

    def out_copies():
        found = []
        for kind, (buffer, kept) in enumerate(zip(buffers, (keys_hbm, values_hbm))):
            target = kept.at[layer] if sliding else kept
            found.append(pltpu.make_async_copy(buffer, target, out_sem.at[kind]))
        return found

    variants = 2 if sliding else 4
    which = me % variants

    @pl.when(step == 0)
    def _():
        for index in range(variants):
            @pl.when(which == index)
            def _():
                for copy in cache_copies(index):
                    copy.start()
        for copy in unit_copies():
            copy.start()
        wo_copy().start()
        rows32 = h_ref[...]
        centered = rows32 - jnp.mean(rows32, axis=-1, keepdims=True)
        variance = jnp.mean(centered * centered, axis=-1, keepdims=True)
        scaled = centered * lax.rsqrt(variance + NORM_EPS)
        normed = scaled * gain_ref[...].astype(jnp.float32)
        padded = jnp.concatenate([normed, jnp.zeros((PAD - n_rows, normed.shape[1]), jnp.float32)], axis=0).astype(jnp.bfloat16)
        for part in range(K_STEPS):
            u_ref[part] = padded[:, part * width:(part + 1) * width]
        q_acc[...] = jnp.zeros_like(q_acc)
        k_acc[...] = jnp.zeros_like(k_acc)
        v_acc[...] = jnp.zeros_like(v_acc)
        g_acc[...] = jnp.zeros_like(g_acc)
        up_acc[...] = jnp.zeros_like(up_acc)

    @pl.when(step < K_STEPS)
    def _():
        part = u_ref[jnp.minimum(step, K_STEPS - 1)]
        nt = (((1,), (1,)), ((), ()))
        q_acc[...] += jnp.dot(part, wq_ref[0], preferred_element_type=jnp.float32)
        k_acc[...] += lax.dot_general(wk_ref[0], part, nt, preferred_element_type=jnp.float32)
        v_acc[...] += lax.dot_general(wv_ref[0], part, nt, preferred_element_type=jnp.float32)
        g_acc[...] += jnp.dot(part, wg_ref[0], preferred_element_type=jnp.float32)
        up_acc[...] += jnp.dot(part, wu_ref[0], preferred_element_type=jnp.float32)

    @pl.when(step == K_STEPS - 1)
    def _():
        gate = g_acc[...]
        act_ref[...] = (gate * jax.nn.sigmoid(gate) * up_acc[...]).astype(jnp.bfloat16)
        query = q_acc[:8]
        k_new = k_acc[...]
        if sliding:
            lane = lax.broadcasted_iota(jnp.int32, query.shape, 1)
            swapped = jnp.where(lane % dim < dim // 2, pltpu.roll(query, q_width - dim // 2, 1), pltpu.roll(query, dim // 2, 1))
            query = query * cq_ref[...] + swapped * sq_ref[...]
            first = k_new[:dim // 2]
            second = k_new[dim // 2:]
            cosine = ck_ref[...]
            sine = sk_ref[...]
            k_new = jnp.concatenate([first * cosine - second * sine, second * cosine + first * sine], axis=0)
        kn_ref[...] = k_new.astype(jnp.bfloat16).astype(jnp.float32)
        vn_ref[...] = v_acc[...].astype(jnp.bfloat16).astype(jnp.float32)
        spread = [jnp.broadcast_to(query[r:r + 1], (heads, q_width)) for r in range(n_rows)]
        spread = jnp.concatenate(spread, axis=0)
        row = lax.broadcasted_iota(jnp.int32, spread.shape, 0)
        lane = lax.broadcasted_iota(jnp.int32, spread.shape, 1)
        masked = jnp.where(lane // dim == row % heads, spread, 0.0).astype(jnp.bfloat16)
        pick_row = lax.broadcasted_iota(jnp.int32, (q_width, dim), 0)
        pick_col = lax.broadcasted_iota(jnp.int32, (q_width, dim), 1)
        pick = jnp.where(pick_row % dim == pick_col, 1.0, 0.0).astype(jnp.bfloat16)
        q_ref[...] = jnp.dot(masked, pick, preferred_element_type=jnp.float32).astype(jnp.bfloat16)

    @pl.when(step == K_STEPS)
    def _():
        for index in range(variants):
            @pl.when(which == index)
            def _():
                for copy in cache_copies(index):
                    copy.wait()
        for copy in unit_copies():
            copy.wait()
        column = lax.broadcasted_iota(jnp.int32, (dim, PAD), 1)
        lane = lax.broadcasted_iota(jnp.int32, (dim, LANES), 1)
        for row in range(n_rows):
            edge = info_ref[4 + row]
            border = edge // LANES
            cols = pl.ds(pl.multiple_of(border * LANES, LANES), LANES)
            slot = lane + border * LANES
            before = [buffer[row, :, cols] for buffer in buffers]
            if sliding:
                for half in range(2):
                    start = info_ref[8 + 2 * row + half]
                    count = info_ref[12 + 2 * row + half]
                    base = info_ref[16 + 2 * row + half]

                    def place_unit(unit, carry, half=half, start=start, base=base):
                        to = pl.ds(pl.multiple_of(unit * LANES, LANES), LANES)
                        for kind, buffer in enumerate(buffers):
                            buffer[row, :, to] = units_ref[half, kind, base + unit - start]
                        return carry

                    lax.fori_loop(start, start + count, place_unit, 0)
                border_half = border // HALF_UNITS
                border_place = jnp.clip(info_ref[16 + 2 * row + border_half] + border - info_ref[8 + 2 * row + border_half], 0, MAX_UNITS - 1)
                keep = jnp.logical_xor(slot < edge, chip == 0)
            else:
                def clear_unit(unit, carry):
                    to = pl.ds(pl.multiple_of(unit * LANES, LANES), LANES)
                    for buffer in buffers:
                        buffer[row, :, to] = jnp.zeros((dim, LANES), buffer.dtype)
                    return carry

                lax.fori_loop(border + 1, 4 * HALF_UNITS, clear_unit, 0)
                keep = slot < edge
            for kind, (buffer, new) in enumerate(zip(buffers, (kn_ref, vn_ref))):
                picked = jnp.sum(jnp.where(column == row, new[...], 0.0), axis=1, keepdims=True)
                if sliding:
                    remote = units_ref[border_half, kind, border_place].astype(jnp.float32)
                else:
                    remote = jnp.zeros((dim, LANES), jnp.float32)
                merged = jnp.where(keep, before[kind].astype(jnp.float32), remote)
                merged = jnp.where(slot == edge, jnp.broadcast_to(picked, (dim, LANES)), merged)
                buffer[row, :, cols] = merged.astype(buffer.dtype)
        for copy in out_copies():
            copy.start()
        mixed = []
        for row in range(n_rows):
            edge = info_ref[4 + row]
            scores = jnp.dot(q_ref[heads * row:heads * (row + 1)], keys_ref[row], preferred_element_type=jnp.float32) * dim ** -0.5
            if not sliding:
                position = lax.broadcasted_iota(jnp.int32, scores.shape, 1)
                scores = jnp.where(position <= edge, scores, -1e30)
            top = jnp.max(scores, axis=-1, keepdims=True)
            raised = jnp.exp(scores - top)
            weights = (raised / jnp.sum(raised, axis=-1, keepdims=True)).astype(jnp.bfloat16)
            mixed.append(lax.dot_general(weights, values_ref[row], (((1,), (1,)), ((), ())), preferred_element_type=jnp.float32))
        both = jnp.concatenate(mixed, axis=0).astype(jnp.bfloat16)
        pick_row = lax.broadcasted_iota(jnp.int32, (dim, q_width), 0)
        pick_col = lax.broadcasted_iota(jnp.int32, (dim, q_width), 1)
        pick = jnp.where(pick_col % dim == pick_row, 1.0, 0.0).astype(jnp.bfloat16)
        wide = jnp.dot(both, pick, preferred_element_type=jnp.float32)
        at_row = lax.broadcasted_iota(jnp.int32, wide.shape, 0)
        at_col = lax.broadcasted_iota(jnp.int32, wide.shape, 1)
        spread_ref[...] = jnp.where(at_col // dim == at_row % heads, wide, 0.0).astype(jnp.bfloat16)

    @pl.when(step >= K_STEPS)
    def _():
        mlp_ref[jnp.maximum(step - K_STEPS, 0)] = jnp.dot(act_ref[...], wd_ref[0], preferred_element_type=jnp.float32)

    @pl.when(step == K_STEPS + N_STEPS - 1)
    def _():
        wo_copy().wait()
        product = jnp.dot(spread_ref[...], wo_ref[...], preferred_element_type=jnp.float32)
        sums = [jnp.sum(product[heads * r:heads * (r + 1)], axis=0, keepdims=True) for r in range(n_rows)]
        sums = jnp.concatenate(sums, axis=0)
        n_len = mlp_ref.shape[2]
        for part in range(N_STEPS):
            where = slice(part * n_len, (part + 1) * n_len)
            out_ref[:, where] = sums[:, where] + mlp_ref[part][:n_rows]
        for copy in out_copies():
            copy.wait()


def layer_call(layer, sliding, info, h, gain, tables, w_query, wk_t, wv_t, w_out, w_gate, w_up, w_down, k_t, v_t, partner, far, held):
    n_rows, model = h.shape
    q_width = w_query.shape[2]
    dim = wk_t.shape[1]
    hidden = w_gate.shape[2]
    half_len = k_t.shape[-1]
    heads = q_width // dim
    k_len = model // K_STEPS
    n_len = model // N_STEPS
    last_k = K_STEPS - 1
    whole = lambda shape: pl.BlockSpec(shape, lambda i, info: (0,) * len(shape))
    by_k = lambda shape: pl.BlockSpec(shape, lambda i, info: (layer, jnp.minimum(i, last_k), 0))
    by_kt = pl.BlockSpec((1, dim, k_len), lambda i, info: (layer, 0, jnp.minimum(i, last_k)))
    anywhere = pl.BlockSpec(memory_space=pl.ANY)
    total = (2 if sliding else 4) * half_len
    kept = (3, n_rows, dim, total) if sliding else (n_rows, dim, total)
    kept_shape = jax.ShapeDtypeStruct(kept, k_t.dtype)
    args = [h, gain, *tables, w_query, wk_t, wv_t, w_gate, w_up, w_down, w_out, k_t, v_t, partner, *far]
    in_specs = [
        whole((n_rows, model)), pl.BlockSpec((1, model), lambda i, info: (0, 0)),
        whole(tables[0].shape), whole(tables[1].shape), whole(tables[2].shape), whole(tables[3].shape),
        by_k((1, k_len, q_width)), by_kt, by_kt, by_k((1, k_len, hidden)), by_k((1, k_len, hidden)),
        pl.BlockSpec((1, hidden, n_len), lambda i, info: (layer, 0, jnp.maximum(i - K_STEPS, 0))),
    ] + [anywhere] * (4 + len(far))
    aliases = {}
    if held is not None:
        for place, array in enumerate(held):
            aliases[1 + len(args)] = 1 + place
            in_specs.append(anywhere)
            args.append(array)
    weight_bytes = 2 * (2 * model * q_width + 2 * dim * model + 3 * model * hidden)
    units = (2, 2, MAX_UNITS, dim, LANES) if sliding else (8, LANES)
    return pl.pallas_call(
        functools.partial(layer_kernel, layer, sliding, len(far)),
        grid_spec=pltpu.PrefetchScalarGridSpec(
            num_scalar_prefetch=1, grid=(K_STEPS + N_STEPS,), in_specs=in_specs,
            out_specs=(whole((n_rows, model)), anywhere, anywhere),
            scratch_shapes=[
                pltpu.VMEM((K_STEPS, PAD, k_len), jnp.bfloat16),
                pltpu.VMEM((PAD, q_width), jnp.float32),
                pltpu.VMEM((dim, PAD), jnp.float32),
                pltpu.VMEM((dim, PAD), jnp.float32),
                pltpu.VMEM((PAD, hidden), jnp.float32),
                pltpu.VMEM((PAD, hidden), jnp.float32),
                pltpu.VMEM((PAD, hidden), jnp.bfloat16),
                pltpu.VMEM((n_rows * heads, dim), jnp.bfloat16),
                pltpu.VMEM((dim, PAD), jnp.float32),
                pltpu.VMEM((dim, PAD), jnp.float32),
                pltpu.VMEM((N_STEPS, PAD, n_len), jnp.float32),
                pltpu.VMEM((q_width, model), jnp.bfloat16),
                pltpu.VMEM((n_rows, dim, total), jnp.bfloat16),
                pltpu.VMEM((n_rows, dim, total), jnp.bfloat16),
                pltpu.VMEM(units, jnp.bfloat16),
                pltpu.VMEM((n_rows * heads, q_width), jnp.bfloat16),
                pltpu.SemaphoreType.DMA((13,)),
                pltpu.SemaphoreType.DMA((2,)),
            ]),
        out_shape=(jax.ShapeDtypeStruct((n_rows, model), jnp.float32), kept_shape, kept_shape),
        input_output_aliases=aliases,
        compiler_params=pltpu.CompilerParams(dimension_semantics=("arbitrary",), vmem_limit_bytes=VMEM_GRANT),
        cost_estimate=pl.CostEstimate(flops=PAD * weight_bytes, bytes_accessed=weight_bytes, transcendentals=0),
        name="layer_%d" % layer,
    )(info, *args)


def rotary_tables(positions, dim, heads):
    half = dim // 2
    inv_freq = 1.0 / (ROPE_BASE ** (jnp.arange(half, dtype=jnp.float32) * 2.0 / dim))
    angles = positions.astype(jnp.float32)[:, None] * inv_freq[None, :]
    cosine = jnp.cos(angles)
    sine = jnp.sin(angles)
    n_rows = positions.shape[0]
    cq = jnp.pad(jnp.tile(jnp.concatenate([cosine, cosine], axis=1), (1, heads)), ((0, 8 - n_rows), (0, 0)))
    sq = jnp.pad(jnp.tile(jnp.concatenate([-sine, sine], axis=1), (1, heads)), ((0, 8 - n_rows), (0, 0)))
    ck = jnp.pad(cosine.T, ((0, 0), (0, PAD - n_rows)))
    sk = jnp.pad(sine.T, ((0, 0), (0, PAD - n_rows)))
    return cq, sq, ck, sk


def sum_kernel(n_tp, part_ref, resid_ref, out_ref, slots, send_sem, recv_sem):
    me = lax.axis_index("tp")
    barrier = pltpu.get_barrier_semaphore()
    for flip in range(1, n_tp):
        pl.semaphore_signal(barrier, inc=1, device_id={"tp": me ^ flip}, device_id_type=MESH_ID)
    pl.semaphore_wait(barrier, n_tp - 1)
    copies = []
    for flip in range(1, n_tp):
        copy = pltpu.make_async_remote_copy(
            src_ref=part_ref, dst_ref=slots.at[me], send_sem=send_sem.at[flip - 1], recv_sem=recv_sem.at[flip - 1],
            device_id={"tp": me ^ flip}, device_id_type=MESH_ID)
        copy.start()
        copies.append(copy)
    slots[me] = part_ref[...]
    for copy in copies:
        copy.wait()
    total = slots[0]
    for index in range(1, n_tp):
        total = total + slots[index]
    out_ref[...] = (resid_ref[...] + total).astype(jnp.bfloat16).astype(jnp.float32)


def sum_call(part, resid, n_tp):
    return pl.pallas_call(
        functools.partial(sum_kernel, n_tp),
        out_shape=jax.ShapeDtypeStruct(part.shape, jnp.float32),
        in_specs=[pl.BlockSpec(memory_space=pltpu.VMEM)] * 2,
        out_specs=pl.BlockSpec(memory_space=pltpu.VMEM),
        scratch_shapes=[
            pltpu.VMEM((n_tp,) + part.shape, jnp.float32),
            pltpu.SemaphoreType.DMA((n_tp - 1,)),
            pltpu.SemaphoreType.DMA((n_tp - 1,)),
        ],
        compiler_params=pltpu.CompilerParams(collective_id=0, has_side_effects=True),
        name="sum_tp",
    )(part, resid)


LANES = 128
HALF_UNITS = 16
CHIP_ROWS = 4
MAX_UNITS = CHIP_ROWS * HALF_UNITS
HEAVY_LEVELS = (32, 40, 44, 48, 52, 56, 60, 64)
LIGHT_LEVELS = (8, 16, 20, 24, 28, 32, 36, 40, 44, 48, 56, 64)


def unit_table(offsets):
    half = jnp.arange(2, dtype=jnp.int32)[None, :] * HALF_UNITS
    edge = offsets[:, None]
    upper_end = jnp.clip((edge + LANES - 1) // LANES, half, half + HALF_UNITS)
    lower_start = jnp.clip((edge + 1) // LANES, half, half + HALF_UNITS)
    from_upper = jnp.arange(offsets.shape[0], dtype=jnp.int32)[:, None] < CHIP_ROWS
    start = jnp.where(from_upper, half, lower_start)
    count = jnp.where(from_upper, upper_end - half, half + HALF_UNITS - lower_start)
    by_chip = count.reshape(2, CHIP_ROWS, 2)
    ends = jnp.cumsum(by_chip, axis=1)
    base = (ends - by_chip).reshape(count.shape)
    return start, count, base, ends[:, -1]


def pack_kernel(info_ref, k_ref, v_ref, out_ref):
    for row in range(CHIP_ROWS):
        first = info_ref[1 + 3 * row]
        count = info_ref[2 + 3 * row]
        base = info_ref[3 + 3 * row]
        for unit in range(HALF_UNITS):
            @pl.when(jnp.logical_and(unit >= first, unit < first + count))
            def _():
                place = base + unit - first
                cols = pl.ds(unit * LANES, LANES)
                out_ref[0, 0, place] = k_ref[0, row, :, cols]
                out_ref[0, 1, place] = v_ref[0, row, :, cols]


def pack_call(info, k_t, v_t, n_layers):
    dim, half_len = k_t.shape[2:]
    block = pl.BlockSpec((1, CHIP_ROWS, dim, half_len), lambda l, info: (l, info[0], 0, 0))
    return pl.pallas_call(
        pack_kernel,
        grid_spec=pltpu.PrefetchScalarGridSpec(
            num_scalar_prefetch=1, grid=(n_layers,), in_specs=[block, block],
            out_specs=pl.BlockSpec((1, 2, MAX_UNITS, dim, LANES), lambda l, info: (l, 0, 0, 0, 0))),
        out_shape=jax.ShapeDtypeStruct((n_layers, 2, MAX_UNITS, dim, LANES), k_t.dtype),
        compiler_params=pltpu.CompilerParams(dimension_semantics=("arbitrary",), vmem_limit_bytes=VMEM_GRANT),
        name="pack_units",
    )(info, k_t, v_t)


def send_kernel(heavy, n_units, packed_ref, k_ref, v_ref, *rest):
    if heavy:
        got_ref, partner_ref, send_sem, recv_sem, fsend_sem, frecv_sem, psend_sem, precv_sem = rest
        phase = 0
    else:
        _, got_ref, send_sem, recv_sem, fsend_sem, frecv_sem = rest
        phase = 1
    me = lax.axis_index("sp")
    middle = jnp.logical_or(me == 1, me == 2)
    sender = middle if heavy else jnp.logical_not(middle)
    across = (me + 2) % 4
    partner = me + 1 - 2 * (me % 2)
    n_layers = packed_ref.shape[0]
    barrier = pltpu.get_barrier_semaphore()
    for peer in (across, partner):
        pl.semaphore_signal(barrier, inc=1, device_id={"sp": peer}, device_id_type=MESH_ID)
    pl.semaphore_wait(barrier, 2)
    direct = []
    onward = []
    for layer in range(n_layers):
        for kind in range(2):
            index = layer * 2 + kind
            part = pl.ds(0, n_units)
            target = got_ref.at[phase, layer, kind, part]
            direct.append(pltpu.make_async_remote_copy(
                src_ref=packed_ref.at[layer, kind, part], dst_ref=target, send_sem=send_sem.at[index], recv_sem=recv_sem.at[index],
                device_id={"sp": across}, device_id_type=MESH_ID))
            onward.append(pltpu.make_async_remote_copy(
                src_ref=target, dst_ref=target, send_sem=fsend_sem.at[index], recv_sem=frecv_sem.at[index],
                device_id={"sp": partner}, device_id_type=MESH_ID))

    @pl.when(sender)
    def _():
        for copy in direct:
            copy.start()

    shares = []
    if heavy:
        rows = partner_ref.shape[2]
        for kind, source in enumerate((k_ref, v_ref)):
            for layer in range(source.shape[0]):
                index = layer * 2 + kind
                shares.append(pltpu.make_async_remote_copy(
                    src_ref=source.at[layer, pl.ds(rows * partner, rows)], dst_ref=partner_ref.at[kind, layer],
                    send_sem=psend_sem.at[index], recv_sem=precv_sem.at[index],
                    device_id={"sp": partner}, device_id_type=MESH_ID))
        for copy in shares:
            copy.start()

    @pl.when(jnp.logical_not(sender))
    def _():
        for near, far in zip(direct, onward):
            near.wait_recv()
            far.start()
        for far in onward:
            far.wait_send()

    @pl.when(sender)
    def _():
        for near, far in zip(direct, onward):
            near.wait_send()
            far.wait_recv()

    for copy in shares:
        copy.wait()


def send_call(heavy, n_units, slot, packed, k_t, v_t, got=None):
    n_layers = packed.shape[0]
    n_copies = 2 * n_layers
    anywhere = pl.BlockSpec(memory_space=pl.ANY)
    got_shape = jax.ShapeDtypeStruct((2,) + packed.shape, packed.dtype)
    sems = [pltpu.SemaphoreType.DMA((n_copies,)) for _ in range(4)]
    if heavy:
        args = (packed, k_t, v_t)
        rows = k_t.shape[1] // 4
        out_shape = (got_shape, jax.ShapeDtypeStruct((2, k_t.shape[0], rows) + k_t.shape[2:], k_t.dtype))
        sems += [pltpu.SemaphoreType.DMA((2 * k_t.shape[0],)) for _ in range(2)]
        aliases = {}
        out_specs = (anywhere, anywhere)
    else:
        args = (packed, k_t, v_t, got)
        out_shape = got_shape
        aliases = {3: 0}
        out_specs = anywhere
    return pl.pallas_call(
        functools.partial(send_kernel, heavy, n_units),
        out_shape=out_shape, in_specs=[anywhere] * len(args), out_specs=out_specs, scratch_shapes=sems,
        input_output_aliases=aliases,
        compiler_params=pltpu.CompilerParams(collective_id=slot, has_side_effects=True),
        name="send_%s_%d" % ("heavy" if heavy else "light", n_units),
    )(*args)


def solution(mesh):
    cache_spec = P(None, "dp", "tp", "sp", None)
    row_spec = P(("dp", "sp"), None)
    col_spec = P(None, None, "tp")
    inner_spec = P(None, "tp", None)
    window_spec = P(None, ("dp", "sp"), "tp", None, None)
    global_spec = P(("dp", "sp"), "tp", None, None)
    in_specs = (cache_spec, cache_spec, P("dp"), row_spec, P(None, None), col_spec, col_spec, col_spec, inner_spec, col_spec, col_spec, inner_spec)
    out_specs = (row_spec, window_spec, window_spec, global_spec, global_spec)

    def device_step(k_cache, v_cache, lengths, hidden, ln_gain, w_query, w_key, w_value, w_out, w_gate, w_up, w_down):
        n_layers = w_query.shape[0]
        rows_dev = hidden.shape[0]
        head_dim = k_cache.shape[-1]
        n_tp = mesh.shape["tp"]
        me = lax.axis_index("sp")
        core = me % 2
        chip = me // 2
        my_lengths = lax.dynamic_slice_in_dim(lengths, me * rows_dev, rows_dev)
        k_t = k_cache[:, :, 0].swapaxes(-1, -2)
        v_t = v_cache[:, :, 0].swapaxes(-1, -2)
        start, count, base, totals = unit_table(lengths - WINDOW)
        other_lengths = lax.ppermute(lengths, "dp", [(0, 1), (1, 0)])
        other_totals = unit_table(other_lengths - WINDOW)[3]
        most = jnp.maximum(totals, other_totals)
        heavy_need = jnp.maximum(most[0, 0], most[1, 1])
        light_need = jnp.maximum(most[0, 1], most[1, 0])
        heavy_index = jnp.sum(heavy_need > jnp.array(HEAVY_LEVELS, jnp.int32)).astype(jnp.int32)
        light_index = jnp.sum(light_need > jnp.array(LIGHT_LEVELS, jnp.int32)).astype(jnp.int32)

        table = jnp.stack([start, count, base], axis=-1)
        sent = lax.dynamic_slice(table, ((1 - chip) * CHIP_ROWS, core, 0), (CHIP_ROWS, 1, 3))[:, 0]
        sent = sent - jnp.array([1, 0, 0], jnp.int32) * (core * HALF_UNITS)
        pack_info = jnp.concatenate([(1 - chip)[None], sent.reshape(-1)]).astype(jnp.int32)
        mine = lax.dynamic_slice_in_dim(table, me * rows_dev, rows_dev)
        window_info = jnp.concatenate([
            jnp.stack([core, chip, me * rows_dev, me]), my_lengths - WINDOW, jnp.stack([chip, 1 - chip]),
            mine[:, :, 0].reshape(-1), mine[:, :, 1].reshape(-1), mine[:, :, 2].reshape(-1)]).astype(jnp.int32)
        global_info = jnp.concatenate([jnp.stack([core, chip, me * rows_dev, me]), my_lengths]).astype(jnp.int32)

        packed = pack_call(pack_info, k_t, v_t, n_layers - 1)
        heavy_calls = [functools.partial(send_call, True, n, 1 + i) for i, n in enumerate(HEAVY_LEVELS)]
        light_calls = [functools.partial(send_call, False, n, 1 + len(HEAVY_LEVELS) + i) for i, n in enumerate(LIGHT_LEVELS)]
        got, partner = lax.switch(heavy_index, heavy_calls, packed, k_t, v_t)
        got = lax.switch(light_index, light_calls, packed, k_t, v_t, got)

        got, after = lax.optimization_barrier((got, me))
        far = []
        for flip in (2, 3):
            first = (after ^ flip) * rows_dev
            rows = jnp.concatenate([
                lax.dynamic_slice(part, (n_layers - 1, first, 0, 0), (1, rows_dev) + part.shape[2:]) for part in (k_t, v_t)])
            far.append(lax.ppermute(rows, "sp", [(i, i ^ flip) for i in range(4)]))

        residual = hidden.astype(jnp.float32)
        tables = rotary_tables(my_lengths, head_dim, w_query.shape[2] // head_dim)
        wk_t = w_key.swapaxes(1, 2)
        wv_t = w_value.swapaxes(1, 2)
        held = None
        for layer in range(n_layers):
            sliding = layer < n_layers - 1
            common = (residual, ln_gain[layer:layer + 1], tables, w_query, wk_t, wv_t, w_out, w_gate, w_up, w_down, k_t, v_t, partner)
            if sliding:
                part, *held = layer_call(layer, True, window_info, *common, [got], held)
            else:
                part, *kept = layer_call(layer, False, global_info, *common, far, None)
            residual = sum_call(part, residual, n_tp)

        def back(rows_t):
            return rows_t.swapaxes(-1, -2)

        return (residual.astype(jnp.bfloat16), back(held[0])[:, :, None], back(held[1])[:, :, None],
                back(kept[0])[:, None], back(kept[1])[:, None])

    return jax.shard_map(device_step, mesh=mesh, in_specs=in_specs, out_specs=out_specs, check_vma=False)
```

```python
import functools

import jax
import jax.numpy as jnp
from jax import lax
from jax.experimental import pallas as pl
from jax.experimental.pallas import tpu as pltpu
from jax.sharding import PartitionSpec as P

WINDOW = 4096
ROPE_BASE = 50000
NORM_EPS = 1e-5


PAD = 16
K_STEPS = 4
DOWN_ROWS = 384
MESH_ID = pl.DeviceIdType.MESH


VMEM_GRANT = 58 * 2 ** 20


def layer_kernel(layer, sliding, n_far, info_ref, h_ref, gain_ref, cq_ref, sq_ref, ck_ref, sk_ref, *refs):
    wq_hbm, wk_hbm, wv_hbm, wg_hbm, wu_hbm, wd_hbm, wo_hbm, k_hbm, v_hbm, partner_hbm = refs[:10]
    far = refs[10:10 + n_far]
    (out_ref, keys_hbm, values_hbm, wq_ref, wk_ref, wv_ref, wg_ref, wu_ref, wd_ref, wo_ref, keys_ref, values_ref, units_ref,
     weight_sem, in_sem, out_sem) = refs[-16:]
    n_rows, model = h_ref.shape
    dim = wk_ref.shape[0]
    q_width = wq_ref.shape[1]
    hidden = wg_ref.shape[1]
    heads = q_width // dim
    half_len = k_hbm.shape[-1]
    me = info_ref[3]
    chip = info_ref[1]
    first_row = info_ref[2]
    buffers = (keys_ref, values_ref)

    def cache_copies(index):
        found = []
        pieces = 2 if sliding else 4
        for kind, (source, buffer) in enumerate(zip((k_hbm, v_hbm), buffers)):
            for piece in range(pieces):
                place = pl.ds(piece * half_len, half_len)
                who = piece ^ (index % 2) if sliding else piece ^ index
                if who == 0:
                    origin = source.at[layer, pl.ds(first_row, n_rows)]
                elif who == 1:
                    origin = partner_hbm.at[kind, layer]
                else:
                    origin = far[who - 2].at[kind]
                found.append(pltpu.make_async_copy(origin, buffer.at[:, :, place], in_sem.at[kind * 4 + piece]))
        return found

    variants = 2 if sliding else 4
    which = me % variants

    def each_variant(act):
        for index in range(variants):
            @pl.when(which == index)
            def _():
                for copy in cache_copies(index):
                    act(copy)

    unit_copies = []
    if sliding:
        for half in range(2):
            for kind in range(2):
                unit_copies.append(pltpu.make_async_copy(
                    far[0].at[info_ref[6 + half], layer, kind], units_ref.at[half, kind], in_sem.at[8 + half * 2 + kind]))

    n_sem = [0]

    def weight_copy(source, target, first, size):
        rows = pl.ds(first, size)
        copy = pltpu.make_async_copy(source.at[layer, rows], target.at[rows], weight_sem.at[n_sem[0]])
        n_sem[0] += 1
        return copy

    k_len = model // K_STEPS
    down_cuts = [(first, min(DOWN_ROWS, hidden - first)) for first in range(0, hidden, DOWN_ROWS)]
    proj_copies = [weight_copy(wq_hbm, wq_ref, 0, model), weight_copy(wk_hbm, wk_ref, 0, dim), weight_copy(wv_hbm, wv_ref, 0, dim)]
    up_copies = [[weight_copy(wg_hbm, wg_ref, part * k_len, k_len), weight_copy(wu_hbm, wu_ref, part * k_len, k_len)] for part in range(K_STEPS)]
    out_weight = weight_copy(wo_hbm, wo_ref, 0, q_width)
    down_copies = [weight_copy(wd_hbm, wd_ref, first, size) for first, size in down_cuts]

    def start(copies):
        for copy in copies:
            copy.start()

    def wait(copies):
        for copy in copies:
            copy.wait()

    start(proj_copies)
    each_variant(lambda copy: copy.start())
    start(unit_copies)
    start(up_copies[0])
    start(up_copies[1])

    rows32 = h_ref[...]
    centered = rows32 - jnp.mean(rows32, axis=-1, keepdims=True)
    variance = jnp.mean(centered * centered, axis=-1, keepdims=True)
    scaled = centered * lax.rsqrt(variance + NORM_EPS)
    normed = scaled * gain_ref[...].astype(jnp.float32)
    normed = jnp.concatenate([normed, jnp.zeros((PAD - n_rows, model), jnp.float32)], axis=0).astype(jnp.bfloat16)

    nt = (((1,), (1,)), ((), ()))
    wait(proj_copies)
    query = jnp.dot(normed, wq_ref[...], preferred_element_type=jnp.float32)[:8]
    k_new = lax.dot_general(wk_ref[...], normed, nt, preferred_element_type=jnp.float32)
    v_new = lax.dot_general(wv_ref[...], normed, nt, preferred_element_type=jnp.float32)
    if sliding:
        lane = lax.broadcasted_iota(jnp.int32, query.shape, 1)
        swapped = jnp.where(lane % dim < dim // 2, pltpu.roll(query, q_width - dim // 2, 1), pltpu.roll(query, dim // 2, 1))
        query = query * cq_ref[...] + swapped * sq_ref[...]
        first = k_new[:dim // 2]
        second = k_new[dim // 2:]
        cosine = ck_ref[...]
        sine = sk_ref[...]
        k_new = jnp.concatenate([first * cosine - second * sine, second * cosine + first * sine], axis=0)
    k_new = k_new.astype(jnp.bfloat16).astype(jnp.float32)
    v_new = v_new.astype(jnp.bfloat16).astype(jnp.float32)
    spread = [jnp.broadcast_to(query[r:r + 1], (heads, q_width)) for r in range(n_rows)]
    spread = jnp.concatenate(spread, axis=0)
    at_row = lax.broadcasted_iota(jnp.int32, spread.shape, 0)
    at_col = lax.broadcasted_iota(jnp.int32, spread.shape, 1)
    own_head = at_col // dim == at_row % heads
    masked = jnp.where(own_head, spread, 0.0).astype(jnp.bfloat16)
    pick_row = lax.broadcasted_iota(jnp.int32, (dim, q_width), 0)
    pick_col = lax.broadcasted_iota(jnp.int32, (dim, q_width), 1)
    pick = jnp.where(pick_col % dim == pick_row, 1.0, 0.0).astype(jnp.bfloat16)
    head_q = lax.dot_general(masked, pick, nt, preferred_element_type=jnp.float32).astype(jnp.bfloat16)

    start(up_copies[2])
    each_variant(lambda copy: copy.wait())
    wait(unit_copies)
    column = lax.broadcasted_iota(jnp.int32, (dim, PAD), 1)
    lane = lax.broadcasted_iota(jnp.int32, (dim, LANES), 1)
    for row in range(n_rows):
        edge = info_ref[4 + row]
        border = edge // LANES
        cols = pl.ds(pl.multiple_of(border * LANES, LANES), LANES)
        slot = lane + border * LANES
        before = [buffer[row, :, cols] for buffer in buffers]
        if sliding:
            for half in range(2):
                begin = info_ref[8 + 2 * row + half]
                count = info_ref[12 + 2 * row + half]
                base = info_ref[16 + 2 * row + half]

                def place_unit(unit, carry, half=half, begin=begin, base=base):
                    to = pl.ds(pl.multiple_of(unit * LANES, LANES), LANES)
                    for kind, buffer in enumerate(buffers):
                        buffer[row, :, to] = units_ref[half, kind, base + unit - begin]
                    return carry

                lax.fori_loop(begin, begin + count, place_unit, 0)
            border_half = border // HALF_UNITS
            border_place = jnp.clip(info_ref[16 + 2 * row + border_half] + border - info_ref[8 + 2 * row + border_half], 0, MAX_UNITS - 1)
            keep = jnp.logical_xor(slot < edge, chip == 0)
        else:
            def clear_unit(unit, carry):
                to = pl.ds(pl.multiple_of(unit * LANES, LANES), LANES)
                for buffer in buffers:
                    buffer[row, :, to] = jnp.zeros((dim, LANES), buffer.dtype)
                return carry

            lax.fori_loop(border + 1, 4 * HALF_UNITS, clear_unit, 0)
            keep = slot < edge
        for kind, (buffer, new) in enumerate(zip(buffers, (k_new, v_new))):
            picked = jnp.sum(jnp.where(column == row, new, 0.0), axis=1, keepdims=True)
            if sliding:
                remote = units_ref[border_half, kind, border_place].astype(jnp.float32)
            else:
                remote = jnp.zeros((dim, LANES), jnp.float32)
            merged = jnp.where(keep, before[kind].astype(jnp.float32), remote)
            merged = jnp.where(slot == edge, jnp.broadcast_to(picked, (dim, LANES)), merged)
            buffer[row, :, cols] = merged.astype(buffer.dtype)
    start(up_copies[3])
    out_copies = []
    for kind, (buffer, kept) in enumerate(zip(buffers, (keys_hbm, values_hbm))):
        target = kept.at[layer] if sliding else kept
        out_copies.append(pltpu.make_async_copy(buffer, target, out_sem.at[kind]))
    start(out_copies)
    mixed = []
    for row in range(n_rows):
        edge = info_ref[4 + row]
        scores = jnp.dot(head_q[heads * row:heads * (row + 1)], keys_ref[row], preferred_element_type=jnp.float32) * dim ** -0.5
        if not sliding:
            position = lax.broadcasted_iota(jnp.int32, scores.shape, 1)
            scores = jnp.where(position <= edge, scores, -1e30)
        top = jnp.max(scores, axis=-1, keepdims=True)
        raised = jnp.exp(scores - top)
        weights = (raised / jnp.sum(raised, axis=-1, keepdims=True)).astype(jnp.bfloat16)
        mixed.append(lax.dot_general(weights, values_ref[row], nt, preferred_element_type=jnp.float32))
    both = jnp.concatenate(mixed, axis=0).astype(jnp.bfloat16)
    wide = jnp.dot(both, pick, preferred_element_type=jnp.float32)
    wide = jnp.where(own_head, wide, 0.0).astype(jnp.bfloat16)

    start([out_weight])
    start(down_copies)
    gate = jnp.zeros((PAD, hidden), jnp.float32)
    raise_ = jnp.zeros((PAD, hidden), jnp.float32)
    for part in range(K_STEPS):
        wait(up_copies[part])
        rows = slice(part * k_len, (part + 1) * k_len)
        gate = gate + jnp.dot(normed[:, rows], wg_ref[rows], preferred_element_type=jnp.float32)
        raise_ = raise_ + jnp.dot(normed[:, rows], wu_ref[rows], preferred_element_type=jnp.float32)
    active = (gate * jax.nn.sigmoid(gate) * raise_).astype(jnp.bfloat16)

    wait([out_weight])
    product = jnp.dot(wide, wo_ref[...], preferred_element_type=jnp.float32)
    sums = jnp.concatenate([jnp.sum(product[heads * r:heads * (r + 1)], axis=0, keepdims=True) for r in range(n_rows)], axis=0)
    total = jnp.zeros((PAD, model), jnp.float32)
    for copy, (first, size) in zip(down_copies, down_cuts):
        copy.wait()
        total = total + jnp.dot(active[:, first:first + size], wd_ref[first:first + size], preferred_element_type=jnp.float32)
    out_ref[...] = sums + total[:n_rows]
    wait(out_copies)


def layer_call(layer, sliding, info, h, gain, tables, w_query, wk_t, wv_t, w_out, w_gate, w_up, w_down, k_t, v_t, partner, far, held):
    n_rows, model = h.shape
    q_width = w_query.shape[2]
    dim = wk_t.shape[1]
    hidden = w_gate.shape[2]
    half_len = k_t.shape[-1]
    in_vmem = pl.BlockSpec(memory_space=pltpu.VMEM)
    anywhere = pl.BlockSpec(memory_space=pl.ANY)
    total = (2 if sliding else 4) * half_len
    kept = (3, n_rows, dim, total) if sliding else (n_rows, dim, total)
    kept_shape = jax.ShapeDtypeStruct(kept, k_t.dtype)
    args = [info, h, gain, *tables, w_query, wk_t, wv_t, w_gate, w_up, w_down, w_out, k_t, v_t, partner, *far]
    in_specs = [pl.BlockSpec(memory_space=pltpu.SMEM)] + [in_vmem] * 6 + [anywhere] * (10 + len(far))
    aliases = {}
    if held is not None:
        for place, array in enumerate(held):
            aliases[len(args)] = 1 + place
            in_specs.append(anywhere)
            args.append(array)
    weight_bytes = 2 * (2 * model * q_width + 2 * dim * model + 3 * model * hidden)
    units = (2, 2, MAX_UNITS, dim, LANES) if sliding else (8, LANES)
    n_weight = 4 + 2 * K_STEPS + -(-hidden // DOWN_ROWS)
    return pl.pallas_call(
        functools.partial(layer_kernel, layer, sliding, len(far)),
        in_specs=in_specs, out_specs=(in_vmem, anywhere, anywhere),
        scratch_shapes=[
            pltpu.VMEM((model, q_width), jnp.bfloat16),
            pltpu.VMEM((dim, model), jnp.bfloat16),
            pltpu.VMEM((dim, model), jnp.bfloat16),
            pltpu.VMEM((model, hidden), jnp.bfloat16),
            pltpu.VMEM((model, hidden), jnp.bfloat16),
            pltpu.VMEM((hidden, model), jnp.bfloat16),
            pltpu.VMEM((q_width, model), jnp.bfloat16),
            pltpu.VMEM((n_rows, dim, total), jnp.bfloat16),
            pltpu.VMEM((n_rows, dim, total), jnp.bfloat16),
            pltpu.VMEM(units, jnp.bfloat16),
            pltpu.SemaphoreType.DMA((n_weight,)),
            pltpu.SemaphoreType.DMA((12,)),
            pltpu.SemaphoreType.DMA((2,)),
        ],
        out_shape=(jax.ShapeDtypeStruct((n_rows, model), jnp.float32), kept_shape, kept_shape),
        input_output_aliases=aliases,
        compiler_params=pltpu.CompilerParams(vmem_limit_bytes=VMEM_GRANT),
        cost_estimate=pl.CostEstimate(flops=PAD * weight_bytes, bytes_accessed=weight_bytes, transcendentals=0),
        name="layer_%d" % layer,
    )(*args)


def rotary_tables(positions, dim, heads):
    half = dim // 2
    inv_freq = 1.0 / (ROPE_BASE ** (jnp.arange(half, dtype=jnp.float32) * 2.0 / dim))
    angles = positions.astype(jnp.float32)[:, None] * inv_freq[None, :]
    cosine = jnp.cos(angles)
    sine = jnp.sin(angles)
    n_rows = positions.shape[0]
    cq = jnp.pad(jnp.tile(jnp.concatenate([cosine, cosine], axis=1), (1, heads)), ((0, 8 - n_rows), (0, 0)))
    sq = jnp.pad(jnp.tile(jnp.concatenate([-sine, sine], axis=1), (1, heads)), ((0, 8 - n_rows), (0, 0)))
    ck = jnp.pad(cosine.T, ((0, 0), (0, PAD - n_rows)))
    sk = jnp.pad(sine.T, ((0, 0), (0, PAD - n_rows)))
    return cq, sq, ck, sk


def sum_kernel(n_tp, part_ref, resid_ref, out_ref, slots, send_sem, recv_sem):
    me = lax.axis_index("tp")
    barrier = pltpu.get_barrier_semaphore()
    for flip in range(1, n_tp):
        pl.semaphore_signal(barrier, inc=1, device_id={"tp": me ^ flip}, device_id_type=MESH_ID)
    pl.semaphore_wait(barrier, n_tp - 1)
    copies = []
    for flip in range(1, n_tp):
        copy = pltpu.make_async_remote_copy(
            src_ref=part_ref, dst_ref=slots.at[me], send_sem=send_sem.at[flip - 1], recv_sem=recv_sem.at[flip - 1],
            device_id={"tp": me ^ flip}, device_id_type=MESH_ID)
        copy.start()
        copies.append(copy)
    slots[me] = part_ref[...]
    for copy in copies:
        copy.wait()
    total = slots[0]
    for index in range(1, n_tp):
        total = total + slots[index]
    out_ref[...] = (resid_ref[...] + total).astype(jnp.bfloat16).astype(jnp.float32)


def sum_call(part, resid, n_tp):
    return pl.pallas_call(
        functools.partial(sum_kernel, n_tp),
        out_shape=jax.ShapeDtypeStruct(part.shape, jnp.float32),
        in_specs=[pl.BlockSpec(memory_space=pltpu.VMEM)] * 2,
        out_specs=pl.BlockSpec(memory_space=pltpu.VMEM),
        scratch_shapes=[
            pltpu.VMEM((n_tp,) + part.shape, jnp.float32),
            pltpu.SemaphoreType.DMA((n_tp - 1,)),
            pltpu.SemaphoreType.DMA((n_tp - 1,)),
        ],
        compiler_params=pltpu.CompilerParams(collective_id=0, has_side_effects=True),
        name="sum_tp",
    )(part, resid)


LANES = 128
HALF_UNITS = 16
CHIP_ROWS = 4
MAX_UNITS = CHIP_ROWS * HALF_UNITS
HEAVY_LEVELS = (32, 40, 44, 48, 52, 56, 60, 64)
LIGHT_LEVELS = (8, 16, 20, 24, 28, 32, 36, 40, 44, 48, 56, 64)


def unit_table(offsets):
    half = jnp.arange(2, dtype=jnp.int32)[None, :] * HALF_UNITS
    edge = offsets[:, None]
    upper_end = jnp.clip((edge + LANES - 1) // LANES, half, half + HALF_UNITS)
    lower_start = jnp.clip((edge + 1) // LANES, half, half + HALF_UNITS)
    from_upper = jnp.arange(offsets.shape[0], dtype=jnp.int32)[:, None] < CHIP_ROWS
    start = jnp.where(from_upper, half, lower_start)
    count = jnp.where(from_upper, upper_end - half, half + HALF_UNITS - lower_start)
    by_chip = count.reshape(2, CHIP_ROWS, 2)
    ends = jnp.cumsum(by_chip, axis=1)
    base = (ends - by_chip).reshape(count.shape)
    return start, count, base, ends[:, -1]


def pack_kernel(info_ref, k_ref, v_ref, out_ref):
    for row in range(CHIP_ROWS):
        first = info_ref[1 + 3 * row]
        count = info_ref[2 + 3 * row]
        base = info_ref[3 + 3 * row]
        for unit in range(HALF_UNITS):
            @pl.when(jnp.logical_and(unit >= first, unit < first + count))
            def _():
                place = base + unit - first
                cols = pl.ds(unit * LANES, LANES)
                out_ref[0, 0, place] = k_ref[0, row, :, cols]
                out_ref[0, 1, place] = v_ref[0, row, :, cols]


def pack_call(info, k_t, v_t, n_layers):
    dim, half_len = k_t.shape[2:]
    block = pl.BlockSpec((1, CHIP_ROWS, dim, half_len), lambda l, info: (l, info[0], 0, 0))
    return pl.pallas_call(
        pack_kernel,
        grid_spec=pltpu.PrefetchScalarGridSpec(
            num_scalar_prefetch=1, grid=(n_layers,), in_specs=[block, block],
            out_specs=pl.BlockSpec((1, 2, MAX_UNITS, dim, LANES), lambda l, info: (l, 0, 0, 0, 0))),
        out_shape=jax.ShapeDtypeStruct((n_layers, 2, MAX_UNITS, dim, LANES), k_t.dtype),
        compiler_params=pltpu.CompilerParams(dimension_semantics=("arbitrary",), vmem_limit_bytes=VMEM_GRANT),
        name="pack_units",
    )(info, k_t, v_t)


def send_kernel(heavy, n_units, packed_ref, k_ref, v_ref, *rest):
    if heavy:
        got_ref, partner_ref, send_sem, recv_sem, fsend_sem, frecv_sem, psend_sem, precv_sem = rest
        phase = 0
    else:
        _, got_ref, send_sem, recv_sem, fsend_sem, frecv_sem = rest
        phase = 1
    me = lax.axis_index("sp")
    middle = jnp.logical_or(me == 1, me == 2)
    sender = middle if heavy else jnp.logical_not(middle)
    across = (me + 2) % 4
    partner = me + 1 - 2 * (me % 2)
    n_layers = packed_ref.shape[0]
    barrier = pltpu.get_barrier_semaphore()
    for peer in (across, partner):
        pl.semaphore_signal(barrier, inc=1, device_id={"sp": peer}, device_id_type=MESH_ID)
    pl.semaphore_wait(barrier, 2)
    direct = []
    onward = []
    for layer in range(n_layers):
        for kind in range(2):
            index = layer * 2 + kind
            part = pl.ds(0, n_units)
            target = got_ref.at[phase, layer, kind, part]
            direct.append(pltpu.make_async_remote_copy(
                src_ref=packed_ref.at[layer, kind, part], dst_ref=target, send_sem=send_sem.at[index], recv_sem=recv_sem.at[index],
                device_id={"sp": across}, device_id_type=MESH_ID))
            onward.append(pltpu.make_async_remote_copy(
                src_ref=target, dst_ref=target, send_sem=fsend_sem.at[index], recv_sem=frecv_sem.at[index],
                device_id={"sp": partner}, device_id_type=MESH_ID))

    @pl.when(sender)
    def _():
        for copy in direct:
            copy.start()

    shares = []
    if heavy:
        rows = partner_ref.shape[2]
        for kind, source in enumerate((k_ref, v_ref)):
            for layer in range(source.shape[0]):
                index = layer * 2 + kind
                shares.append(pltpu.make_async_remote_copy(
                    src_ref=source.at[layer, pl.ds(rows * partner, rows)], dst_ref=partner_ref.at[kind, layer],
                    send_sem=psend_sem.at[index], recv_sem=precv_sem.at[index],
                    device_id={"sp": partner}, device_id_type=MESH_ID))
        for copy in shares:
            copy.start()

    @pl.when(jnp.logical_not(sender))
    def _():
        for near, far in zip(direct, onward):
            near.wait_recv()
            far.start()
        for far in onward:
            far.wait_send()

    @pl.when(sender)
    def _():
        for near, far in zip(direct, onward):
            near.wait_send()
            far.wait_recv()

    for copy in shares:
        copy.wait()


def send_call(heavy, n_units, slot, packed, k_t, v_t, got=None):
    n_layers = packed.shape[0]
    n_copies = 2 * n_layers
    anywhere = pl.BlockSpec(memory_space=pl.ANY)
    got_shape = jax.ShapeDtypeStruct((2,) + packed.shape, packed.dtype)
    sems = [pltpu.SemaphoreType.DMA((n_copies,)) for _ in range(4)]
    if heavy:
        args = (packed, k_t, v_t)
        rows = k_t.shape[1] // 4
        out_shape = (got_shape, jax.ShapeDtypeStruct((2, k_t.shape[0], rows) + k_t.shape[2:], k_t.dtype))
        sems += [pltpu.SemaphoreType.DMA((2 * k_t.shape[0],)) for _ in range(2)]
        aliases = {}
        out_specs = (anywhere, anywhere)
    else:
        args = (packed, k_t, v_t, got)
        out_shape = got_shape
        aliases = {3: 0}
        out_specs = anywhere
    return pl.pallas_call(
        functools.partial(send_kernel, heavy, n_units),
        out_shape=out_shape, in_specs=[anywhere] * len(args), out_specs=out_specs, scratch_shapes=sems,
        input_output_aliases=aliases,
        compiler_params=pltpu.CompilerParams(collective_id=slot, has_side_effects=True),
        name="send_%s_%d" % ("heavy" if heavy else "light", n_units),
    )(*args)


def solution(mesh):
    cache_spec = P(None, "dp", "tp", "sp", None)
    row_spec = P(("dp", "sp"), None)
    col_spec = P(None, None, "tp")
    inner_spec = P(None, "tp", None)
    window_spec = P(None, ("dp", "sp"), "tp", None, None)
    global_spec = P(("dp", "sp"), "tp", None, None)
    in_specs = (cache_spec, cache_spec, P("dp"), row_spec, P(None, None), col_spec, col_spec, col_spec, inner_spec, col_spec, col_spec, inner_spec)
    out_specs = (row_spec, window_spec, window_spec, global_spec, global_spec)

    def device_step(k_cache, v_cache, lengths, hidden, ln_gain, w_query, w_key, w_value, w_out, w_gate, w_up, w_down):
        n_layers = w_query.shape[0]
        rows_dev = hidden.shape[0]
        head_dim = k_cache.shape[-1]
        n_tp = mesh.shape["tp"]
        me = lax.axis_index("sp")
        core = me % 2
        chip = me // 2
        my_lengths = lax.dynamic_slice_in_dim(lengths, me * rows_dev, rows_dev)
        k_t = k_cache[:, :, 0].swapaxes(-1, -2)
        v_t = v_cache[:, :, 0].swapaxes(-1, -2)
        start, count, base, totals = unit_table(lengths - WINDOW)
        other_lengths = lax.ppermute(lengths, "dp", [(0, 1), (1, 0)])
        other_totals = unit_table(other_lengths - WINDOW)[3]
        most = jnp.maximum(totals, other_totals)
        heavy_need = jnp.maximum(most[0, 0], most[1, 1])
        light_need = jnp.maximum(most[0, 1], most[1, 0])
        heavy_index = jnp.sum(heavy_need > jnp.array(HEAVY_LEVELS, jnp.int32)).astype(jnp.int32)
        light_index = jnp.sum(light_need > jnp.array(LIGHT_LEVELS, jnp.int32)).astype(jnp.int32)

        table = jnp.stack([start, count, base], axis=-1)
        sent = lax.dynamic_slice(table, ((1 - chip) * CHIP_ROWS, core, 0), (CHIP_ROWS, 1, 3))[:, 0]
        sent = sent - jnp.array([1, 0, 0], jnp.int32) * (core * HALF_UNITS)
        pack_info = jnp.concatenate([(1 - chip)[None], sent.reshape(-1)]).astype(jnp.int32)
        mine = lax.dynamic_slice_in_dim(table, me * rows_dev, rows_dev)
        window_info = jnp.concatenate([
            jnp.stack([core, chip, me * rows_dev, me]), my_lengths - WINDOW, jnp.stack([chip, 1 - chip]),
            mine[:, :, 0].reshape(-1), mine[:, :, 1].reshape(-1), mine[:, :, 2].reshape(-1)]).astype(jnp.int32)
        global_info = jnp.concatenate([jnp.stack([core, chip, me * rows_dev, me]), my_lengths]).astype(jnp.int32)

        packed = pack_call(pack_info, k_t, v_t, n_layers - 1)
        heavy_calls = [functools.partial(send_call, True, n, 1 + i) for i, n in enumerate(HEAVY_LEVELS)]
        light_calls = [functools.partial(send_call, False, n, 1 + len(HEAVY_LEVELS) + i) for i, n in enumerate(LIGHT_LEVELS)]
        got, partner = lax.switch(heavy_index, heavy_calls, packed, k_t, v_t)
        got = lax.switch(light_index, light_calls, packed, k_t, v_t, got)

        got, after = lax.optimization_barrier((got, me))
        far = []
        for flip in (2, 3):
            first = (after ^ flip) * rows_dev
            rows = jnp.concatenate([
                lax.dynamic_slice(part, (n_layers - 1, first, 0, 0), (1, rows_dev) + part.shape[2:]) for part in (k_t, v_t)])
            far.append(lax.ppermute(rows, "sp", [(i, i ^ flip) for i in range(4)]))

        residual = hidden.astype(jnp.float32)
        tables = rotary_tables(my_lengths, head_dim, w_query.shape[2] // head_dim)
        wk_t = w_key.swapaxes(1, 2)
        wv_t = w_value.swapaxes(1, 2)
        held = None
        for layer in range(n_layers):
            sliding = layer < n_layers - 1
            common = (residual, ln_gain[layer:layer + 1], tables, w_query, wk_t, wv_t, w_out, w_gate, w_up, w_down, k_t, v_t, partner)
            if sliding:
                part, *held = layer_call(layer, True, window_info, *common, [got], held)
            else:
                part, *kept = layer_call(layer, False, global_info, *common, far, None)
            residual = sum_call(part, residual, n_tp)

        def back(rows_t):
            return rows_t.swapaxes(-1, -2)

        return (residual.astype(jnp.bfloat16), back(held[0])[:, :, None], back(held[1])[:, :, None],
                back(kept[0])[:, None], back(kept[1])[:, None])

    return jax.shard_map(device_step, mesh=mesh, in_specs=in_specs, out_specs=out_specs, check_vma=False)
```

```python
import functools

import jax
import jax.numpy as jnp
from jax import lax
from jax.experimental import pallas as pl
from jax.experimental.pallas import tpu as pltpu
from jax.sharding import PartitionSpec as P

WINDOW = 4096
ROPE_BASE = 50000
NORM_EPS = 1e-5


PAD = 16
K_STEPS = 4
DOWN_ROWS = 384
MESH_ID = pl.DeviceIdType.MESH


VMEM_GRANT = 58 * 2 ** 20


def layer_kernel(layer, sliding, n_far, n_tp, info_ref, h_ref, gain_ref, cq_ref, sq_ref, ck_ref, sk_ref, *refs):
    wq_hbm, wk_hbm, wv_hbm, wg_hbm, wu_hbm, wd_hbm, wo_hbm, k_hbm, v_hbm, partner_hbm = refs[:10]
    far = refs[10:10 + n_far]
    fused = n_tp > 0
    if fused:
        part_ref = refs[10 + n_far]
        (out_ref, h_out, keys_hbm, values_hbm, wq_ref, wk_ref, wv_ref, wg_ref, wu_ref, wd_ref, wo_ref, keys_ref, values_ref, units_ref,
         weight_sem, in_sem, out_sem, slots, send_sem, recv_sem) = refs[-20:]
    else:
        (out_ref, keys_hbm, values_hbm, wq_ref, wk_ref, wv_ref, wg_ref, wu_ref, wd_ref, wo_ref, keys_ref, values_ref, units_ref,
         weight_sem, in_sem, out_sem) = refs[-16:]
    n_rows, model = h_ref.shape
    dim = wk_ref.shape[0]
    q_width = wq_ref.shape[1]
    hidden = wg_ref.shape[1]
    heads = q_width // dim
    half_len = k_hbm.shape[-1]
    me = lax.axis_index("sp")
    chip = me // 2
    first_row = me * n_rows
    buffers = (keys_ref, values_ref)

    def cache_copies(index):
        found = []
        pieces = 2 if sliding else 4
        for kind, (source, buffer) in enumerate(zip((k_hbm, v_hbm), buffers)):
            for piece in range(pieces):
                place = pl.ds(piece * half_len, half_len)
                who = piece ^ (index % 2) if sliding else piece ^ index
                if who == 0:
                    origin = source.at[layer, pl.ds(first_row, n_rows)]
                elif who == 1:
                    origin = partner_hbm.at[kind, layer]
                else:
                    origin = far[who - 2].at[kind]
                found.append(pltpu.make_async_copy(origin, buffer.at[:, :, place], in_sem.at[kind * 4 + piece]))
        return found

    variants = 2 if sliding else 4
    which = me % variants

    def each_variant(act):
        for index in range(variants):
            @pl.when(which == index)
            def _():
                for copy in cache_copies(index):
                    act(copy)

    unit_copies = []
    if sliding:
        for half in range(2):
            for kind in range(2):
                unit_copies.append(pltpu.make_async_copy(
                    far[0].at[(chip + half) % 2, layer, kind], units_ref.at[half, kind], in_sem.at[8 + half * 2 + kind]))

    n_sem = [0]

    def weight_copy(source, target, first, size):
        rows = pl.ds(first, size)
        copy = pltpu.make_async_copy(source.at[layer, rows], target.at[rows], weight_sem.at[n_sem[0]])
        n_sem[0] += 1
        return copy

    k_len = model // K_STEPS
    down_cuts = [(first, min(DOWN_ROWS, hidden - first)) for first in range(0, hidden, DOWN_ROWS)]
    proj_copies = [weight_copy(wq_hbm, wq_ref, 0, model), weight_copy(wk_hbm, wk_ref, 0, dim), weight_copy(wv_hbm, wv_ref, 0, dim)]
    up_copies = [[weight_copy(wg_hbm, wg_ref, part * k_len, k_len), weight_copy(wu_hbm, wu_ref, part * k_len, k_len)] for part in range(K_STEPS)]
    out_weight = weight_copy(wo_hbm, wo_ref, 0, q_width)
    down_copies = [weight_copy(wd_hbm, wd_ref, first, size) for first, size in down_cuts]

    def start(copies):
        for copy in copies:
            copy.start()

    def wait(copies):
        for copy in copies:
            copy.wait()

    lane = lax.broadcasted_iota(jnp.int32, (dim, LANES), 1)
    if fused:
        here = lax.axis_index("tp")
        barrier = pltpu.get_barrier_semaphore()
        for flip in range(1, n_tp):
            pl.semaphore_signal(barrier, inc=1, device_id={"tp": here ^ flip}, device_id_type=MESH_ID)
    start(proj_copies)
    each_variant(lambda copy: copy.start())
    start(unit_copies)
    for copies in up_copies[:2]:
        start(copies)
    if fused:
        for copies in up_copies[2:]:
            start(copies)
        start([out_weight])
        start(down_copies)
        pl.semaphore_wait(barrier, n_tp - 1)
        shares = []
        for flip in range(1, n_tp):
            shares.append(pltpu.make_async_remote_copy(
                src_ref=part_ref, dst_ref=slots.at[here], send_sem=send_sem.at[flip - 1], recv_sem=recv_sem.at[flip - 1],
                device_id={"tp": here ^ flip}, device_id_type=MESH_ID))
        start(shares)
        slots[here] = part_ref[...]
        each_variant(lambda copy: copy.wait())
        wait(unit_copies)
        for row in range(n_rows):
            edge = info_ref[4 + row]
            for unit in range(keys_ref.shape[-1] // LANES):
                slot = lane + unit * LANES
                cols = slice(unit * LANES, (unit + 1) * LANES)
                half = unit // HALF_UNITS
                if sliding:
                    keep = jnp.logical_xor(slot < edge, chip == 0)
                    place = jnp.clip(info_ref[16 + 2 * row + half] + unit - info_ref[8 + 2 * row + half], 0, MAX_UNITS - 1)
                elif unit < 2 * HALF_UNITS:
                    continue
                else:
                    keep = slot < edge
                for kind, buffer in enumerate(buffers):
                    remote = units_ref[half, kind, place] if sliding else jnp.zeros((dim, LANES), buffer.dtype)
                    buffer[row, :, cols] = jnp.where(keep, buffer[row, :, cols], remote)
        wait(shares)
        total = slots[0]
        for index in range(1, n_tp):
            total = total + slots[index]
        rows32 = (h_ref[...] + total).astype(jnp.bfloat16).astype(jnp.float32)
        h_out[...] = rows32
    else:
        rows32 = h_ref[...]
    centered = rows32 - jnp.mean(rows32, axis=-1, keepdims=True)
    variance = jnp.mean(centered * centered, axis=-1, keepdims=True)
    scaled = centered * lax.rsqrt(variance + NORM_EPS)
    normed = scaled * gain_ref[...].astype(jnp.float32)
    normed = jnp.concatenate([normed, jnp.zeros((PAD - n_rows, model), jnp.float32)], axis=0).astype(jnp.bfloat16)

    nt = (((1,), (1,)), ((), ()))
    wait(proj_copies)
    query = jnp.dot(normed, wq_ref[...], preferred_element_type=jnp.float32)[:8]
    k_new = lax.dot_general(wk_ref[...], normed, nt, preferred_element_type=jnp.float32)
    v_new = lax.dot_general(wv_ref[...], normed, nt, preferred_element_type=jnp.float32)
    if sliding:
        q_lane = lax.broadcasted_iota(jnp.int32, query.shape, 1)
        swapped = jnp.where(q_lane % dim < dim // 2, pltpu.roll(query, q_width - dim // 2, 1), pltpu.roll(query, dim // 2, 1))
        query = query * cq_ref[...] + swapped * sq_ref[...]
        first = k_new[:dim // 2]
        second = k_new[dim // 2:]
        cosine = ck_ref[...]
        sine = sk_ref[...]
        k_new = jnp.concatenate([first * cosine - second * sine, second * cosine + first * sine], axis=0)
    k_new = k_new.astype(jnp.bfloat16).astype(jnp.float32)
    v_new = v_new.astype(jnp.bfloat16).astype(jnp.float32)
    spread = [jnp.broadcast_to(query[r:r + 1], (heads, q_width)) for r in range(n_rows)]
    spread = jnp.concatenate(spread, axis=0)
    at_row = lax.broadcasted_iota(jnp.int32, spread.shape, 0)
    at_col = lax.broadcasted_iota(jnp.int32, spread.shape, 1)
    own_head = at_col // dim == at_row % heads
    masked = jnp.where(own_head, spread, 0.0).astype(jnp.bfloat16)
    pick_row = lax.broadcasted_iota(jnp.int32, (dim, q_width), 0)
    pick_col = lax.broadcasted_iota(jnp.int32, (dim, q_width), 1)
    pick = jnp.where(pick_col % dim == pick_row, 1.0, 0.0).astype(jnp.bfloat16)
    head_q = lax.dot_general(masked, pick, nt, preferred_element_type=jnp.float32).astype(jnp.bfloat16)

    column = lax.broadcasted_iota(jnp.int32, (dim, PAD), 1)
    if fused:
        for row in range(n_rows):
            edge = info_ref[4 + row]
            for buffer, new in zip(buffers, (k_new, v_new)):
                picked = jnp.sum(jnp.where(column == row, new, 0.0), axis=1, keepdims=True)
                tile = jnp.broadcast_to(picked, (dim, LANES)).astype(buffer.dtype)
                for unit in range(keys_ref.shape[-1] // LANES):
                    if not sliding and unit < 2 * HALF_UNITS:
                        continue
                    cols = slice(unit * LANES, (unit + 1) * LANES)
                    buffer[row, :, cols] = jnp.where(lane + unit * LANES == edge, tile, buffer[row, :, cols])
    else:
        start(up_copies[2])
        each_variant(lambda copy: copy.wait())
        wait(unit_copies)
        for row in range(n_rows):
            edge = info_ref[4 + row]
            border = edge // LANES
            cols = pl.ds(pl.multiple_of(border * LANES, LANES), LANES)
            slot = lane + border * LANES
            before = [buffer[row, :, cols] for buffer in buffers]
            if sliding:
                for half in range(2):
                    begin = info_ref[8 + 2 * row + half]
                    count = info_ref[12 + 2 * row + half]
                    base = info_ref[16 + 2 * row + half]

                    def place_unit(unit, carry, half=half, begin=begin, base=base):
                        to = pl.ds(pl.multiple_of(unit * LANES, LANES), LANES)
                        for kind, buffer in enumerate(buffers):
                            buffer[row, :, to] = units_ref[half, kind, base + unit - begin]
                        return carry

                    lax.fori_loop(begin, begin + count, place_unit, 0)
                border_half = border // HALF_UNITS
                border_place = jnp.clip(info_ref[16 + 2 * row + border_half] + border - info_ref[8 + 2 * row + border_half], 0, MAX_UNITS - 1)
                keep = jnp.logical_xor(slot < edge, chip == 0)
            else:
                def clear_unit(unit, carry):
                    to = pl.ds(pl.multiple_of(unit * LANES, LANES), LANES)
                    for buffer in buffers:
                        buffer[row, :, to] = jnp.zeros((dim, LANES), buffer.dtype)
                    return carry

                lax.fori_loop(border + 1, 4 * HALF_UNITS, clear_unit, 0)
                keep = slot < edge
            for kind, (buffer, new) in enumerate(zip(buffers, (k_new, v_new))):
                picked = jnp.sum(jnp.where(column == row, new, 0.0), axis=1, keepdims=True)
                if sliding:
                    remote = units_ref[border_half, kind, border_place].astype(jnp.float32)
                else:
                    remote = jnp.zeros((dim, LANES), jnp.float32)
                merged = jnp.where(keep, before[kind].astype(jnp.float32), remote)
                merged = jnp.where(slot == edge, jnp.broadcast_to(picked, (dim, LANES)), merged)
                buffer[row, :, cols] = merged.astype(buffer.dtype)
        start(up_copies[3])
    out_copies = []
    for kind, (buffer, kept) in enumerate(zip(buffers, (keys_hbm, values_hbm))):
        target = kept.at[layer] if sliding else kept
        out_copies.append(pltpu.make_async_copy(buffer, target, out_sem.at[kind]))
    start(out_copies)
    mixed = []
    for row in range(n_rows):
        edge = info_ref[4 + row]
        scores = jnp.dot(head_q[heads * row:heads * (row + 1)], keys_ref[row], preferred_element_type=jnp.float32) * dim ** -0.5
        if not sliding:
            position = lax.broadcasted_iota(jnp.int32, scores.shape, 1)
            scores = jnp.where(position <= edge, scores, -1e30)
        top = jnp.max(scores, axis=-1, keepdims=True)
        raised = jnp.exp(scores - top)
        weights = (raised / jnp.sum(raised, axis=-1, keepdims=True)).astype(jnp.bfloat16)
        mixed.append(lax.dot_general(weights, values_ref[row], nt, preferred_element_type=jnp.float32))
    both = jnp.concatenate(mixed, axis=0).astype(jnp.bfloat16)
    wide = jnp.dot(both, pick, preferred_element_type=jnp.float32)
    wide = jnp.where(own_head, wide, 0.0).astype(jnp.bfloat16)

    if not fused:
        start([out_weight])
        start(down_copies)
    gate = jnp.zeros((PAD, hidden), jnp.float32)
    raise_ = jnp.zeros((PAD, hidden), jnp.float32)
    for part in range(K_STEPS):
        wait(up_copies[part])
        rows = slice(part * k_len, (part + 1) * k_len)
        gate = gate + jnp.dot(normed[:, rows], wg_ref[rows], preferred_element_type=jnp.float32)
        raise_ = raise_ + jnp.dot(normed[:, rows], wu_ref[rows], preferred_element_type=jnp.float32)
    active = (gate * jax.nn.sigmoid(gate) * raise_).astype(jnp.bfloat16)

    wait([out_weight])
    product = jnp.dot(wide, wo_ref[...], preferred_element_type=jnp.float32)
    sums = jnp.concatenate([jnp.sum(product[heads * r:heads * (r + 1)], axis=0, keepdims=True) for r in range(n_rows)], axis=0)
    total = jnp.zeros((PAD, model), jnp.float32)
    for copy, (first, size) in zip(down_copies, down_cuts):
        copy.wait()
        total = total + jnp.dot(active[:, first:first + size], wd_ref[first:first + size], preferred_element_type=jnp.float32)
    out_ref[...] = sums + total[:n_rows]
    wait(out_copies)


def layer_call(layer, sliding, info, h, gain, tables, w_query, wk_t, wv_t, w_out, w_gate, w_up, w_down, k_t, v_t, partner, far, held, part=None, n_tp=0):
    n_rows, model = h.shape
    q_width = w_query.shape[2]
    dim = wk_t.shape[1]
    hidden = w_gate.shape[2]
    half_len = k_t.shape[-1]
    in_vmem = pl.BlockSpec(memory_space=pltpu.VMEM)
    anywhere = pl.BlockSpec(memory_space=pl.ANY)
    total = (2 if sliding else 4) * half_len
    kept = (3, n_rows, dim, total) if sliding else (n_rows, dim, total)
    kept_shape = jax.ShapeDtypeStruct(kept, k_t.dtype)
    args = [info, h, gain, *tables, w_query, wk_t, wv_t, w_gate, w_up, w_down, w_out, k_t, v_t, partner, *far]
    in_specs = [pl.BlockSpec(memory_space=pltpu.SMEM)] + [in_vmem] * 6 + [anywhere] * (10 + len(far))
    fused = part is not None
    if fused:
        args.append(part)
        in_specs.append(in_vmem)
    aliases = {}
    n_small = 2 if fused else 1
    if held is not None:
        for place, array in enumerate(held):
            aliases[len(args)] = n_small + place
            in_specs.append(anywhere)
            args.append(array)
    weight_bytes = 2 * (2 * model * q_width + 2 * dim * model + 3 * model * hidden)
    units = (2, 2, MAX_UNITS, dim, LANES) if sliding else (8, LANES)
    n_weight = 4 + 2 * K_STEPS + -(-hidden // DOWN_ROWS)
    row_shape = jax.ShapeDtypeStruct((n_rows, model), jnp.float32)
    if fused:
        remote = [pltpu.VMEM((n_tp, n_rows, model), jnp.float32), pltpu.SemaphoreType.DMA((n_tp - 1,)), pltpu.SemaphoreType.DMA((n_tp - 1,))]
        params = pltpu.CompilerParams(vmem_limit_bytes=VMEM_GRANT, collective_id=40 + layer, has_side_effects=True)
    else:
        remote = []
        params = pltpu.CompilerParams(vmem_limit_bytes=VMEM_GRANT)
    return pl.pallas_call(
        functools.partial(layer_kernel, layer, sliding, len(far), n_tp if fused else 0),
        in_specs=in_specs, out_specs=(in_vmem,) * n_small + (anywhere, anywhere),
        scratch_shapes=[
            pltpu.VMEM((model, q_width), jnp.bfloat16),
            pltpu.VMEM((dim, model), jnp.bfloat16),
            pltpu.VMEM((dim, model), jnp.bfloat16),
            pltpu.VMEM((model, hidden), jnp.bfloat16),
            pltpu.VMEM((model, hidden), jnp.bfloat16),
            pltpu.VMEM((hidden, model), jnp.bfloat16),
            pltpu.VMEM((q_width, model), jnp.bfloat16),
            pltpu.VMEM((n_rows, dim, total), jnp.bfloat16),
            pltpu.VMEM((n_rows, dim, total), jnp.bfloat16),
            pltpu.VMEM(units, jnp.bfloat16),
            pltpu.SemaphoreType.DMA((n_weight,)),
            pltpu.SemaphoreType.DMA((12,)),
            pltpu.SemaphoreType.DMA((2,)),
        ] + remote,
        out_shape=(row_shape,) * n_small + (kept_shape, kept_shape),
        input_output_aliases=aliases,
        compiler_params=params,
        cost_estimate=pl.CostEstimate(flops=PAD * weight_bytes, bytes_accessed=weight_bytes, transcendentals=0),
        name="layer_%d" % layer,
    )(*args)


def rotary_tables(positions, dim, heads):
    half = dim // 2
    inv_freq = 1.0 / (ROPE_BASE ** (jnp.arange(half, dtype=jnp.float32) * 2.0 / dim))
    angles = positions.astype(jnp.float32)[:, None] * inv_freq[None, :]
    cosine = jnp.cos(angles)
    sine = jnp.sin(angles)
    n_rows = positions.shape[0]
    cq = jnp.pad(jnp.tile(jnp.concatenate([cosine, cosine], axis=1), (1, heads)), ((0, 8 - n_rows), (0, 0)))
    sq = jnp.pad(jnp.tile(jnp.concatenate([-sine, sine], axis=1), (1, heads)), ((0, 8 - n_rows), (0, 0)))
    ck = jnp.pad(cosine.T, ((0, 0), (0, PAD - n_rows)))
    sk = jnp.pad(sine.T, ((0, 0), (0, PAD - n_rows)))
    return cq, sq, ck, sk


def sum_kernel(n_tp, part_ref, resid_ref, out_ref, slots, send_sem, recv_sem):
    me = lax.axis_index("tp")
    barrier = pltpu.get_barrier_semaphore()
    for flip in range(1, n_tp):
        pl.semaphore_signal(barrier, inc=1, device_id={"tp": me ^ flip}, device_id_type=MESH_ID)
    pl.semaphore_wait(barrier, n_tp - 1)
    copies = []
    for flip in range(1, n_tp):
        copy = pltpu.make_async_remote_copy(
            src_ref=part_ref, dst_ref=slots.at[me], send_sem=send_sem.at[flip - 1], recv_sem=recv_sem.at[flip - 1],
            device_id={"tp": me ^ flip}, device_id_type=MESH_ID)
        copy.start()
        copies.append(copy)
    slots[me] = part_ref[...]
    for copy in copies:
        copy.wait()
    total = slots[0]
    for index in range(1, n_tp):
        total = total + slots[index]
    out_ref[...] = (resid_ref[...] + total).astype(jnp.bfloat16).astype(jnp.float32)


def sum_call(part, resid, n_tp):
    return pl.pallas_call(
        functools.partial(sum_kernel, n_tp),
        out_shape=jax.ShapeDtypeStruct(part.shape, jnp.float32),
        in_specs=[pl.BlockSpec(memory_space=pltpu.VMEM)] * 2,
        out_specs=pl.BlockSpec(memory_space=pltpu.VMEM),
        scratch_shapes=[
            pltpu.VMEM((n_tp,) + part.shape, jnp.float32),
            pltpu.SemaphoreType.DMA((n_tp - 1,)),
            pltpu.SemaphoreType.DMA((n_tp - 1,)),
        ],
        compiler_params=pltpu.CompilerParams(collective_id=0, has_side_effects=True),
        name="sum_tp",
    )(part, resid)


LANES = 128
HALF_UNITS = 16
CHIP_ROWS = 4
MAX_UNITS = CHIP_ROWS * HALF_UNITS
HEAVY_LEVELS = (32, 40, 44, 48, 52, 56, 60, 64)
LIGHT_LEVELS = (8, 16, 20, 24, 28, 32, 36, 40, 44, 48, 56, 64)


def unit_table(offsets):
    half = jnp.arange(2, dtype=jnp.int32)[None, :] * HALF_UNITS
    edge = offsets[:, None]
    upper_end = jnp.clip((edge + LANES - 1) // LANES, half, half + HALF_UNITS)
    lower_start = jnp.clip((edge + 1) // LANES, half, half + HALF_UNITS)
    from_upper = jnp.arange(offsets.shape[0], dtype=jnp.int32)[:, None] < CHIP_ROWS
    start = jnp.where(from_upper, half, lower_start)
    count = jnp.where(from_upper, upper_end - half, half + HALF_UNITS - lower_start)
    by_chip = count.reshape(2, CHIP_ROWS, 2)
    ends = jnp.cumsum(by_chip, axis=1)
    base = (ends - by_chip).reshape(count.shape)
    return start, count, base, ends[:, -1]


def pack_kernel(info_ref, k_ref, v_ref, out_ref):
    for row in range(CHIP_ROWS):
        first = info_ref[1 + 3 * row]
        count = info_ref[2 + 3 * row]
        base = info_ref[3 + 3 * row]
        for unit in range(HALF_UNITS):
            @pl.when(jnp.logical_and(unit >= first, unit < first + count))
            def _():
                place = base + unit - first
                cols = pl.ds(unit * LANES, LANES)
                out_ref[0, 0, place] = k_ref[0, row, :, cols]
                out_ref[0, 1, place] = v_ref[0, row, :, cols]


def pack_call(info, k_t, v_t, n_layers):
    dim, half_len = k_t.shape[2:]
    block = pl.BlockSpec((1, CHIP_ROWS, dim, half_len), lambda l, info: (l, info[0], 0, 0))
    return pl.pallas_call(
        pack_kernel,
        grid_spec=pltpu.PrefetchScalarGridSpec(
            num_scalar_prefetch=1, grid=(n_layers,), in_specs=[block, block],
            out_specs=pl.BlockSpec((1, 2, MAX_UNITS, dim, LANES), lambda l, info: (l, 0, 0, 0, 0))),
        out_shape=jax.ShapeDtypeStruct((n_layers, 2, MAX_UNITS, dim, LANES), k_t.dtype),
        compiler_params=pltpu.CompilerParams(dimension_semantics=("arbitrary",), vmem_limit_bytes=VMEM_GRANT),
        name="pack_units",
    )(info, k_t, v_t)


def send_kernel(heavy, n_units, packed_ref, k_ref, v_ref, *rest):
    if heavy:
        got_ref, partner_ref, send_sem, recv_sem, fsend_sem, frecv_sem, psend_sem, precv_sem = rest
        phase = 0
    else:
        _, got_ref, send_sem, recv_sem, fsend_sem, frecv_sem = rest
        phase = 1
    me = lax.axis_index("sp")
    middle = jnp.logical_or(me == 1, me == 2)
    sender = middle if heavy else jnp.logical_not(middle)
    across = (me + 2) % 4
    partner = me + 1 - 2 * (me % 2)
    n_layers = packed_ref.shape[0]
    barrier = pltpu.get_barrier_semaphore()
    for peer in (across, partner):
        pl.semaphore_signal(barrier, inc=1, device_id={"sp": peer}, device_id_type=MESH_ID)
    pl.semaphore_wait(barrier, 2)
    direct = []
    onward = []
    for layer in range(n_layers):
        for kind in range(2):
            index = layer * 2 + kind
            part = pl.ds(0, n_units)
            target = got_ref.at[phase, layer, kind, part]
            direct.append(pltpu.make_async_remote_copy(
                src_ref=packed_ref.at[layer, kind, part], dst_ref=target, send_sem=send_sem.at[index], recv_sem=recv_sem.at[index],
                device_id={"sp": across}, device_id_type=MESH_ID))
            onward.append(pltpu.make_async_remote_copy(
                src_ref=target, dst_ref=target, send_sem=fsend_sem.at[index], recv_sem=frecv_sem.at[index],
                device_id={"sp": partner}, device_id_type=MESH_ID))

    @pl.when(sender)
    def _():
        for copy in direct:
            copy.start()

    shares = []
    if heavy:
        rows = partner_ref.shape[2]
        for kind, source in enumerate((k_ref, v_ref)):
            for layer in range(source.shape[0]):
                index = layer * 2 + kind
                shares.append(pltpu.make_async_remote_copy(
                    src_ref=source.at[layer, pl.ds(rows * partner, rows)], dst_ref=partner_ref.at[kind, layer],
                    send_sem=psend_sem.at[index], recv_sem=precv_sem.at[index],
                    device_id={"sp": partner}, device_id_type=MESH_ID))
        for copy in shares:
            copy.start()

    @pl.when(jnp.logical_not(sender))
    def _():
        for near, far in zip(direct, onward):
            near.wait_recv()
            far.start()
        for far in onward:
            far.wait_send()

    @pl.when(sender)
    def _():
        for near, far in zip(direct, onward):
            near.wait_send()
            far.wait_recv()

    for copy in shares:
        copy.wait()


def send_call(heavy, n_units, slot, packed, k_t, v_t, got=None):
    n_layers = packed.shape[0]
    n_copies = 2 * n_layers
    anywhere = pl.BlockSpec(memory_space=pl.ANY)
    got_shape = jax.ShapeDtypeStruct((2,) + packed.shape, packed.dtype)
    sems = [pltpu.SemaphoreType.DMA((n_copies,)) for _ in range(4)]
    if heavy:
        args = (packed, k_t, v_t)
        rows = k_t.shape[1] // 4
        out_shape = (got_shape, jax.ShapeDtypeStruct((2, k_t.shape[0], rows) + k_t.shape[2:], k_t.dtype))
        sems += [pltpu.SemaphoreType.DMA((2 * k_t.shape[0],)) for _ in range(2)]
        aliases = {}
        out_specs = (anywhere, anywhere)
    else:
        args = (packed, k_t, v_t, got)
        out_shape = got_shape
        aliases = {3: 0}
        out_specs = anywhere
    return pl.pallas_call(
        functools.partial(send_kernel, heavy, n_units),
        out_shape=out_shape, in_specs=[anywhere] * len(args), out_specs=out_specs, scratch_shapes=sems,
        input_output_aliases=aliases,
        compiler_params=pltpu.CompilerParams(collective_id=slot, has_side_effects=True),
        name="send_%s_%d" % ("heavy" if heavy else "light", n_units),
    )(*args)


def solution(mesh):
    cache_spec = P(None, "dp", "tp", "sp", None)
    row_spec = P(("dp", "sp"), None)
    col_spec = P(None, None, "tp")
    inner_spec = P(None, "tp", None)
    window_spec = P(None, ("dp", "sp"), "tp", None, None)
    global_spec = P(("dp", "sp"), "tp", None, None)
    in_specs = (cache_spec, cache_spec, P("dp"), row_spec, P(None, None), col_spec, col_spec, col_spec, inner_spec, col_spec, col_spec, inner_spec)
    out_specs = (row_spec, window_spec, window_spec, global_spec, global_spec)

    def device_step(k_cache, v_cache, lengths, hidden, ln_gain, w_query, w_key, w_value, w_out, w_gate, w_up, w_down):
        n_layers = w_query.shape[0]
        rows_dev = hidden.shape[0]
        head_dim = k_cache.shape[-1]
        n_tp = mesh.shape["tp"]
        me = lax.axis_index("sp")
        core = me % 2
        chip = me // 2
        my_lengths = lax.dynamic_slice_in_dim(lengths, me * rows_dev, rows_dev)
        k_t = k_cache[:, :, 0].swapaxes(-1, -2)
        v_t = v_cache[:, :, 0].swapaxes(-1, -2)
        start, count, base, totals = unit_table(lengths - WINDOW)
        other_lengths = lax.ppermute(lengths, "dp", [(0, 1), (1, 0)])
        other_totals = unit_table(other_lengths - WINDOW)[3]
        most = jnp.maximum(totals, other_totals)
        heavy_need = jnp.maximum(most[0, 0], most[1, 1])
        light_need = jnp.maximum(most[0, 1], most[1, 0])
        heavy_index = jnp.sum(heavy_need > jnp.array(HEAVY_LEVELS, jnp.int32)).astype(jnp.int32)
        light_index = jnp.sum(light_need > jnp.array(LIGHT_LEVELS, jnp.int32)).astype(jnp.int32)

        table = jnp.stack([start, count, base], axis=-1)
        sent = lax.dynamic_slice(table, ((1 - chip) * CHIP_ROWS, core, 0), (CHIP_ROWS, 1, 3))[:, 0]
        sent = sent - jnp.array([1, 0, 0], jnp.int32) * (core * HALF_UNITS)
        pack_info = jnp.concatenate([(1 - chip)[None], sent.reshape(-1)]).astype(jnp.int32)
        mine = lax.dynamic_slice_in_dim(table, me * rows_dev, rows_dev)
        window_info = jnp.concatenate([
            jnp.stack([core, chip, me * rows_dev, me]), my_lengths - WINDOW, jnp.stack([chip, 1 - chip]),
            mine[:, :, 0].reshape(-1), mine[:, :, 1].reshape(-1), mine[:, :, 2].reshape(-1)]).astype(jnp.int32)
        global_info = jnp.concatenate([jnp.stack([core, chip, me * rows_dev, me]), my_lengths]).astype(jnp.int32)

        packed = pack_call(pack_info, k_t, v_t, n_layers - 1)
        heavy_calls = [functools.partial(send_call, True, n, 1 + i) for i, n in enumerate(HEAVY_LEVELS)]
        light_calls = [functools.partial(send_call, False, n, 1 + len(HEAVY_LEVELS) + i) for i, n in enumerate(LIGHT_LEVELS)]
        got, partner = lax.switch(heavy_index, heavy_calls, packed, k_t, v_t)
        got = lax.switch(light_index, light_calls, packed, k_t, v_t, got)

        got, after = lax.optimization_barrier((got, me))
        far = []
        for flip in (2, 3):
            first = (after ^ flip) * rows_dev
            rows = jnp.concatenate([
                lax.dynamic_slice(part, (n_layers - 1, first, 0, 0), (1, rows_dev) + part.shape[2:]) for part in (k_t, v_t)])
            far.append(lax.ppermute(rows, "sp", [(i, i ^ flip) for i in range(4)]))

        residual = hidden.astype(jnp.float32)
        tables = rotary_tables(my_lengths, head_dim, w_query.shape[2] // head_dim)
        wk_t = w_key.swapaxes(1, 2)
        wv_t = w_value.swapaxes(1, 2)
        held = None
        part = None
        for layer in range(n_layers):
            sliding = layer < n_layers - 1
            common = (residual, ln_gain[layer:layer + 1], tables, w_query, wk_t, wv_t, w_out, w_gate, w_up, w_down, k_t, v_t, partner)
            info, outside, before = (window_info, [got], held) if sliding else (global_info, far, None)
            result = layer_call(layer, sliding, info, *common, outside, before, part, n_tp)
            if part is not None:
                residual = result[1]
            part = result[0]
            if sliding:
                held = result[-2:]
            else:
                kept = result[-2:]
        residual = sum_call(part, residual, n_tp)

        def back(rows_t):
            return rows_t.swapaxes(-1, -2)

        return (residual.astype(jnp.bfloat16), back(held[0])[:, :, None], back(held[1])[:, :, None],
                back(kept[0])[:, None], back(kept[1])[:, None])

    return jax.shard_map(device_step, mesh=mesh, in_specs=in_specs, out_specs=out_specs, check_vma=False)
```

```python
import functools

import jax
import jax.numpy as jnp
from jax import lax
from jax.experimental import pallas as pl
from jax.experimental.pallas import tpu as pltpu
from jax.sharding import PartitionSpec as P

WINDOW = 4096
ROPE_BASE = 50000
NORM_EPS = 1e-5


PAD = 16
K_STEPS = 4
DOWN_ROWS = 384
MESH_ID = pl.DeviceIdType.MESH


VMEM_GRANT = 58 * 2 ** 20


def layer_kernel(layer, sliding, n_far, n_tp, lengths_ref, h_ref, gain_ref, cq_ref, sq_ref, ck_ref, sk_ref, *refs):
    wq_hbm, wk_hbm, wv_hbm, wg_hbm, wu_hbm, wd_hbm, wo_hbm, k_hbm, v_hbm, partner_hbm = refs[:10]
    far = refs[10:10 + n_far]
    fused = n_tp > 0
    units_ref_v = None
    if sliding and n_far > 1:
        refs, units_ref_v = refs[:-1], refs[-1]
    if fused:
        part_ref = refs[10 + n_far]
        (out_ref, h_out, keys_hbm, values_hbm, wq_ref, wk_ref, wv_ref, wg_ref, wu_ref, wd_ref, wo_ref, keys_ref, values_ref, units_ref,
         weight_sem, in_sem, out_sem, slots, send_sem, recv_sem) = refs[-20:]
    else:
        (out_ref, keys_hbm, values_hbm, wq_ref, wk_ref, wv_ref, wg_ref, wu_ref, wd_ref, wo_ref, keys_ref, values_ref, units_ref,
         weight_sem, in_sem, out_sem) = refs[-16:]
    n_rows, model = h_ref.shape
    dim = wk_ref.shape[0]
    q_width = wq_ref.shape[1]
    hidden = wg_ref.shape[1]
    heads = q_width // dim
    half_len = k_hbm.shape[-1]
    me = lax.axis_index("sp")
    chip = me // 2
    first_row = me * n_rows
    core = me % 2
    buffers = (keys_ref, values_ref)
    loose_v = sliding and n_far > 1
    edges = [lengths_ref[first_row + row] - (WINDOW if sliding else 0) for row in range(n_rows)]
    listed = [[None] * 2 for _ in range(n_rows)]
    if sliding:
        for half in range(2):
            rows, _ = list_of(lengths_ref, chip, half)
            for row in range(n_rows):
                listed[row][half] = [jnp.where(core == 0, one, two) for one, two in zip(rows[row], rows[n_rows + row])]

    def cache_copies(index):
        found = []
        pieces = 2 if sliding else 4
        for kind, (source, buffer) in enumerate(zip((k_hbm, v_hbm), buffers)):
            for piece in range(pieces):
                place = pl.ds(piece * half_len, half_len)
                who = piece ^ (index % 2) if sliding else piece ^ index
                if who == 0:
                    origin = source.at[layer, pl.ds(first_row, n_rows)]
                elif who == 1:
                    origin = partner_hbm.at[kind, layer]
                else:
                    origin = far[who - 2].at[kind]
                found.append(pltpu.make_async_copy(origin, buffer.at[:, :, place], in_sem.at[kind * 4 + piece]))
        if loose_v:
            for piece in range(2):
                place = pl.ds(piece * half_len, half_len)
                found.append(pltpu.make_async_copy(far[1 + (piece ^ (index % 2))].at[0], units_ref_v.at[:, :, place], in_sem.at[12 + piece]))
        return found

    variants = 2 if sliding else 4
    which = me % variants

    def each_variant(act):
        for index in range(variants):
            @pl.when(which == index)
            def _():
                for copy in cache_copies(index):
                    act(copy)

    unit_copies = []
    if sliding:
        for half in range(2):
            for kind in range(1 if loose_v else 2):
                unit_copies.append(pltpu.make_async_copy(
                    far[0].at[(chip + half) % 2, layer, kind], units_ref.at[half, kind], in_sem.at[8 + half * 2 + kind]))

    n_sem = [0]

    def weight_copy(source, target, first, size):
        rows = pl.ds(first, size)
        copy = pltpu.make_async_copy(source.at[layer, rows], target.at[rows], weight_sem.at[n_sem[0]])
        n_sem[0] += 1
        return copy

    k_len = model // K_STEPS
    down_cuts = [(first, min(DOWN_ROWS, hidden - first)) for first in range(0, hidden, DOWN_ROWS)]
    proj_copies = [weight_copy(wq_hbm, wq_ref, 0, model), weight_copy(wk_hbm, wk_ref, 0, dim), weight_copy(wv_hbm, wv_ref, 0, dim)]
    up_copies = [[weight_copy(wg_hbm, wg_ref, part * k_len, k_len), weight_copy(wu_hbm, wu_ref, part * k_len, k_len)] for part in range(K_STEPS)]
    out_weight = weight_copy(wo_hbm, wo_ref, 0, q_width)
    down_copies = [weight_copy(wd_hbm, wd_ref, first, size) for first, size in down_cuts]

    def start(copies):
        for copy in copies:
            copy.start()

    def wait(copies):
        for copy in copies:
            copy.wait()

    lane = lax.broadcasted_iota(jnp.int32, (dim, LANES), 1)
    if fused:
        here = lax.axis_index("tp")
        barrier = pltpu.get_barrier_semaphore()
        for flip in range(1, n_tp):
            pl.semaphore_signal(barrier, inc=1, device_id={"tp": here ^ flip}, device_id_type=MESH_ID)
    start(proj_copies)
    each_variant(lambda copy: copy.start())
    start(unit_copies)
    if fused:
        pl.semaphore_wait(barrier, n_tp - 1)
        shares = []
        for flip in range(1, n_tp):
            shares.append(pltpu.make_async_remote_copy(
                src_ref=part_ref, dst_ref=slots.at[here], send_sem=send_sem.at[flip - 1], recv_sem=recv_sem.at[flip - 1],
                device_id={"tp": here ^ flip}, device_id_type=MESH_ID))
        start(shares)
        for copies in up_copies:
            start(copies)
        start([out_weight])
        start(down_copies)
        slots[here] = part_ref[...]
    else:
        for copies in up_copies[:2]:
            start(copies)
    if fused:
        each_variant(lambda copy: copy.wait())
        wait(unit_copies)
        for row in range(n_rows):
            edge = edges[row]
            for unit in range(keys_ref.shape[-1] // LANES):
                slot = lane + unit * LANES
                cols = slice(unit * LANES, (unit + 1) * LANES)
                half = unit // HALF_UNITS
                if sliding:
                    begin, _, base = listed[row][half]
                    keep = jnp.logical_xor(slot < edge, chip == 0)
                    place = jnp.clip(base + unit - begin, 0, MAX_UNITS - 1)
                elif unit < 2 * HALF_UNITS:
                    continue
                else:
                    keep = slot < edge
                for kind, buffer in enumerate(buffers):
                    if not sliding:
                        remote = jnp.zeros((dim, LANES), buffer.dtype)
                    elif kind == 1 and loose_v:
                        remote = units_ref_v[row, :, cols]
                    else:
                        remote = units_ref[half, kind, place]
                    buffer[row, :, cols] = jnp.where(keep, buffer[row, :, cols], remote)
        wait(shares)
        total = slots[0]
        for index in range(1, n_tp):
            total = total + slots[index]
        rows32 = (h_ref[...] + total).astype(jnp.bfloat16).astype(jnp.float32)
        h_out[...] = rows32
    else:
        rows32 = h_ref[...]
    centered = rows32 - jnp.mean(rows32, axis=-1, keepdims=True)
    variance = jnp.mean(centered * centered, axis=-1, keepdims=True)
    scaled = centered * lax.rsqrt(variance + NORM_EPS)
    normed = scaled * gain_ref[...].astype(jnp.float32)
    normed = jnp.concatenate([normed, jnp.zeros((PAD - n_rows, model), jnp.float32)], axis=0).astype(jnp.bfloat16)

    nt = (((1,), (1,)), ((), ()))
    wait(proj_copies)
    query = jnp.dot(normed, wq_ref[...], preferred_element_type=jnp.float32)[:8]
    k_new = lax.dot_general(wk_ref[...], normed, nt, preferred_element_type=jnp.float32)
    v_new = lax.dot_general(wv_ref[...], normed, nt, preferred_element_type=jnp.float32)
    if sliding:
        q_lane = lax.broadcasted_iota(jnp.int32, query.shape, 1)
        swapped = jnp.where(q_lane % dim < dim // 2, pltpu.roll(query, q_width - dim // 2, 1), pltpu.roll(query, dim // 2, 1))
        query = query * cq_ref[...] + swapped * sq_ref[...]
        first = k_new[:dim // 2]
        second = k_new[dim // 2:]
        cosine = ck_ref[...]
        sine = sk_ref[...]
        k_new = jnp.concatenate([first * cosine - second * sine, second * cosine + first * sine], axis=0)
    k_new = k_new.astype(jnp.bfloat16).astype(jnp.float32)
    v_new = v_new.astype(jnp.bfloat16).astype(jnp.float32)
    spread = [jnp.broadcast_to(query[r:r + 1], (heads, q_width)) for r in range(n_rows)]
    spread = jnp.concatenate(spread, axis=0)
    at_row = lax.broadcasted_iota(jnp.int32, spread.shape, 0)
    at_col = lax.broadcasted_iota(jnp.int32, spread.shape, 1)
    own_head = at_col // dim == at_row % heads
    masked = jnp.where(own_head, spread, 0.0).astype(jnp.bfloat16)
    pick_row = lax.broadcasted_iota(jnp.int32, (dim, q_width), 0)
    pick_col = lax.broadcasted_iota(jnp.int32, (dim, q_width), 1)
    pick = jnp.where(pick_col % dim == pick_row, 1.0, 0.0).astype(jnp.bfloat16)
    head_q = lax.dot_general(masked, pick, nt, preferred_element_type=jnp.float32).astype(jnp.bfloat16)

    column = lax.broadcasted_iota(jnp.int32, (dim, PAD), 1)
    if fused:
        for row in range(n_rows):
            edge = edges[row]
            for buffer, new in zip(buffers, (k_new, v_new)):
                picked = jnp.sum(jnp.where(column == row, new, 0.0), axis=1, keepdims=True)
                tile = jnp.broadcast_to(picked, (dim, LANES)).astype(buffer.dtype)
                for unit in range(keys_ref.shape[-1] // LANES):
                    if not sliding and unit < 2 * HALF_UNITS:
                        continue
                    cols = slice(unit * LANES, (unit + 1) * LANES)
                    buffer[row, :, cols] = jnp.where(lane + unit * LANES == edge, tile, buffer[row, :, cols])
    else:
        start(up_copies[2])
        each_variant(lambda copy: copy.wait())
        wait(unit_copies)
        for row in range(n_rows):
            edge = edges[row]
            border = edge // LANES
            cols = pl.ds(pl.multiple_of(border * LANES, LANES), LANES)
            slot = lane + border * LANES
            before = [buffer[row, :, cols] for buffer in buffers]
            if sliding:
                for half in range(2):
                    begin, count, base = listed[row][half]

                    def place_unit(unit, carry, half=half, begin=begin, base=base):
                        to = pl.ds(pl.multiple_of(unit * LANES, LANES), LANES)
                        for kind, buffer in enumerate(buffers):
                            buffer[row, :, to] = units_ref[half, kind, base + unit - begin]
                        return carry

                    lax.fori_loop(begin, begin + count, place_unit, 0)
                border_half = border // HALF_UNITS
                border_base = jnp.where(border_half == 0, listed[row][0][2] - listed[row][0][0], listed[row][1][2] - listed[row][1][0])
                border_place = jnp.clip(border_base + border, 0, MAX_UNITS - 1)
                keep = jnp.logical_xor(slot < edge, chip == 0)
            else:
                def clear_unit(unit, carry):
                    to = pl.ds(pl.multiple_of(unit * LANES, LANES), LANES)
                    for buffer in buffers:
                        buffer[row, :, to] = jnp.zeros((dim, LANES), buffer.dtype)
                    return carry

                lax.fori_loop(border + 1, 4 * HALF_UNITS, clear_unit, 0)
                keep = slot < edge
            for kind, (buffer, new) in enumerate(zip(buffers, (k_new, v_new))):
                picked = jnp.sum(jnp.where(column == row, new, 0.0), axis=1, keepdims=True)
                if sliding:
                    remote = units_ref[border_half, kind, border_place].astype(jnp.float32)
                else:
                    remote = jnp.zeros((dim, LANES), jnp.float32)
                merged = jnp.where(keep, before[kind].astype(jnp.float32), remote)
                merged = jnp.where(slot == edge, jnp.broadcast_to(picked, (dim, LANES)), merged)
                buffer[row, :, cols] = merged.astype(buffer.dtype)
        start(up_copies[3])
    out_copies = []
    for kind, (buffer, kept) in enumerate(zip(buffers, (keys_hbm, values_hbm))):
        target = kept.at[layer] if sliding else kept
        out_copies.append(pltpu.make_async_copy(buffer, target, out_sem.at[kind]))
    start(out_copies)
    mixed = []
    for row in range(n_rows):
        edge = edges[row]
        scores = jnp.dot(head_q[heads * row:heads * (row + 1)], keys_ref[row], preferred_element_type=jnp.float32) * dim ** -0.5
        if not sliding:
            position = lax.broadcasted_iota(jnp.int32, scores.shape, 1)
            scores = jnp.where(position <= edge, scores, -1e30)
        top = jnp.max(scores, axis=-1, keepdims=True)
        raised = jnp.exp(scores - top)
        weights = (raised / jnp.sum(raised, axis=-1, keepdims=True)).astype(jnp.bfloat16)
        mixed.append(lax.dot_general(weights, values_ref[row], nt, preferred_element_type=jnp.float32))
    both = jnp.concatenate(mixed, axis=0).astype(jnp.bfloat16)
    wide = jnp.dot(both, pick, preferred_element_type=jnp.float32)
    wide = jnp.where(own_head, wide, 0.0).astype(jnp.bfloat16)

    if not fused:
        start([out_weight])
        start(down_copies)
    gate = jnp.zeros((PAD, hidden), jnp.float32)
    raise_ = jnp.zeros((PAD, hidden), jnp.float32)
    for part in range(K_STEPS):
        wait(up_copies[part])
        rows = slice(part * k_len, (part + 1) * k_len)
        gate = gate + jnp.dot(normed[:, rows], wg_ref[rows], preferred_element_type=jnp.float32)
        raise_ = raise_ + jnp.dot(normed[:, rows], wu_ref[rows], preferred_element_type=jnp.float32)
    active = (gate * jax.nn.sigmoid(gate) * raise_).astype(jnp.bfloat16)

    wait([out_weight])
    product = jnp.dot(wide, wo_ref[...], preferred_element_type=jnp.float32)
    sums = jnp.concatenate([jnp.sum(product[heads * r:heads * (r + 1)], axis=0, keepdims=True) for r in range(n_rows)], axis=0)
    total = jnp.zeros((PAD, model), jnp.float32)
    for copy, (first, size) in zip(down_copies, down_cuts):
        copy.wait()
        total = total + jnp.dot(active[:, first:first + size], wd_ref[first:first + size], preferred_element_type=jnp.float32)
    out_ref[...] = sums + total[:n_rows]
    wait(out_copies)


def layer_call(layer, sliding, lengths, h, gain, tables, w_query, wk_t, wv_t, w_out, w_gate, w_up, w_down, k_t, v_t, partner, far, held, part=None, n_tp=0):
    n_rows, model = h.shape
    q_width = w_query.shape[2]
    dim = wk_t.shape[1]
    hidden = w_gate.shape[2]
    half_len = k_t.shape[-1]
    in_vmem = pl.BlockSpec(memory_space=pltpu.VMEM)
    anywhere = pl.BlockSpec(memory_space=pl.ANY)
    total = (2 if sliding else 4) * half_len
    kept = (3, n_rows, dim, total) if sliding else (n_rows, dim, total)
    kept_shape = jax.ShapeDtypeStruct(kept, k_t.dtype)
    args = [lengths, h, gain, *tables, w_query, wk_t, wv_t, w_gate, w_up, w_down, w_out, k_t, v_t, partner, *far]
    in_specs = [pl.BlockSpec(memory_space=pltpu.SMEM)] + [in_vmem] * 6 + [anywhere] * (10 + len(far))
    fused = part is not None
    if fused:
        args.append(part)
        in_specs.append(in_vmem)
    aliases = {}
    n_small = 2 if fused else 1
    if held is not None:
        for place, array in enumerate(held):
            aliases[len(args)] = n_small + place
            in_specs.append(anywhere)
            args.append(array)
    weight_bytes = 2 * (2 * model * q_width + 2 * dim * model + 3 * model * hidden)
    units = (2, 2, MAX_UNITS, dim, LANES) if sliding else (8, LANES)
    n_weight = 4 + 2 * K_STEPS + -(-hidden // DOWN_ROWS)
    row_shape = jax.ShapeDtypeStruct((n_rows, model), jnp.float32)
    loose = [pltpu.VMEM((n_rows, dim, total), jnp.bfloat16)] if sliding and len(far) > 1 else []
    if fused:
        remote = [pltpu.VMEM((n_tp, n_rows, model), jnp.float32), pltpu.SemaphoreType.DMA((n_tp - 1,)), pltpu.SemaphoreType.DMA((n_tp - 1,))]
        params = pltpu.CompilerParams(vmem_limit_bytes=VMEM_GRANT, collective_id=40 + layer, has_side_effects=True)
    else:
        remote = []
        params = pltpu.CompilerParams(vmem_limit_bytes=VMEM_GRANT)
    return pl.pallas_call(
        functools.partial(layer_kernel, layer, sliding, len(far), n_tp if fused else 0),
        in_specs=in_specs, out_specs=(in_vmem,) * n_small + (anywhere, anywhere),
        scratch_shapes=[
            pltpu.VMEM((model, q_width), jnp.bfloat16),
            pltpu.VMEM((dim, model), jnp.bfloat16),
            pltpu.VMEM((dim, model), jnp.bfloat16),
            pltpu.VMEM((model, hidden), jnp.bfloat16),
            pltpu.VMEM((model, hidden), jnp.bfloat16),
            pltpu.VMEM((hidden, model), jnp.bfloat16),
            pltpu.VMEM((q_width, model), jnp.bfloat16),
            pltpu.VMEM((n_rows, dim, total), jnp.bfloat16),
            pltpu.VMEM((n_rows, dim, total), jnp.bfloat16),
            pltpu.VMEM(units, jnp.bfloat16),
            pltpu.SemaphoreType.DMA((n_weight,)),
            pltpu.SemaphoreType.DMA((14,)),
            pltpu.SemaphoreType.DMA((2,)),
        ] + remote + loose,
        out_shape=(row_shape,) * n_small + (kept_shape, kept_shape),
        input_output_aliases=aliases,
        compiler_params=params,
        cost_estimate=pl.CostEstimate(flops=PAD * weight_bytes, bytes_accessed=weight_bytes, transcendentals=0),
        name="layer_%d" % layer,
    )(*args)


def rotary_tables(positions, dim, heads):
    half = dim // 2
    low, high = positions[0].astype(jnp.float32), positions[1].astype(jnp.float32)

    def angles(feature, row):
        inv_freq = 1.0 / (ROPE_BASE ** (feature.astype(jnp.float32) * 2.0 / dim))
        return jnp.where(row == 0, low, high) * inv_freq

    wide = (8, heads * dim)
    lane = lax.broadcasted_iota(jnp.int32, wide, 1)
    turn = angles(lane % half, lax.broadcasted_iota(jnp.int32, wide, 0))
    tall = (half, PAD)
    turn_t = angles(lax.broadcasted_iota(jnp.int32, tall, 0), lax.broadcasted_iota(jnp.int32, tall, 1))
    return jnp.cos(turn), jnp.where(lane % dim < half, -jnp.sin(turn), jnp.sin(turn)), jnp.cos(turn_t), jnp.sin(turn_t)


def sum_kernel(n_tp, part_ref, resid_ref, out_ref, slots, send_sem, recv_sem):
    me = lax.axis_index("tp")
    barrier = pltpu.get_barrier_semaphore()
    for flip in range(1, n_tp):
        pl.semaphore_signal(barrier, inc=1, device_id={"tp": me ^ flip}, device_id_type=MESH_ID)
    pl.semaphore_wait(barrier, n_tp - 1)
    copies = []
    for flip in range(1, n_tp):
        copy = pltpu.make_async_remote_copy(
            src_ref=part_ref, dst_ref=slots.at[me], send_sem=send_sem.at[flip - 1], recv_sem=recv_sem.at[flip - 1],
            device_id={"tp": me ^ flip}, device_id_type=MESH_ID)
        copy.start()
        copies.append(copy)
    slots[me] = part_ref[...]
    for copy in copies:
        copy.wait()
    total = slots[0]
    for index in range(1, n_tp):
        total = total + slots[index]
    out_ref[...] = (resid_ref[...] + total).astype(jnp.bfloat16).astype(jnp.float32)


def sum_call(part, resid, n_tp):
    return pl.pallas_call(
        functools.partial(sum_kernel, n_tp),
        out_shape=jax.ShapeDtypeStruct(part.shape, jnp.float32),
        in_specs=[pl.BlockSpec(memory_space=pltpu.VMEM)] * 2,
        out_specs=pl.BlockSpec(memory_space=pltpu.VMEM),
        scratch_shapes=[
            pltpu.VMEM((n_tp,) + part.shape, jnp.float32),
            pltpu.SemaphoreType.DMA((n_tp - 1,)),
            pltpu.SemaphoreType.DMA((n_tp - 1,)),
        ],
        compiler_params=pltpu.CompilerParams(collective_id=0, has_side_effects=True),
        name="sum_tp",
    )(part, resid)


LANES = 128
HALF_UNITS = 16
CHIP_ROWS = 4
MAX_UNITS = CHIP_ROWS * HALF_UNITS
HEAVY_LEVELS = (32, 40, 44, 48, 52, 56, 60, 64)
LIGHT_LEVELS = (8, 16, 20, 24, 28, 32, 36, 40, 44, 48, 56, 64)


def row_units(edge, half, from_upper):
    low = half * HALF_UNITS
    upper_end = jnp.clip((edge + LANES - 1) // LANES, low, low + HALF_UNITS)
    lower_start = jnp.clip((edge + 1) // LANES, low, low + HALF_UNITS)
    start = jnp.where(from_upper, low, lower_start)
    count = jnp.where(from_upper, upper_end - low, low + HALF_UNITS - lower_start)
    return start, count


def list_of(lengths_ref, chip, half):
    base = jnp.int32(0)
    found = []
    for row in range(CHIP_ROWS):
        start, count = row_units(lengths_ref[CHIP_ROWS * chip + row] - WINDOW, half, chip == 0)
        found.append((start, count, base))
        base = base + count
    return found, base


def pack_kernel(lengths_ref, other_ref, k_ref, v_ref, out_ref, level_ref):
    me = lax.axis_index("sp")
    core = me % 2
    chip = me // 2
    layer = pl.program_id(0)

    @pl.when(layer == 0)
    def _():
        for place, (levels, swap) in enumerate(((HEAVY_LEVELS, 0), (LIGHT_LEVELS, 1))):
            need = jnp.int32(0)
            for ref in (lengths_ref, other_ref):
                for target in range(2):
                    need = jnp.maximum(need, list_of(ref, target, target ^ swap)[1])
            index = jnp.int32(0)
            for level in levels[:-1]:
                index = index + jnp.where(need > level, 1, 0)
            level_ref[place] = index

    rows, _ = list_of(lengths_ref, 1 - chip, core)
    for row, (start, count, base) in enumerate(rows):
        first = start - core * HALF_UNITS
        for unit in range(HALF_UNITS):
            @pl.when(jnp.logical_and(unit >= first, unit < first + count))
            def _():
                place = base + unit - first
                cols = pl.ds(unit * LANES, LANES)
                out_ref[0, 0, place] = k_ref[0, row, :, cols]
                out_ref[0, 1, place] = v_ref[0, row, :, cols]


def pack_call(lengths, other, k_t, v_t, n_layers):
    dim, half_len = k_t.shape[2:]
    block = pl.BlockSpec((1, CHIP_ROWS, dim, half_len), lambda l: (l, 1 - lax.axis_index("sp") // 2, 0, 0))
    small = pl.BlockSpec(memory_space=pltpu.SMEM)
    return pl.pallas_call(
        pack_kernel,
        grid=(n_layers,), in_specs=[small, small, block, block],
        out_specs=(pl.BlockSpec((1, 2, MAX_UNITS, dim, LANES), lambda l: (l, 0, 0, 0, 0)), small),
        out_shape=(jax.ShapeDtypeStruct((n_layers, 2, MAX_UNITS, dim, LANES), k_t.dtype), jax.ShapeDtypeStruct((2,), jnp.int32)),
        compiler_params=pltpu.CompilerParams(dimension_semantics=("arbitrary",), vmem_limit_bytes=VMEM_GRANT),
        name="pack_units",
    )(lengths, other, k_t, v_t)


def send_kernel(heavy, n_units, packed_ref, k_ref, v_ref, *rest):
    if heavy:
        got_ref, partner_ref, send_sem, recv_sem, fsend_sem, frecv_sem, psend_sem, precv_sem = rest
        phase = 0
    else:
        _, got_ref, send_sem, recv_sem, fsend_sem, frecv_sem = rest
        phase = 1
    me = lax.axis_index("sp")
    middle = jnp.logical_or(me == 1, me == 2)
    sender = middle if heavy else jnp.logical_not(middle)
    across = (me + 2) % 4
    partner = me + 1 - 2 * (me % 2)
    n_layers = packed_ref.shape[0]
    barrier = pltpu.get_barrier_semaphore()
    for peer in (across, partner):
        pl.semaphore_signal(barrier, inc=1, device_id={"sp": peer}, device_id_type=MESH_ID)
    pl.semaphore_wait(barrier, 2)
    direct = []
    onward = []
    for layer in range(n_layers):
        for kind in range(2):
            index = layer * 2 + kind
            if index == 2 * n_layers - 1:
                continue
            part = pl.ds(0, n_units)
            target = got_ref.at[phase, layer, kind, part]
            direct.append(pltpu.make_async_remote_copy(
                src_ref=packed_ref.at[layer, kind, part], dst_ref=target, send_sem=send_sem.at[index], recv_sem=recv_sem.at[index],
                device_id={"sp": across}, device_id_type=MESH_ID))
            onward.append(pltpu.make_async_remote_copy(
                src_ref=target, dst_ref=target, send_sem=fsend_sem.at[index], recv_sem=frecv_sem.at[index],
                device_id={"sp": partner}, device_id_type=MESH_ID))

    @pl.when(sender)
    def _():
        for copy in direct:
            copy.start()

    shares = []
    if heavy:
        rows = partner_ref.shape[2]
        for kind, source in enumerate((k_ref, v_ref)):
            for layer in range(source.shape[0]):
                index = layer * 2 + kind
                shares.append(pltpu.make_async_remote_copy(
                    src_ref=source.at[layer, pl.ds(rows * partner, rows)], dst_ref=partner_ref.at[kind, layer],
                    send_sem=psend_sem.at[index], recv_sem=precv_sem.at[index],
                    device_id={"sp": partner}, device_id_type=MESH_ID))
        for copy in shares:
            copy.start()

    @pl.when(jnp.logical_not(sender))
    def _():
        for near, far in zip(direct, onward):
            near.wait_recv()
            far.start()
        for far in onward:
            far.wait_send()

    @pl.when(sender)
    def _():
        for near, far in zip(direct, onward):
            near.wait_send()
            far.wait_recv()

    for copy in shares:
        copy.wait()


def send_call(heavy, n_units, slot, packed, k_t, v_t, got=None):
    n_layers = packed.shape[0]
    n_copies = 2 * n_layers - 1
    anywhere = pl.BlockSpec(memory_space=pl.ANY)
    got_shape = jax.ShapeDtypeStruct((2,) + packed.shape, packed.dtype)
    sems = [pltpu.SemaphoreType.DMA((n_copies,)) for _ in range(4)]
    if heavy:
        args = (packed, k_t, v_t)
        rows = k_t.shape[1] // 4
        out_shape = (got_shape, jax.ShapeDtypeStruct((2, k_t.shape[0], rows) + k_t.shape[2:], k_t.dtype))
        sems += [pltpu.SemaphoreType.DMA((2 * k_t.shape[0],)) for _ in range(2)]
        aliases = {}
        out_specs = (anywhere, anywhere)
    else:
        args = (packed, k_t, v_t, got)
        out_shape = got_shape
        aliases = {3: 0}
        out_specs = anywhere
    return pl.pallas_call(
        functools.partial(send_kernel, heavy, n_units),
        out_shape=out_shape, in_specs=[anywhere] * len(args), out_specs=out_specs, scratch_shapes=sems,
        input_output_aliases=aliases,
        compiler_params=pltpu.CompilerParams(collective_id=slot, has_side_effects=True),
        name="send_%s_%d" % ("heavy" if heavy else "light", n_units),
    )(*args)


def solution(mesh):
    cache_spec = P(None, "dp", "tp", "sp", None)
    row_spec = P(("dp", "sp"), None)
    col_spec = P(None, None, "tp")
    inner_spec = P(None, "tp", None)
    window_spec = P(None, ("dp", "sp"), "tp", None, None)
    global_spec = P(("dp", "sp"), "tp", None, None)
    in_specs = (cache_spec, cache_spec, P("dp"), row_spec, P(None, None), col_spec, col_spec, col_spec, inner_spec, col_spec, col_spec, inner_spec)
    out_specs = (row_spec, window_spec, window_spec, global_spec, global_spec)

    def device_step(k_cache, v_cache, lengths, hidden, ln_gain, w_query, w_key, w_value, w_out, w_gate, w_up, w_down):
        n_layers = w_query.shape[0]
        rows_dev = hidden.shape[0]
        head_dim = k_cache.shape[-1]
        n_tp = mesh.shape["tp"]
        me = lax.axis_index("sp")
        my_lengths = lax.dynamic_slice_in_dim(lengths, me * rows_dev, rows_dev)
        k_t = k_cache[:, :, 0].swapaxes(-1, -2)
        v_t = v_cache[:, :, 0].swapaxes(-1, -2)
        last = n_layers - 1

        def shift(parts, layer, flip, origin):
            first = (origin ^ flip) * rows_dev
            cut = [lax.dynamic_slice(part, (layer, first, 0, 0), (1, rows_dev) + part.shape[2:]) for part in parts]
            return lax.ppermute(jnp.concatenate(cut), "sp", [(i, i ^ flip) for i in range(4)])

        other = lax.ppermute(lengths, "dp", [(0, 1), (1, 0)])
        packed, levels = pack_call(lengths, other, k_t, v_t, n_layers - 1)
        last_across = shift((k_t, v_t), last, 2, me)
        heavy_calls = [functools.partial(send_call, True, n, 1 + i) for i, n in enumerate(HEAVY_LEVELS)]
        light_calls = [functools.partial(send_call, False, n, 1 + len(HEAVY_LEVELS) + i) for i, n in enumerate(LIGHT_LEVELS)]
        got, partner = lax.switch(levels[0], heavy_calls, packed, k_t, v_t)
        got = lax.switch(levels[1], light_calls, packed, k_t, v_t, got)
        got, after = lax.optimization_barrier((got, me))
        third_v = [shift((v_t,), last - 1, flip, after) for flip in (2, 3)]

        residual = hidden.astype(jnp.float32)
        tables = rotary_tables(my_lengths, head_dim, w_query.shape[2] // head_dim)
        wk_t = w_key.swapaxes(1, 2)
        wv_t = w_value.swapaxes(1, 2)
        held = None
        part = None
        for layer in range(n_layers):
            sliding = layer < last
            common = (residual, ln_gain[layer:layer + 1], tables, w_query, wk_t, wv_t, w_out, w_gate, w_up, w_down, k_t, v_t, partner)
            if layer == last:
                outside, before = [last_across, last_diagonal], None
            else:
                outside, before = [got] + (third_v if layer == last - 1 else []), held
            result = layer_call(layer, sliding, lengths, *common, outside, before, part, n_tp)
            if part is not None:
                residual = result[1]
            part = result[0]
            if layer == 0:
                part, later = lax.optimization_barrier((part, after))
                last_diagonal = shift((k_t, v_t), last, 3, later)
            if sliding:
                held = result[-2:]
            else:
                kept = result[-2:]
        residual = sum_call(part, residual, n_tp)

        def back(rows_t):
            return rows_t.swapaxes(-1, -2)

        return (residual.astype(jnp.bfloat16), back(held[0])[:, :, None], back(held[1])[:, :, None],
                back(kept[0])[:, None], back(kept[1])[:, None])

    return jax.shard_map(device_step, mesh=mesh, in_specs=in_specs, out_specs=out_specs, check_vma=False)
```

```python
import functools

import jax
import jax.numpy as jnp
from jax import lax
from jax.experimental import pallas as pl
from jax.experimental.pallas import tpu as pltpu
from jax.sharding import PartitionSpec as P

WINDOW = 4096
ROPE_BASE = 50000
NORM_EPS = 1e-5


PAD = 16
K_STEPS = 4
DOWN_ROWS = 384
MESH_ID = pl.DeviceIdType.MESH


VMEM_GRANT = 63 * 2 ** 20


def layer_kernel(layer, sliding, n_far, n_tp, lengths_ref, h_ref, gain_ref, cq_ref, sq_ref, ck_ref, sk_ref, *refs):
    wq_hbm, wk_hbm, wv_hbm, wg_hbm, wu_hbm, wd_hbm, wo_hbm, k_hbm, v_hbm, partner_hbm = refs[:10]
    far = refs[10:10 + n_far]
    fused = n_tp > 0
    if fused:
        part_ref = refs[10 + n_far]
        (out_ref, h_out, keys_hbm, values_hbm, wq_ref, wk_ref, wv_ref, wg_ref, wu_ref, wd_ref, wo_ref, keys_ref, values_ref, units_ref,
         weight_sem, in_sem, out_sem, slots, send_sem, recv_sem) = refs[-20:]
    else:
        (out_ref, keys_hbm, values_hbm, wq_ref, wk_ref, wv_ref, wg_ref, wu_ref, wd_ref, wo_ref, keys_ref, values_ref, units_ref,
         weight_sem, in_sem, out_sem) = refs[-16:]
    n_rows, model = h_ref.shape
    dim = wk_ref.shape[0]
    q_width = wq_ref.shape[1]
    hidden = wg_ref.shape[1]
    heads = q_width // dim
    half_len = k_hbm.shape[-1]
    me = lax.axis_index("sp")
    chip = me // 2
    first_row = me * n_rows
    core = me % 2
    buffers = (keys_ref, values_ref)
    edges = [lengths_ref[first_row + row] - (WINDOW if sliding else 0) for row in range(n_rows)]
    listed = [[None] * 2 for _ in range(n_rows)]
    if sliding:
        for half in range(2):
            rows, _ = list_of(lengths_ref, chip, half)
            for row in range(n_rows):
                listed[row][half] = [jnp.where(core == 0, one, two) for one, two in zip(rows[row], rows[n_rows + row])]

    def cache_copies(index):
        found = []
        pieces = 2 if sliding else 4
        for kind, (source, buffer) in enumerate(zip((k_hbm, v_hbm), buffers)):
            for piece in range(pieces):
                place = pl.ds(piece * half_len, half_len)
                who = piece ^ (index % 2) if sliding else piece ^ index
                if who == 0:
                    origin = source.at[layer, pl.ds(first_row, n_rows)]
                elif who == 1:
                    origin = partner_hbm.at[kind, layer]
                else:
                    origin = far[who - 2].at[kind]
                found.append(pltpu.make_async_copy(origin, buffer.at[:, :, place], in_sem.at[kind * 4 + piece]))
        return found

    variants = 2 if sliding else 4
    which = me % variants

    def each_variant(act):
        for index in range(variants):
            @pl.when(which == index)
            def _():
                for copy in cache_copies(index):
                    act(copy)

    unit_copies = []
    if sliding:
        for half in range(2):
            for kind in range(2):
                unit_copies.append(pltpu.make_async_copy(
                    far[0].at[(chip + half) % 2, layer, kind], units_ref.at[half, kind], in_sem.at[8 + half * 2 + kind]))

    n_sem = [0]

    def weight_copy(source, target, first, size):
        rows = pl.ds(first, size)
        copy = pltpu.make_async_copy(source.at[layer, rows], target.at[rows], weight_sem.at[n_sem[0]])
        n_sem[0] += 1
        return copy

    k_len = model // K_STEPS
    down_cuts = [(first, min(DOWN_ROWS, hidden - first)) for first in range(0, hidden, DOWN_ROWS)]
    proj_copies = [weight_copy(wq_hbm, wq_ref, 0, model), weight_copy(wk_hbm, wk_ref, 0, dim), weight_copy(wv_hbm, wv_ref, 0, dim)]
    up_copies = [[weight_copy(wg_hbm, wg_ref, part * k_len, k_len), weight_copy(wu_hbm, wu_ref, part * k_len, k_len)] for part in range(K_STEPS)]
    out_weight = weight_copy(wo_hbm, wo_ref, 0, q_width)
    down_copies = [weight_copy(wd_hbm, wd_ref, first, size) for first, size in down_cuts]

    def start(copies):
        for copy in copies:
            copy.start()

    def wait(copies):
        for copy in copies:
            copy.wait()

    lane = lax.broadcasted_iota(jnp.int32, (dim, LANES), 1)
    if fused:
        here = lax.axis_index("tp")
        barrier = pltpu.get_barrier_semaphore()
        for flip in range(1, n_tp):
            pl.semaphore_signal(barrier, inc=1, device_id={"tp": here ^ flip}, device_id_type=MESH_ID)
    start(proj_copies)
    each_variant(lambda copy: copy.start())
    start(unit_copies)
    if fused:
        pl.semaphore_wait(barrier, n_tp - 1)
        shares = []
        for flip in range(1, n_tp):
            shares.append(pltpu.make_async_remote_copy(
                src_ref=part_ref, dst_ref=slots.at[here], send_sem=send_sem.at[flip - 1], recv_sem=recv_sem.at[flip - 1],
                device_id={"tp": here ^ flip}, device_id_type=MESH_ID))
        start(shares)
        for copies in up_copies:
            start(copies)
        start([out_weight])
        start(down_copies)
        slots[here] = part_ref[...]
    else:
        for copies in up_copies[:2]:
            start(copies)
    if fused:
        each_variant(lambda copy: copy.wait())
        wait(unit_copies)
        for row in range(n_rows):
            edge = edges[row]
            for unit in range(keys_ref.shape[-1] // LANES):
                slot = lane + unit * LANES
                cols = slice(unit * LANES, (unit + 1) * LANES)
                half = unit // HALF_UNITS
                if sliding:
                    begin, _, base = listed[row][half]
                    keep = jnp.logical_xor(slot < edge, chip == 0)
                    place = jnp.clip(base + unit - begin, 0, MAX_UNITS - 1)
                elif unit < 2 * HALF_UNITS:
                    continue
                else:
                    keep = slot < edge
                for kind, buffer in enumerate(buffers):
                    if not sliding:
                        remote = jnp.zeros((dim, LANES), buffer.dtype)
                    else:
                        remote = units_ref[half, kind, place]
                    buffer[row, :, cols] = jnp.where(keep, buffer[row, :, cols], remote)
        wait(shares)
        total = slots[0]
        for index in range(1, n_tp):
            total = total + slots[index]
        rows32 = (h_ref[...] + total).astype(jnp.bfloat16).astype(jnp.float32)
        h_out[...] = rows32
    else:
        rows32 = h_ref[...]
    centered = rows32 - jnp.mean(rows32, axis=-1, keepdims=True)
    variance = jnp.mean(centered * centered, axis=-1, keepdims=True)
    scaled = centered * lax.rsqrt(variance + NORM_EPS)
    normed = scaled * gain_ref[...].astype(jnp.float32)
    normed = jnp.concatenate([normed, jnp.zeros((PAD - n_rows, model), jnp.float32)], axis=0).astype(jnp.bfloat16)

    nt = (((1,), (1,)), ((), ()))
    wait(proj_copies)
    query = jnp.dot(normed, wq_ref[...], preferred_element_type=jnp.float32)[:8]
    k_new = lax.dot_general(wk_ref[...], normed, nt, preferred_element_type=jnp.float32)
    v_new = lax.dot_general(wv_ref[...], normed, nt, preferred_element_type=jnp.float32)
    if sliding:
        q_lane = lax.broadcasted_iota(jnp.int32, query.shape, 1)
        swapped = jnp.where(q_lane % dim < dim // 2, pltpu.roll(query, q_width - dim // 2, 1), pltpu.roll(query, dim // 2, 1))
        query = query * cq_ref[...] + swapped * sq_ref[...]
        first = k_new[:dim // 2]
        second = k_new[dim // 2:]
        cosine = ck_ref[...]
        sine = sk_ref[...]
        k_new = jnp.concatenate([first * cosine - second * sine, second * cosine + first * sine], axis=0)
    k_new = k_new.astype(jnp.bfloat16).astype(jnp.float32)
    v_new = v_new.astype(jnp.bfloat16).astype(jnp.float32)
    spread = [jnp.broadcast_to(query[r:r + 1], (heads, q_width)) for r in range(n_rows)]
    spread = jnp.concatenate(spread, axis=0)
    at_row = lax.broadcasted_iota(jnp.int32, spread.shape, 0)
    at_col = lax.broadcasted_iota(jnp.int32, spread.shape, 1)
    own_head = at_col // dim == at_row % heads
    masked = jnp.where(own_head, spread, 0.0).astype(jnp.bfloat16)
    pick_row = lax.broadcasted_iota(jnp.int32, (dim, q_width), 0)
    pick_col = lax.broadcasted_iota(jnp.int32, (dim, q_width), 1)
    pick = jnp.where(pick_col % dim == pick_row, 1.0, 0.0).astype(jnp.bfloat16)
    head_q = lax.dot_general(masked, pick, nt, preferred_element_type=jnp.float32).astype(jnp.bfloat16)

    column = lax.broadcasted_iota(jnp.int32, (dim, PAD), 1)
    if fused:
        for row in range(n_rows):
            edge = edges[row]
            for buffer, new in zip(buffers, (k_new, v_new)):
                picked = jnp.sum(jnp.where(column == row, new, 0.0), axis=1, keepdims=True)
                tile = jnp.broadcast_to(picked, (dim, LANES)).astype(buffer.dtype)
                for unit in range(keys_ref.shape[-1] // LANES):
                    if not sliding and unit < 2 * HALF_UNITS:
                        continue
                    cols = slice(unit * LANES, (unit + 1) * LANES)
                    buffer[row, :, cols] = jnp.where(lane + unit * LANES == edge, tile, buffer[row, :, cols])
    else:
        start(up_copies[2])
        each_variant(lambda copy: copy.wait())
        wait(unit_copies)
        for row in range(n_rows):
            edge = edges[row]
            border = edge // LANES
            cols = pl.ds(pl.multiple_of(border * LANES, LANES), LANES)
            slot = lane + border * LANES
            before = [buffer[row, :, cols] for buffer in buffers]
            if sliding:
                for half in range(2):
                    begin, count, base = listed[row][half]

                    def place_unit(unit, carry, half=half, begin=begin, base=base):
                        to = pl.ds(pl.multiple_of(unit * LANES, LANES), LANES)
                        for kind, buffer in enumerate(buffers):
                            buffer[row, :, to] = units_ref[half, kind, base + unit - begin]
                        return carry

                    lax.fori_loop(begin, begin + count, place_unit, 0)
                border_half = border // HALF_UNITS
                border_base = jnp.where(border_half == 0, listed[row][0][2] - listed[row][0][0], listed[row][1][2] - listed[row][1][0])
                border_place = jnp.clip(border_base + border, 0, MAX_UNITS - 1)
                keep = jnp.logical_xor(slot < edge, chip == 0)
            else:
                def clear_unit(unit, carry):
                    to = pl.ds(pl.multiple_of(unit * LANES, LANES), LANES)
                    for buffer in buffers:
                        buffer[row, :, to] = jnp.zeros((dim, LANES), buffer.dtype)
                    return carry

                lax.fori_loop(border + 1, 4 * HALF_UNITS, clear_unit, 0)
                keep = slot < edge
            for kind, (buffer, new) in enumerate(zip(buffers, (k_new, v_new))):
                picked = jnp.sum(jnp.where(column == row, new, 0.0), axis=1, keepdims=True)
                if sliding:
                    remote = units_ref[border_half, kind, border_place].astype(jnp.float32)
                else:
                    remote = jnp.zeros((dim, LANES), jnp.float32)
                merged = jnp.where(keep, before[kind].astype(jnp.float32), remote)
                merged = jnp.where(slot == edge, jnp.broadcast_to(picked, (dim, LANES)), merged)
                buffer[row, :, cols] = merged.astype(buffer.dtype)
        start(up_copies[3])
    out_copies = []
    for kind, (buffer, kept) in enumerate(zip(buffers, (keys_hbm, values_hbm))):
        target = kept.at[0] if layer == 0 else kept
        out_copies.append(pltpu.make_async_copy(buffer, target, out_sem.at[kind]))
    start(out_copies)
    mixed = []
    for row in range(n_rows):
        edge = edges[row]
        scores = jnp.dot(head_q[heads * row:heads * (row + 1)], keys_ref[row], preferred_element_type=jnp.float32) * dim ** -0.5
        if not sliding:
            position = lax.broadcasted_iota(jnp.int32, scores.shape, 1)
            scores = jnp.where(position <= edge, scores, -1e30)
        top = jnp.max(scores, axis=-1, keepdims=True)
        raised = jnp.exp(scores - top)
        weights = (raised / jnp.sum(raised, axis=-1, keepdims=True)).astype(jnp.bfloat16)
        mixed.append(lax.dot_general(weights, values_ref[row], nt, preferred_element_type=jnp.float32))
    both = jnp.concatenate(mixed, axis=0).astype(jnp.bfloat16)
    wide = jnp.dot(both, pick, preferred_element_type=jnp.float32)
    wide = jnp.where(own_head, wide, 0.0).astype(jnp.bfloat16)

    if not fused:
        start([out_weight])
        start(down_copies)
    gate = jnp.zeros((PAD, hidden), jnp.float32)
    raise_ = jnp.zeros((PAD, hidden), jnp.float32)
    for part in range(K_STEPS):
        wait(up_copies[part])
        rows = slice(part * k_len, (part + 1) * k_len)
        gate = gate + jnp.dot(normed[:, rows], wg_ref[rows], preferred_element_type=jnp.float32)
        raise_ = raise_ + jnp.dot(normed[:, rows], wu_ref[rows], preferred_element_type=jnp.float32)
    active = (gate * jax.nn.sigmoid(gate) * raise_).astype(jnp.bfloat16)

    wait([out_weight])
    product = jnp.dot(wide, wo_ref[...], preferred_element_type=jnp.float32)
    sums = jnp.concatenate([jnp.sum(product[heads * r:heads * (r + 1)], axis=0, keepdims=True) for r in range(n_rows)], axis=0)
    total = jnp.zeros((PAD, model), jnp.float32)
    for copy, (first, size) in zip(down_copies, down_cuts):
        copy.wait()
        total = total + jnp.dot(active[:, first:first + size], wd_ref[first:first + size], preferred_element_type=jnp.float32)
    out_ref[...] = sums + total[:n_rows]
    wait(out_copies)


def layer_call(layer, sliding, lengths, h, gain, tables, w_query, wk_t, wv_t, w_out, w_gate, w_up, w_down, k_t, v_t, partner, far, part=None, n_tp=0):
    n_rows, model = h.shape
    q_width = w_query.shape[2]
    dim = wk_t.shape[1]
    hidden = w_gate.shape[2]
    half_len = k_t.shape[-1]
    in_vmem = pl.BlockSpec(memory_space=pltpu.VMEM)
    anywhere = pl.BlockSpec(memory_space=pl.ANY)
    total = (2 if sliding else 4) * half_len
    kept = (3, n_rows, dim, total) if layer == 0 else (n_rows, dim, total)
    kept_shape = jax.ShapeDtypeStruct(kept, k_t.dtype)
    args = [lengths, h, gain, *tables, w_query, wk_t, wv_t, w_gate, w_up, w_down, w_out, k_t, v_t, partner, *far]
    in_specs = [pl.BlockSpec(memory_space=pltpu.SMEM)] + [in_vmem] * 6 + [anywhere] * (10 + len(far))
    fused = part is not None
    if fused:
        args.append(part)
        in_specs.append(in_vmem)
    n_small = 2 if fused else 1
    weight_bytes = 2 * (2 * model * q_width + 2 * dim * model + 3 * model * hidden)
    units = (2, 2, MAX_UNITS, dim, LANES) if sliding else (8, LANES)
    n_weight = 4 + 2 * K_STEPS + -(-hidden // DOWN_ROWS)
    row_shape = jax.ShapeDtypeStruct((n_rows, model), jnp.float32)
    if fused:
        remote = [pltpu.VMEM((n_tp, n_rows, model), jnp.float32), pltpu.SemaphoreType.DMA((n_tp - 1,)), pltpu.SemaphoreType.DMA((n_tp - 1,))]
        params = pltpu.CompilerParams(vmem_limit_bytes=VMEM_GRANT, collective_id=40 + layer, has_side_effects=True)
    else:
        remote = []
        params = pltpu.CompilerParams(vmem_limit_bytes=VMEM_GRANT)
    return pl.pallas_call(
        functools.partial(layer_kernel, layer, sliding, len(far), n_tp if fused else 0),
        in_specs=in_specs, out_specs=(in_vmem,) * n_small + (anywhere, anywhere),
        scratch_shapes=[
            pltpu.VMEM((model, q_width), jnp.bfloat16),
            pltpu.VMEM((dim, model), jnp.bfloat16),
            pltpu.VMEM((dim, model), jnp.bfloat16),
            pltpu.VMEM((model, hidden), jnp.bfloat16),
            pltpu.VMEM((model, hidden), jnp.bfloat16),
            pltpu.VMEM((hidden, model), jnp.bfloat16),
            pltpu.VMEM((q_width, model), jnp.bfloat16),
            pltpu.VMEM((n_rows, dim, total), jnp.bfloat16),
            pltpu.VMEM((n_rows, dim, total), jnp.bfloat16),
            pltpu.VMEM(units, jnp.bfloat16),
            pltpu.SemaphoreType.DMA((n_weight,)),
            pltpu.SemaphoreType.DMA((12,)),
            pltpu.SemaphoreType.DMA((2,)),
        ] + remote,
        out_shape=(row_shape,) * n_small + (kept_shape, kept_shape),
        compiler_params=params,
        cost_estimate=pl.CostEstimate(flops=PAD * weight_bytes, bytes_accessed=weight_bytes, transcendentals=0),
        name="layer_%d" % layer,
    )(*args)


def rotary_tables(positions, dim, heads):
    half = dim // 2
    low, high = positions[0].astype(jnp.float32), positions[1].astype(jnp.float32)

    def angles(feature, row):
        inv_freq = 1.0 / (ROPE_BASE ** (feature.astype(jnp.float32) * 2.0 / dim))
        return jnp.where(row == 0, low, high) * inv_freq

    wide = (8, heads * dim)
    lane = lax.broadcasted_iota(jnp.int32, wide, 1)
    turn = angles(lane % half, lax.broadcasted_iota(jnp.int32, wide, 0))
    tall = (half, PAD)
    turn_t = angles(lax.broadcasted_iota(jnp.int32, tall, 0), lax.broadcasted_iota(jnp.int32, tall, 1))
    return jnp.cos(turn), jnp.where(lane % dim < half, -jnp.sin(turn), jnp.sin(turn)), jnp.cos(turn_t), jnp.sin(turn_t)


def sum_kernel(n_tp, part_ref, resid_ref, out_ref, slots, send_sem, recv_sem):
    me = lax.axis_index("tp")
    barrier = pltpu.get_barrier_semaphore()
    for flip in range(1, n_tp):
        pl.semaphore_signal(barrier, inc=1, device_id={"tp": me ^ flip}, device_id_type=MESH_ID)
    pl.semaphore_wait(barrier, n_tp - 1)
    copies = []
    for flip in range(1, n_tp):
        copy = pltpu.make_async_remote_copy(
            src_ref=part_ref, dst_ref=slots.at[me], send_sem=send_sem.at[flip - 1], recv_sem=recv_sem.at[flip - 1],
            device_id={"tp": me ^ flip}, device_id_type=MESH_ID)
        copy.start()
        copies.append(copy)
    slots[me] = part_ref[...]
    for copy in copies:
        copy.wait()
    total = slots[0]
    for index in range(1, n_tp):
        total = total + slots[index]
    out_ref[...] = (resid_ref[...] + total).astype(jnp.bfloat16)


def sum_call(part, resid, n_tp):
    return pl.pallas_call(
        functools.partial(sum_kernel, n_tp),
        out_shape=jax.ShapeDtypeStruct(part.shape, jnp.bfloat16),
        in_specs=[pl.BlockSpec(memory_space=pltpu.VMEM)] * 2,
        out_specs=pl.BlockSpec(memory_space=pltpu.VMEM),
        scratch_shapes=[
            pltpu.VMEM((n_tp,) + part.shape, jnp.float32),
            pltpu.SemaphoreType.DMA((n_tp - 1,)),
            pltpu.SemaphoreType.DMA((n_tp - 1,)),
        ],
        compiler_params=pltpu.CompilerParams(collective_id=0, has_side_effects=True),
        name="sum_tp",
    )(part, resid)


LANES = 128
HALF_UNITS = 16
CHIP_ROWS = 4
MAX_UNITS = CHIP_ROWS * HALF_UNITS
HEAVY_LEVELS = (32, 40, 44, 48, 52, 56, 60, 64)
LIGHT_LEVELS = (8, 16, 20, 24, 28, 32, 36, 40, 44, 48, 56, 64)


def row_units(edge, half, from_upper):
    low = half * HALF_UNITS
    upper_end = jnp.clip((edge + LANES - 1) // LANES, low, low + HALF_UNITS)
    lower_start = jnp.clip((edge + 1) // LANES, low, low + HALF_UNITS)
    start = jnp.where(from_upper, low, lower_start)
    count = jnp.where(from_upper, upper_end - low, low + HALF_UNITS - lower_start)
    return start, count


def list_of(lengths_ref, chip, half):
    base = jnp.int32(0)
    found = []
    for row in range(CHIP_ROWS):
        start, count = row_units(lengths_ref[CHIP_ROWS * chip + row] - WINDOW, half, chip == 0)
        found.append((start, count, base))
        base = base + count
    return found, base


def pack_kernel(n_packed, lengths_ref, other_ref, k_ref, v_ref, out_ref, level_ref, across_ref, diagonal_ref):
    me = lax.axis_index("sp")
    core = me % 2
    chip = me // 2
    layer = pl.program_id(0)

    @pl.when(layer == 0)
    def _():
        for place, (levels, swap) in enumerate(((HEAVY_LEVELS, 0), (LIGHT_LEVELS, 1))):
            need = jnp.int32(0)
            for ref in (lengths_ref, other_ref):
                for target in range(2):
                    need = jnp.maximum(need, list_of(ref, target, target ^ swap)[1])
            index = jnp.int32(0)
            for level in levels[:-1]:
                index = index + jnp.where(need > level, 1, 0)
            level_ref[place] = index

    rows, _ = list_of(lengths_ref, 1 - chip, core)
    for row, (start, count, base) in enumerate(rows):
        first = start - core * HALF_UNITS
        for unit in range(HALF_UNITS):
            @pl.when(jnp.logical_and(layer < n_packed, jnp.logical_and(unit >= first, unit < first + count)))
            def _():
                place = base + unit - first
                cols = pl.ds(unit * LANES, LANES)
                out_ref[0, 0, place] = k_ref[0, row, :, cols]
                out_ref[0, 1, place] = v_ref[0, row, :, cols]

    @pl.when(layer == n_packed)
    def _():
        pair = CHIP_ROWS // 2
        for kind, ref in enumerate((k_ref, v_ref)):
            across_ref[kind] = ref[0, pl.ds(pair * core, pair)]
            diagonal_ref[kind] = ref[0, pl.ds(pair * (1 - core), pair)]


def pack_call(lengths, other, k_t, v_t, n_layers):
    dim, half_len = k_t.shape[2:]
    whole_shape = (2, CHIP_ROWS // 2, dim, half_len)
    whole = pl.BlockSpec(whole_shape, lambda l: (0, 0, 0, 0))
    block = pl.BlockSpec((1, CHIP_ROWS, dim, half_len), lambda l: (l, 1 - lax.axis_index("sp") // 2, 0, 0))
    small = pl.BlockSpec(memory_space=pltpu.SMEM)
    return pl.pallas_call(
        functools.partial(pack_kernel, n_layers),
        grid=(n_layers + 1,), in_specs=[small, small, block, block],
        out_specs=(pl.BlockSpec((1, 2, MAX_UNITS, dim, LANES), lambda l: (jnp.minimum(l, n_layers - 1), 0, 0, 0, 0)), small, whole, whole),
        out_shape=(
            jax.ShapeDtypeStruct((n_layers, 2, MAX_UNITS, dim, LANES), k_t.dtype), jax.ShapeDtypeStruct((2,), jnp.int32),
            jax.ShapeDtypeStruct(whole_shape, k_t.dtype), jax.ShapeDtypeStruct(whole_shape, k_t.dtype)),
        compiler_params=pltpu.CompilerParams(dimension_semantics=("arbitrary",), vmem_limit_bytes=VMEM_GRANT),
        name="pack_units",
    )(lengths, other, k_t, v_t)


def send_kernel(heavy, n_units, packed_ref, k_ref, v_ref, *rest):
    if heavy:
        got_ref, partner_ref, send_sem, recv_sem, fsend_sem, frecv_sem, psend_sem, precv_sem = rest
        phase = 0
    else:
        _, got_ref, send_sem, recv_sem, fsend_sem, frecv_sem = rest
        phase = 1
    me = lax.axis_index("sp")
    middle = jnp.logical_or(me == 1, me == 2)
    sender = middle if heavy else jnp.logical_not(middle)
    across = (me + 2) % 4
    partner = me + 1 - 2 * (me % 2)
    n_layers = packed_ref.shape[0]
    barrier = pltpu.get_barrier_semaphore()
    for peer in (across, partner):
        pl.semaphore_signal(barrier, inc=1, device_id={"sp": peer}, device_id_type=MESH_ID)
    pl.semaphore_wait(barrier, 2)
    direct = []
    onward = []
    for layer in range(n_layers):
        for kind in range(2):
            index = layer * 2 + kind
            part = pl.ds(0, n_units)
            target = got_ref.at[phase, layer, kind, part]
            direct.append(pltpu.make_async_remote_copy(
                src_ref=packed_ref.at[layer, kind, part], dst_ref=target, send_sem=send_sem.at[index], recv_sem=recv_sem.at[index],
                device_id={"sp": across}, device_id_type=MESH_ID))
            onward.append(pltpu.make_async_remote_copy(
                src_ref=target, dst_ref=target, send_sem=fsend_sem.at[index], recv_sem=frecv_sem.at[index],
                device_id={"sp": partner}, device_id_type=MESH_ID))

    @pl.when(sender)
    def _():
        for copy in direct:
            copy.start()

    shares = []
    if heavy:
        rows = partner_ref.shape[2]
        for kind, source in enumerate((k_ref, v_ref)):
            for layer in range(source.shape[0]):
                index = layer * 2 + kind
                shares.append(pltpu.make_async_remote_copy(
                    src_ref=source.at[layer, pl.ds(rows * partner, rows)], dst_ref=partner_ref.at[kind, layer],
                    send_sem=psend_sem.at[index], recv_sem=precv_sem.at[index],
                    device_id={"sp": partner}, device_id_type=MESH_ID))
        for copy in shares:
            copy.start()

    @pl.when(jnp.logical_not(sender))
    def _():
        for near, far in zip(direct, onward):
            near.wait_recv()
            far.start()
        for far in onward:
            far.wait_send()

    @pl.when(sender)
    def _():
        for near, far in zip(direct, onward):
            near.wait_send()
            far.wait_recv()

    for copy in shares:
        copy.wait()


def send_call(heavy, n_units, slot, packed, k_t, v_t, got=None):
    n_layers = packed.shape[0]
    n_copies = 2 * n_layers
    anywhere = pl.BlockSpec(memory_space=pl.ANY)
    got_shape = jax.ShapeDtypeStruct((2,) + packed.shape, packed.dtype)
    sems = [pltpu.SemaphoreType.DMA((n_copies,)) for _ in range(4)]
    if heavy:
        args = (packed, k_t, v_t)
        rows = k_t.shape[1] // 4
        out_shape = (got_shape, jax.ShapeDtypeStruct((2, k_t.shape[0], rows) + k_t.shape[2:], k_t.dtype))
        sems += [pltpu.SemaphoreType.DMA((2 * k_t.shape[0],)) for _ in range(2)]
        aliases = {}
        out_specs = (anywhere, anywhere)
    else:
        args = (packed, k_t, v_t, got)
        out_shape = got_shape
        aliases = {3: 0}
        out_specs = anywhere
    return pl.pallas_call(
        functools.partial(send_kernel, heavy, n_units),
        out_shape=out_shape, in_specs=[anywhere] * len(args), out_specs=out_specs, scratch_shapes=sems,
        input_output_aliases=aliases,
        compiler_params=pltpu.CompilerParams(collective_id=slot, has_side_effects=True),
        name="send_%s_%d" % ("heavy" if heavy else "light", n_units),
    )(*args)


def gather_kernel(n_window, *refs):
    sources, targets = refs[:6], refs[8:12]
    stage, in_sem, out_sem = refs[12:15], refs[15], refs[16]
    windows = [(sources[2 * i + kind], targets[kind].at[1 + i], 2 * i + kind) for i in range(n_window) for kind in range(2)]
    globals_ = [(sources[2 * n_window + kind], targets[2 + kind], 2 * n_window + kind) for kind in range(2)]
    moves = []
    for source, target, place in windows + globals_:
        held = stage[0].at[place] if place < 2 * n_window else stage[1 + place - 2 * n_window]
        moves.append((pltpu.make_async_copy(source, held, in_sem.at[place]), pltpu.make_async_copy(held, target, out_sem.at[place])))
    for bring, _ in moves:
        bring.start()
    for bring, send in moves:
        bring.wait()
        send.start()
    for _, send in moves:
        send.wait()


def gather_call(stacked, windows, globals_):
    n_window = len(windows)
    anywhere = pl.BlockSpec(memory_space=pl.ANY)
    args = [array for pair in windows for array in pair] + list(globals_) + list(stacked)
    window = windows[0][0]
    whole = globals_[0]
    return pl.pallas_call(
        functools.partial(gather_kernel, n_window),
        in_specs=[anywhere] * len(args), out_specs=(anywhere,) * 4,
        out_shape=tuple(jax.ShapeDtypeStruct(a.shape, a.dtype) for a in (*stacked, *globals_)),
        scratch_shapes=[
            pltpu.VMEM((2 * n_window,) + window.shape, window.dtype), pltpu.VMEM(whole.shape, whole.dtype), pltpu.VMEM(whole.shape, whole.dtype),
            pltpu.SemaphoreType.DMA((2 * n_window + 2,)), pltpu.SemaphoreType.DMA((2 * n_window + 2,))],
        input_output_aliases={2 * n_window + 2: 0, 2 * n_window + 3: 1},
        compiler_params=pltpu.CompilerParams(vmem_limit_bytes=VMEM_GRANT),
        name="gather_rows",
    )(*args)


def solution(mesh):
    cache_spec = P(None, "dp", "tp", "sp", None)
    row_spec = P(("dp", "sp"), None)
    col_spec = P(None, None, "tp")
    inner_spec = P(None, "tp", None)
    window_spec = P(None, ("dp", "sp"), "tp", None, None)
    global_spec = P(("dp", "sp"), "tp", None, None)
    in_specs = (cache_spec, cache_spec, P("dp"), row_spec, P(None, None), col_spec, col_spec, col_spec, inner_spec, col_spec, col_spec, inner_spec)
    out_specs = (row_spec, window_spec, window_spec, global_spec, global_spec)

    def device_step(k_cache, v_cache, lengths, hidden, ln_gain, w_query, w_key, w_value, w_out, w_gate, w_up, w_down):
        n_layers = w_query.shape[0]
        rows_dev = hidden.shape[0]
        head_dim = k_cache.shape[-1]
        n_tp = mesh.shape["tp"]
        me = lax.axis_index("sp")
        my_lengths = lax.dynamic_slice_in_dim(lengths, me * rows_dev, rows_dev)
        k_t = k_cache[:, :, 0].swapaxes(-1, -2)
        v_t = v_cache[:, :, 0].swapaxes(-1, -2)
        last = n_layers - 1

        other = lax.ppermute(lengths, "dp", [(0, 1), (1, 0)])
        packed, levels, *whole_rows = pack_call(lengths, other, k_t, v_t, n_layers - 1)
        heavy_calls = [functools.partial(send_call, True, n, 1 + i) for i, n in enumerate(HEAVY_LEVELS)]
        light_calls = [functools.partial(send_call, False, n, 1 + len(HEAVY_LEVELS) + i) for i, n in enumerate(LIGHT_LEVELS)]
        got, partner = lax.switch(levels[0], heavy_calls, packed, k_t, v_t)
        got = lax.switch(levels[1], light_calls, packed, k_t, v_t, got)
        got, *whole_rows = lax.optimization_barrier((got, *whole_rows))
        whole_got = [lax.ppermute(rows, "sp", [(i, i ^ flip) for i in range(4)]) for flip, rows in zip((2, 3), whole_rows)]

        residual = hidden.astype(jnp.float32)
        tables = rotary_tables(my_lengths, head_dim, w_query.shape[2] // head_dim)
        wk_t = w_key.swapaxes(1, 2)
        wv_t = w_value.swapaxes(1, 2)
        rows_kept = []
        part = None
        for layer in range(n_layers):
            sliding = layer < last
            common = (residual, ln_gain[layer:layer + 1], tables, w_query, wk_t, wv_t, w_out, w_gate, w_up, w_down, k_t, v_t, partner)
            outside = [got] if sliding else whole_got
            result = layer_call(layer, sliding, lengths, *common, outside, part, n_tp)
            if part is not None:
                residual = result[1]
            part = result[0]
            rows_kept.append(result[-2:])
        residual = sum_call(part, residual, n_tp)

        def back(rows_t):
            return rows_t.swapaxes(-1, -2)

        win_k, win_v, all_k, all_v = gather_call(rows_kept[0], rows_kept[1:last], rows_kept[last])
        return residual, back(win_k)[:, :, None], back(win_v)[:, :, None], back(all_k)[:, None], back(all_v)[:, None]

    return jax.shard_map(device_step, mesh=mesh, in_specs=in_specs, out_specs=out_specs, check_vma=False)
```

```python
import functools

import jax
import jax.numpy as jnp
import numpy as np
from jax import lax
from jax.experimental import pallas as pl
from jax.experimental.pallas import tpu as pltpu
from jax.sharding import PartitionSpec as P

WINDOW = 4096
ROPE_BASE = 50000
NORM_EPS = 1e-5


PAD = 16
K_STEPS = 4
DOWN_ROWS = 384
MESH_ID = pl.DeviceIdType.MESH


VMEM_GRANT = 63 * 2 ** 20


def layer_kernel(layer, sliding, n_far, n_tp, lengths_ref, h_ref, gain_ref, cq_ref, sq_ref, ck_ref, sk_ref, *refs):
    wq_hbm, wk_hbm, wv_hbm, wg_hbm, wu_hbm, wd_hbm, wo_hbm, k_hbm, v_hbm, partner_hbm = refs[:10]
    far = refs[10:10 + n_far]
    fused = n_tp > 0
    final = not sliding
    if final:
        refs, (end_ref, end_slots, end_send, end_recv) = refs[:-4], refs[-4:]
    if fused:
        part_ref = refs[10 + n_far]
        (out_ref, h_out, keys_hbm, values_hbm, wq_ref, wk_ref, wv_ref, wg_ref, wu_ref, wd_ref, wo_ref, keys_ref, values_ref, units_ref,
         weight_sem, in_sem, out_sem, slots, send_sem, recv_sem) = refs[-20:]
    else:
        (out_ref, keys_hbm, values_hbm, wq_ref, wk_ref, wv_ref, wg_ref, wu_ref, wd_ref, wo_ref, keys_ref, values_ref, units_ref,
         weight_sem, in_sem, out_sem) = refs[-16:]
    n_rows, model = h_ref.shape
    dim = wk_ref.shape[0]
    q_width = wq_ref.shape[1]
    hidden = wg_ref.shape[1]
    heads = q_width // dim
    half_len = k_hbm.shape[-1]
    me = lax.axis_index("sp")
    chip = me // 2
    first_row = me * n_rows
    core = me % 2
    buffers = (keys_ref, values_ref)
    edges = [lengths_ref[first_row + row] - (WINDOW if sliding else 0) for row in range(n_rows)]
    listed = [[None] * 2 for _ in range(n_rows)]
    if sliding:
        for half in range(2):
            rows, _ = list_of(lengths_ref, chip, half)
            for row in range(n_rows):
                listed[row][half] = [jnp.where(core == 0, one, two) for one, two in zip(rows[row], rows[n_rows + row])]

    def cache_copies(index):
        found = []
        pieces = 2 if sliding else 4
        for kind, (source, buffer) in enumerate(zip((k_hbm, v_hbm), buffers)):
            for piece in range(pieces):
                place = pl.ds(piece * half_len, half_len)
                who = piece ^ (index % 2) if sliding else piece ^ index
                if who == 0:
                    origin = source.at[layer, pl.ds(first_row, n_rows)]
                elif who == 1:
                    origin = partner_hbm.at[kind, layer]
                else:
                    origin = far[who - 2].at[kind]
                found.append(pltpu.make_async_copy(origin, buffer.at[:, :, place], in_sem.at[kind * 4 + piece]))
        return found

    variants = 2 if sliding else 4
    which = me % variants

    def each_variant(act):
        for index in range(variants):
            @pl.when(which == index)
            def _():
                for copy in cache_copies(index):
                    act(copy)

    unit_copies = []
    if sliding:
        for half in range(2):
            for kind in range(2):
                unit_copies.append(pltpu.make_async_copy(
                    far[0].at[(chip + half) % 2, layer, kind], units_ref.at[half, kind], in_sem.at[8 + half * 2 + kind]))

    n_sem = [0]

    def weight_copy(source, target, first, size):
        rows = pl.ds(first, size)
        copy = pltpu.make_async_copy(source.at[layer, rows], target.at[rows], weight_sem.at[n_sem[0]])
        n_sem[0] += 1
        return copy

    k_len = model // K_STEPS
    down_cuts = [(first, min(DOWN_ROWS, hidden - first)) for first in range(0, hidden, DOWN_ROWS)]
    proj_copies = [weight_copy(wq_hbm, wq_ref, 0, model), weight_copy(wk_hbm, wk_ref, 0, dim), weight_copy(wv_hbm, wv_ref, 0, dim)]
    up_copies = [[weight_copy(wg_hbm, wg_ref, part * k_len, k_len), weight_copy(wu_hbm, wu_ref, part * k_len, k_len)] for part in range(K_STEPS)]
    out_weight = weight_copy(wo_hbm, wo_ref, 0, q_width)
    down_copies = [weight_copy(wd_hbm, wd_ref, first, size) for first, size in down_cuts]

    def start(copies):
        for copy in copies:
            copy.start()

    def wait(copies):
        for copy in copies:
            copy.wait()

    lane = lax.broadcasted_iota(jnp.int32, (dim, LANES), 1)
    if fused:
        here = lax.axis_index("tp")
        barrier = pltpu.get_barrier_semaphore()
        for flip in range(1, n_tp):
            pl.semaphore_signal(barrier, inc=1, device_id={"tp": here ^ flip}, device_id_type=MESH_ID)
    start(proj_copies)
    each_variant(lambda copy: copy.start())
    start(unit_copies)
    if fused:
        pl.semaphore_wait(barrier, n_tp - 1)
        shares = []
        for flip in range(1, n_tp):
            shares.append(pltpu.make_async_remote_copy(
                src_ref=part_ref, dst_ref=slots.at[here], send_sem=send_sem.at[flip - 1], recv_sem=recv_sem.at[flip - 1],
                device_id={"tp": here ^ flip}, device_id_type=MESH_ID))
        start(shares)
        for copies in up_copies:
            start(copies)
        start([out_weight])
        start(down_copies)
        slots[here] = part_ref[...]
    else:
        for copies in up_copies[:2]:
            start(copies)
    if fused:
        each_variant(lambda copy: copy.wait())
        wait(unit_copies)
        for row in range(n_rows):
            edge = edges[row]
            for unit in range(keys_ref.shape[-1] // LANES):
                slot = lane + unit * LANES
                cols = slice(unit * LANES, (unit + 1) * LANES)
                half = unit // HALF_UNITS
                if sliding:
                    begin, _, base = listed[row][half]
                    keep = jnp.logical_xor(slot < edge, chip == 0)
                    place = jnp.clip(base + unit - begin, 0, MAX_UNITS - 1)
                elif unit < 2 * HALF_UNITS:
                    continue
                else:
                    keep = slot < edge
                for kind, buffer in enumerate(buffers):
                    if not sliding:
                        remote = jnp.zeros((dim, LANES), buffer.dtype)
                    else:
                        remote = units_ref[half, kind, place]
                    buffer[row, :, cols] = jnp.where(keep, buffer[row, :, cols], remote)
        wait(shares)
        total = slots[0]
        for index in range(1, n_tp):
            total = total + slots[index]
        rows32 = (h_ref[...].astype(jnp.float32) + total).astype(jnp.bfloat16).astype(jnp.float32)
        h_out[...] = rows32
    else:
        rows32 = h_ref[...].astype(jnp.float32)
    centered = rows32 - jnp.mean(rows32, axis=-1, keepdims=True)
    variance = jnp.mean(centered * centered, axis=-1, keepdims=True)
    scaled = centered * lax.rsqrt(variance + NORM_EPS)
    normed = scaled * gain_ref[layer:layer + 1].astype(jnp.float32)
    normed = jnp.concatenate([normed, jnp.zeros((PAD - n_rows, model), jnp.float32)], axis=0).astype(jnp.bfloat16)

    nt = (((1,), (1,)), ((), ()))
    wait(proj_copies)
    query = jnp.dot(normed, wq_ref[...], preferred_element_type=jnp.float32)[:n_rows]
    k_new = lax.dot_general(wk_ref[...], normed, nt, preferred_element_type=jnp.float32)
    v_new = lax.dot_general(wv_ref[...], normed, nt, preferred_element_type=jnp.float32)
    if sliding:
        q_lane = lax.broadcasted_iota(jnp.int32, query.shape, 1)
        swapped = jnp.where(q_lane % dim < dim // 2, pltpu.roll(query, q_width - dim // 2, 1), pltpu.roll(query, dim // 2, 1))
        query = query * cq_ref[...] + swapped * sq_ref[...]
        first = k_new[:dim // 2]
        second = k_new[dim // 2:]
        cosine = ck_ref[...]
        sine = sk_ref[...]
        k_new = jnp.concatenate([first * cosine - second * sine, second * cosine + first * sine], axis=0)
    k_new = k_new.astype(jnp.bfloat16).astype(jnp.float32)
    v_new = v_new.astype(jnp.bfloat16).astype(jnp.float32)
    spread = [jnp.broadcast_to(query[r:r + 1], (heads, q_width)) for r in range(n_rows)]
    spread = jnp.concatenate(spread, axis=0)
    at_row = lax.broadcasted_iota(jnp.int32, spread.shape, 0)
    at_col = lax.broadcasted_iota(jnp.int32, spread.shape, 1)
    own_head = at_col // dim == at_row % heads
    masked = jnp.where(own_head, spread, 0.0).astype(jnp.bfloat16)
    pick_row = lax.broadcasted_iota(jnp.int32, (dim, q_width), 0)
    pick_col = lax.broadcasted_iota(jnp.int32, (dim, q_width), 1)
    pick = jnp.where(pick_col % dim == pick_row, 1.0, 0.0).astype(jnp.bfloat16)
    head_q = lax.dot_general(masked, pick, nt, preferred_element_type=jnp.float32).astype(jnp.bfloat16)

    column = lax.broadcasted_iota(jnp.int32, (dim, PAD), 1)
    if fused:
        for row in range(n_rows):
            edge = edges[row]
            for buffer, new in zip(buffers, (k_new, v_new)):
                picked = jnp.sum(jnp.where(column == row, new, 0.0), axis=1, keepdims=True)
                tile = jnp.broadcast_to(picked, (dim, LANES)).astype(buffer.dtype)
                for unit in range(keys_ref.shape[-1] // LANES):
                    if not sliding and unit < 2 * HALF_UNITS:
                        continue
                    cols = slice(unit * LANES, (unit + 1) * LANES)
                    buffer[row, :, cols] = jnp.where(lane + unit * LANES == edge, tile, buffer[row, :, cols])
    else:
        start(up_copies[2])
        each_variant(lambda copy: copy.wait())
        wait(unit_copies)
        for row in range(n_rows):
            edge = edges[row]
            border = edge // LANES
            cols = pl.ds(pl.multiple_of(border * LANES, LANES), LANES)
            slot = lane + border * LANES
            before = [buffer[row, :, cols] for buffer in buffers]
            if sliding:
                for half in range(2):
                    begin, count, base = listed[row][half]

                    def place_unit(unit, carry, half=half, begin=begin, base=base):
                        to = pl.ds(pl.multiple_of(unit * LANES, LANES), LANES)
                        for kind, buffer in enumerate(buffers):
                            buffer[row, :, to] = units_ref[half, kind, base + unit - begin]
                        return carry

                    lax.fori_loop(begin, begin + count, place_unit, 0)
                border_half = border // HALF_UNITS
                border_base = jnp.where(border_half == 0, listed[row][0][2] - listed[row][0][0], listed[row][1][2] - listed[row][1][0])
                border_place = jnp.clip(border_base + border, 0, MAX_UNITS - 1)
                keep = jnp.logical_xor(slot < edge, chip == 0)
            else:
                def clear_unit(unit, carry):
                    to = pl.ds(pl.multiple_of(unit * LANES, LANES), LANES)
                    for buffer in buffers:
                        buffer[row, :, to] = jnp.zeros((dim, LANES), buffer.dtype)
                    return carry

                lax.fori_loop(border + 1, 4 * HALF_UNITS, clear_unit, 0)
                keep = slot < edge
            for kind, (buffer, new) in enumerate(zip(buffers, (k_new, v_new))):
                picked = jnp.sum(jnp.where(column == row, new, 0.0), axis=1, keepdims=True)
                if sliding:
                    remote = units_ref[border_half, kind, border_place].astype(jnp.float32)
                else:
                    remote = jnp.zeros((dim, LANES), jnp.float32)
                merged = jnp.where(keep, before[kind].astype(jnp.float32), remote)
                merged = jnp.where(slot == edge, jnp.broadcast_to(picked, (dim, LANES)), merged)
                buffer[row, :, cols] = merged.astype(buffer.dtype)
        start(up_copies[3])
    out_copies = []
    for kind, (buffer, kept) in enumerate(zip(buffers, (keys_hbm, values_hbm))):
        target = kept.at[0] if layer == 0 else kept
        out_copies.append(pltpu.make_async_copy(buffer, target, out_sem.at[kind]))
    start(out_copies)
    mixed = []
    for row in range(n_rows):
        edge = edges[row]
        scores = jnp.dot(head_q[heads * row:heads * (row + 1)], keys_ref[row], preferred_element_type=jnp.float32) * dim ** -0.5
        if not sliding:
            position = lax.broadcasted_iota(jnp.int32, scores.shape, 1)
            scores = jnp.where(position <= edge, scores, -1e30)
        top = jnp.max(scores, axis=-1, keepdims=True)
        raised = jnp.exp(scores - top)
        weights = (raised / jnp.sum(raised, axis=-1, keepdims=True)).astype(jnp.bfloat16)
        mixed.append(lax.dot_general(weights, values_ref[row], nt, preferred_element_type=jnp.float32))
    both = jnp.concatenate(mixed, axis=0).astype(jnp.bfloat16)
    wide = jnp.dot(both, pick, preferred_element_type=jnp.float32)
    wide = jnp.where(own_head, wide, 0.0).astype(jnp.bfloat16)

    if not fused:
        start([out_weight])
        start(down_copies)
    gate = jnp.zeros((PAD, hidden), jnp.float32)
    raise_ = jnp.zeros((PAD, hidden), jnp.float32)
    for part in range(K_STEPS):
        wait(up_copies[part])
        rows = slice(part * k_len, (part + 1) * k_len)
        gate = gate + jnp.dot(normed[:, rows], wg_ref[rows], preferred_element_type=jnp.float32)
        raise_ = raise_ + jnp.dot(normed[:, rows], wu_ref[rows], preferred_element_type=jnp.float32)
    active = (gate * jax.nn.sigmoid(gate) * raise_).astype(jnp.bfloat16)

    wait([out_weight])
    product = jnp.dot(wide, wo_ref[...], preferred_element_type=jnp.float32)
    sums = jnp.concatenate([jnp.sum(product[heads * r:heads * (r + 1)], axis=0, keepdims=True) for r in range(n_rows)], axis=0)
    total = jnp.zeros((PAD, model), jnp.float32)
    for copy, (first, size) in zip(down_copies, down_cuts):
        copy.wait()
        total = total + jnp.dot(active[:, first:first + size], wd_ref[first:first + size], preferred_element_type=jnp.float32)
    if final:
        end_ref[...] = sums + total[:n_rows]
        wait(out_copies)
        ends = []
        for flip in range(1, n_tp):
            ends.append(pltpu.make_async_remote_copy(
                src_ref=end_ref, dst_ref=end_slots.at[here], send_sem=end_send.at[flip - 1], recv_sem=end_recv.at[flip - 1],
                device_id={"tp": here ^ flip}, device_id_type=MESH_ID))
        start(ends)
        end_slots[here] = end_ref[...]
        wait(ends)
        total = end_slots[0]
        for index in range(1, n_tp):
            total = total + end_slots[index]
        out_ref[...] = (rows32 + total).astype(out_ref.dtype)
    else:
        out_ref[...] = sums + total[:n_rows]
        wait(out_copies)


def layer_call(layer, sliding, lengths, h, gain, tables, w_query, wk_t, wv_t, w_out, w_gate, w_up, w_down, k_t, v_t, partner, far, part=None, n_tp=0):
    n_rows, model = h.shape
    q_width = w_query.shape[2]
    dim = wk_t.shape[1]
    hidden = w_gate.shape[2]
    half_len = k_t.shape[-1]
    in_vmem = pl.BlockSpec(memory_space=pltpu.VMEM)
    anywhere = pl.BlockSpec(memory_space=pl.ANY)
    total = (2 if sliding else 4) * half_len
    kept = (3, n_rows, dim, total) if layer == 0 else (n_rows, dim, total)
    kept_shape = jax.ShapeDtypeStruct(kept, k_t.dtype)
    args = [lengths, h, gain, *tables, w_query, wk_t, wv_t, w_gate, w_up, w_down, w_out, k_t, v_t, partner, *far]
    in_specs = [pl.BlockSpec(memory_space=pltpu.SMEM)] + [in_vmem] * 6 + [anywhere] * (10 + len(far))
    fused = part is not None
    if fused:
        args.append(part)
        in_specs.append(in_vmem)
    n_small = 2 if fused else 1
    weight_bytes = 2 * (2 * model * q_width + 2 * dim * model + 3 * model * hidden)
    units = (2, 2, MAX_UNITS, dim, LANES) if sliding else (8, LANES)
    n_weight = 4 + 2 * K_STEPS + -(-hidden // DOWN_ROWS)
    row_shape = jax.ShapeDtypeStruct((n_rows, model), jnp.float32)
    first_shape = row_shape
    if fused:
        remote = [pltpu.VMEM((n_tp, n_rows, model), jnp.float32), pltpu.SemaphoreType.DMA((n_tp - 1,)), pltpu.SemaphoreType.DMA((n_tp - 1,))]
        if not sliding:
            remote = remote + [pltpu.VMEM((n_rows, model), jnp.float32)] + remote
            first_shape = jax.ShapeDtypeStruct((n_rows, model), jnp.bfloat16)
        params = pltpu.CompilerParams(vmem_limit_bytes=VMEM_GRANT, collective_id=40 + layer, has_side_effects=True)
    else:
        remote = []
        params = pltpu.CompilerParams(vmem_limit_bytes=VMEM_GRANT)
    return pl.pallas_call(
        functools.partial(layer_kernel, layer, sliding, len(far), n_tp if fused else 0),
        in_specs=in_specs, out_specs=(in_vmem,) * n_small + (anywhere, anywhere),
        scratch_shapes=[
            pltpu.VMEM((model, q_width), jnp.bfloat16),
            pltpu.VMEM((dim, model), jnp.bfloat16),
            pltpu.VMEM((dim, model), jnp.bfloat16),
            pltpu.VMEM((model, hidden), jnp.bfloat16),
            pltpu.VMEM((model, hidden), jnp.bfloat16),
            pltpu.VMEM((hidden, model), jnp.bfloat16),
            pltpu.VMEM((q_width, model), jnp.bfloat16),
            pltpu.VMEM((n_rows, dim, total), jnp.bfloat16),
            pltpu.VMEM((n_rows, dim, total), jnp.bfloat16),
            pltpu.VMEM(units, jnp.bfloat16),
            pltpu.SemaphoreType.DMA((n_weight,)),
            pltpu.SemaphoreType.DMA((12,)),
            pltpu.SemaphoreType.DMA((2,)),
        ] + remote,
        out_shape=(first_shape, row_shape)[:n_small] + (kept_shape, kept_shape),
        compiler_params=params,
        cost_estimate=pl.CostEstimate(flops=PAD * weight_bytes, bytes_accessed=weight_bytes, transcendentals=0),
        name="layer_%d" % layer,
    )(*args)


def rotary_tables(positions, dim, heads):
    half = dim // 2
    inv_freq = 1.0 / (float(ROPE_BASE) ** (np.arange(half) * 2.0 / dim))
    wide = np.tile(inv_freq, 2 * heads).astype(np.float32)
    sign = np.tile(np.repeat([-1.0, 1.0], half), heads).astype(np.float32)
    turn = positions.astype(jnp.float32)[:, None] * wide[None, :]
    padded = jnp.pad(positions, (0, PAD - positions.shape[0])).astype(jnp.float32)
    turn_t = inv_freq.astype(np.float32)[:, None] * padded[None, :]
    return jnp.cos(turn), jnp.sin(turn) * sign[None, :], jnp.cos(turn_t), jnp.sin(turn_t)


LANES = 128
HALF_UNITS = 16
CHIP_ROWS = 4
MAX_UNITS = CHIP_ROWS * HALF_UNITS
HEAVY_LEVELS = (28, 36, 40, 44, 46, 48, 50, 52, 54, 56, 58, 60, 62, 64)
LIGHT_LEVELS = (8, 16, 20, 24, 26, 28, 30, 32, 34, 36, 38, 40, 44, 48, 56, 64)


def row_units(edge, half, from_upper):
    low = half * HALF_UNITS
    upper_end = jnp.clip((edge + LANES - 1) // LANES, low, low + HALF_UNITS)
    lower_start = jnp.clip((edge + 1) // LANES, low, low + HALF_UNITS)
    start = jnp.where(from_upper, low, lower_start)
    count = jnp.where(from_upper, upper_end - low, low + HALF_UNITS - lower_start)
    return start, count


def list_of(lengths_ref, chip, half):
    base = jnp.int32(0)
    found = []
    for row in range(CHIP_ROWS):
        start, count = row_units(lengths_ref[CHIP_ROWS * chip + row] - WINDOW, half, chip == 0)
        found.append((start, count, base))
        base = base + count
    return found, base


def pack_kernel(n_packed, lengths_ref, other_ref, k_ref, v_ref, out_ref, level_ref, across_ref, diagonal_ref):
    me = lax.axis_index("sp")
    core = me % 2
    chip = me // 2
    layer = pl.program_id(0)

    @pl.when(layer == 0)
    def _():
        for place, (levels, swap) in enumerate(((HEAVY_LEVELS, 0), (LIGHT_LEVELS, 1))):
            need = jnp.int32(0)
            for ref in (lengths_ref, other_ref):
                for target in range(2):
                    need = jnp.maximum(need, list_of(ref, target, target ^ swap)[1])
            index = jnp.int32(0)
            for level in levels[:-1]:
                index = index + jnp.where(need > level, 1, 0)
            level_ref[place] = index

    rows, _ = list_of(lengths_ref, 1 - chip, core)
    for row, (start, count, base) in enumerate(rows):
        first = start - core * HALF_UNITS
        for unit in range(HALF_UNITS):
            @pl.when(jnp.logical_and(layer < n_packed, jnp.logical_and(unit >= first, unit < first + count)))
            def _():
                place = base + unit - first
                cols = pl.ds(unit * LANES, LANES)
                out_ref[0, 0, place] = k_ref[0, row, :, cols]
                out_ref[0, 1, place] = v_ref[0, row, :, cols]

    @pl.when(layer == n_packed)
    def _():
        pair = CHIP_ROWS // 2
        for kind, ref in enumerate((k_ref, v_ref)):
            across_ref[kind] = ref[0, pl.ds(pair * core, pair)]
            diagonal_ref[kind] = ref[0, pl.ds(pair * (1 - core), pair)]


def pack_call(lengths, other, k_t, v_t, n_layers):
    dim, half_len = k_t.shape[2:]
    whole_shape = (2, CHIP_ROWS // 2, dim, half_len)
    whole = pl.BlockSpec(whole_shape, lambda l: (0, 0, 0, 0))
    block = pl.BlockSpec((1, CHIP_ROWS, dim, half_len), lambda l: (l, 1 - lax.axis_index("sp") // 2, 0, 0))
    small = pl.BlockSpec(memory_space=pltpu.SMEM)
    return pl.pallas_call(
        functools.partial(pack_kernel, n_layers),
        grid=(n_layers + 1,), in_specs=[small, small, block, block],
        out_specs=(pl.BlockSpec((1, 2, MAX_UNITS, dim, LANES), lambda l: (jnp.minimum(l, n_layers - 1), 0, 0, 0, 0)), small, whole, whole),
        out_shape=(
            jax.ShapeDtypeStruct((n_layers, 2, MAX_UNITS, dim, LANES), k_t.dtype), jax.ShapeDtypeStruct((2,), jnp.int32),
            jax.ShapeDtypeStruct(whole_shape, k_t.dtype), jax.ShapeDtypeStruct(whole_shape, k_t.dtype)),
        compiler_params=pltpu.CompilerParams(dimension_semantics=("arbitrary",), vmem_limit_bytes=VMEM_GRANT),
        name="pack_units",
    )(lengths, other, k_t, v_t)


def send_kernel(heavy, n_units, packed_ref, k_ref, v_ref, *rest):
    if heavy:
        got_ref, partner_ref, send_sem, recv_sem, fsend_sem, frecv_sem, psend_sem, precv_sem = rest
        phase = 0
    else:
        _, got_ref, send_sem, recv_sem, fsend_sem, frecv_sem = rest
        phase = 1
    me = lax.axis_index("sp")
    middle = jnp.logical_or(me == 1, me == 2)
    sender = middle if heavy else jnp.logical_not(middle)
    across = (me + 2) % 4
    partner = me + 1 - 2 * (me % 2)
    n_layers = packed_ref.shape[0]
    barrier = pltpu.get_barrier_semaphore()
    for peer in (across, partner):
        pl.semaphore_signal(barrier, inc=1, device_id={"sp": peer}, device_id_type=MESH_ID)
    pl.semaphore_wait(barrier, 2)
    direct = []
    onward = []
    for layer in range(n_layers):
        for kind in range(2):
            index = layer * 2 + kind
            part = pl.ds(0, n_units)
            target = got_ref.at[phase, layer, kind, part]
            direct.append(pltpu.make_async_remote_copy(
                src_ref=packed_ref.at[layer, kind, part], dst_ref=target, send_sem=send_sem.at[index], recv_sem=recv_sem.at[index],
                device_id={"sp": across}, device_id_type=MESH_ID))
            onward.append(pltpu.make_async_remote_copy(
                src_ref=target, dst_ref=target, send_sem=fsend_sem.at[index], recv_sem=frecv_sem.at[index],
                device_id={"sp": partner}, device_id_type=MESH_ID))

    @pl.when(sender)
    def _():
        for copy in direct:
            copy.start()

    shares = []
    if heavy:
        rows = partner_ref.shape[2]
        for kind, source in enumerate((k_ref, v_ref)):
            for layer in range(source.shape[0]):
                index = layer * 2 + kind
                shares.append(pltpu.make_async_remote_copy(
                    src_ref=source.at[layer, pl.ds(rows * partner, rows)], dst_ref=partner_ref.at[kind, layer],
                    send_sem=psend_sem.at[index], recv_sem=precv_sem.at[index],
                    device_id={"sp": partner}, device_id_type=MESH_ID))
        for copy in shares:
            copy.start()

    @pl.when(jnp.logical_not(sender))
    def _():
        for near, far in zip(direct, onward):
            near.wait_recv()
            far.start()
        for far in onward:
            far.wait_send()

    @pl.when(sender)
    def _():
        for near, far in zip(direct, onward):
            near.wait_send()
            far.wait_recv()

    for copy in shares:
        copy.wait()


def send_call(heavy, n_units, slot, packed, k_t, v_t, got=None):
    n_layers = packed.shape[0]
    n_copies = 2 * n_layers
    anywhere = pl.BlockSpec(memory_space=pl.ANY)
    got_shape = jax.ShapeDtypeStruct((2,) + packed.shape, packed.dtype)
    sems = [pltpu.SemaphoreType.DMA((n_copies,)) for _ in range(4)]
    if heavy:
        args = (packed, k_t, v_t)
        rows = k_t.shape[1] // 4
        out_shape = (got_shape, jax.ShapeDtypeStruct((2, k_t.shape[0], rows) + k_t.shape[2:], k_t.dtype))
        sems += [pltpu.SemaphoreType.DMA((2 * k_t.shape[0],)) for _ in range(2)]
        aliases = {}
        out_specs = (anywhere, anywhere)
    else:
        args = (packed, k_t, v_t, got)
        out_shape = got_shape
        aliases = {3: 0}
        out_specs = anywhere
    return pl.pallas_call(
        functools.partial(send_kernel, heavy, n_units),
        out_shape=out_shape, in_specs=[anywhere] * len(args), out_specs=out_specs, scratch_shapes=sems,
        input_output_aliases=aliases,
        compiler_params=pltpu.CompilerParams(collective_id=slot, has_side_effects=True),
        name="send_%s_%d" % ("heavy" if heavy else "light", n_units),
    )(*args)


def gather_kernel(n_window, *refs):
    sources, targets = refs[:6], refs[8:12]
    stage, in_sem, out_sem = refs[12:15], refs[15], refs[16]
    windows = [(sources[2 * i + kind], targets[kind].at[1 + i], 2 * i + kind) for i in range(n_window) for kind in range(2)]
    globals_ = [(sources[2 * n_window + kind], targets[2 + kind], 2 * n_window + kind) for kind in range(2)]
    moves = []
    for source, target, place in windows + globals_:
        held = stage[0].at[place] if place < 2 * n_window else stage[1 + place - 2 * n_window]
        moves.append((pltpu.make_async_copy(source, held, in_sem.at[place]), pltpu.make_async_copy(held, target, out_sem.at[place])))
    for bring, _ in moves:
        bring.start()
    for bring, send in moves:
        bring.wait()
        send.start()
    for _, send in moves:
        send.wait()


def gather_call(stacked, windows, globals_):
    n_window = len(windows)
    anywhere = pl.BlockSpec(memory_space=pl.ANY)
    args = [array for pair in windows for array in pair] + list(globals_) + list(stacked)
    window = windows[0][0]
    whole = globals_[0]
    return pl.pallas_call(
        functools.partial(gather_kernel, n_window),
        in_specs=[anywhere] * len(args), out_specs=(anywhere,) * 4,
        out_shape=tuple(jax.ShapeDtypeStruct(a.shape, a.dtype) for a in (*stacked, *globals_)),
        scratch_shapes=[
            pltpu.VMEM((2 * n_window,) + window.shape, window.dtype), pltpu.VMEM(whole.shape, whole.dtype), pltpu.VMEM(whole.shape, whole.dtype),
            pltpu.SemaphoreType.DMA((2 * n_window + 2,)), pltpu.SemaphoreType.DMA((2 * n_window + 2,))],
        input_output_aliases={2 * n_window + 2: 0, 2 * n_window + 3: 1},
        compiler_params=pltpu.CompilerParams(vmem_limit_bytes=VMEM_GRANT),
        name="gather_rows",
    )(*args)


def solution(mesh):
    cache_spec = P(None, "dp", "tp", "sp", None)
    row_spec = P(("dp", "sp"), None)
    col_spec = P(None, None, "tp")
    inner_spec = P(None, "tp", None)
    window_spec = P(None, ("dp", "sp"), "tp", None, None)
    global_spec = P(("dp", "sp"), "tp", None, None)
    in_specs = (cache_spec, cache_spec, P("dp"), row_spec, P(None, None), col_spec, col_spec, col_spec, inner_spec, col_spec, col_spec, inner_spec)
    out_specs = (row_spec, window_spec, window_spec, global_spec, global_spec)

    def device_step(k_cache, v_cache, lengths, hidden, ln_gain, w_query, w_key, w_value, w_out, w_gate, w_up, w_down):
        n_layers = w_query.shape[0]
        rows_dev = hidden.shape[0]
        head_dim = k_cache.shape[-1]
        n_tp = mesh.shape["tp"]
        me = lax.axis_index("sp")
        my_lengths = lax.dynamic_slice_in_dim(lengths, me * rows_dev, rows_dev)
        k_t = k_cache[:, :, 0].swapaxes(-1, -2)
        v_t = v_cache[:, :, 0].swapaxes(-1, -2)
        last = n_layers - 1

        other = lax.ppermute(lengths, "dp", [(0, 1), (1, 0)])
        packed, levels, *whole_rows = pack_call(lengths, other, k_t, v_t, n_layers - 1)
        heavy_calls = [functools.partial(send_call, True, n, 1 + i) for i, n in enumerate(HEAVY_LEVELS)]
        light_calls = [functools.partial(send_call, False, n, 1 + len(HEAVY_LEVELS) + i) for i, n in enumerate(LIGHT_LEVELS)]
        got, partner = lax.switch(levels[0], heavy_calls, packed, k_t, v_t)
        got = lax.switch(levels[1], light_calls, packed, k_t, v_t, got)
        got, *whole_rows = lax.optimization_barrier((got, *whole_rows))
        whole_got = [lax.ppermute(rows, "sp", [(i, i ^ flip) for i in range(4)]) for flip, rows in zip((2, 3), whole_rows)]

        residual = hidden
        tables = rotary_tables(my_lengths, head_dim, w_query.shape[2] // head_dim)
        wk_t = w_key.swapaxes(1, 2)
        wv_t = w_value.swapaxes(1, 2)
        rows_kept = []
        part = None
        for layer in range(n_layers):
            sliding = layer < last
            common = (residual, ln_gain, tables, w_query, wk_t, wv_t, w_out, w_gate, w_up, w_down, k_t, v_t, partner)
            outside = [got] if sliding else whole_got
            result = layer_call(layer, sliding, lengths, *common, outside, part, n_tp)
            if part is not None:
                residual = result[1]
            part = result[0]
            rows_kept.append(result[-2:])
        def back(rows_t):
            return rows_t.swapaxes(-1, -2)

        win_k, win_v, all_k, all_v = gather_call(rows_kept[0], rows_kept[1:last], rows_kept[last])
        return part, back(win_k)[:, :, None], back(win_v)[:, :, None], back(all_k)[:, None], back(all_v)[:, None]

    return jax.shard_map(device_step, mesh=mesh, in_specs=in_specs, out_specs=out_specs, check_vma=False)
```

```python
import functools

import jax
import jax.numpy as jnp
import numpy as np
from jax import lax
from jax.experimental import pallas as pl
from jax.experimental.pallas import tpu as pltpu
from jax.sharding import PartitionSpec as P


WINDOW = 4096
ROPE_BASE = 50000
NORM_EPS = 1e-5


PAD = 16
K_STEPS = 2
DOWN_ROWS = 384
MESH_ID = pl.DeviceIdType.MESH


VMEM_GRANT = 63 * 2 ** 20


def layer_kernel(layer, sliding, n_far, n_tp, lengths_ref, h_ref, gain_ref, cq_ref, sq_ref, ck_ref, sk_ref, *refs):
    wq_hbm, wk_hbm, wv_hbm, wg_hbm, wu_hbm, wd_hbm, wo_hbm, k_hbm, v_hbm, partner_hbm = refs[:10]
    far = refs[10:10 + n_far]
    fused = n_tp > 0
    final = not sliding
    if final:
        refs, (end_ref, end_slots, end_send, end_recv) = refs[:-4], refs[-4:]
    if fused:
        part_ref = refs[10 + n_far]
        (out_ref, h_out, keys_hbm, values_hbm, wq_ref, wk_ref, wv_ref, wg_ref, wu_ref, wd_ref, wo_ref, keys_ref, values_ref, units_ref,
         weight_sem, in_sem, out_sem, slots, send_sem, recv_sem) = refs[-20:]
    else:
        (out_ref, keys_hbm, values_hbm, wq_ref, wk_ref, wv_ref, wg_ref, wu_ref, wd_ref, wo_ref, keys_ref, values_ref, units_ref,
         weight_sem, in_sem, out_sem) = refs[-16:]
    n_rows, model = h_ref.shape
    dim = wk_ref.shape[0]
    q_width = wq_ref.shape[1]
    hidden = wg_ref.shape[1]
    heads = q_width // dim
    half_len = k_hbm.shape[-1]
    me = lax.axis_index("sp")
    chip = me // 2
    first_row = me * n_rows
    core = me % 2
    buffers = (keys_ref, values_ref)
    edges = [lengths_ref[first_row + row] - (WINDOW if sliding else 0) for row in range(n_rows)]
    listed = [[None] * 2 for _ in range(n_rows)]
    if sliding:
        for half in range(2):
            rows, _ = list_of(lengths_ref, chip, half)
            for row in range(n_rows):
                listed[row][half] = [jnp.where(core == 0, one, two) for one, two in zip(rows[row], rows[n_rows + row])]

    def cache_copies(index):
        found = []
        pieces = 2 if sliding else 4
        for kind, (source, buffer) in enumerate(zip((k_hbm, v_hbm), buffers)):
            for piece in range(pieces):
                place = pl.ds(piece * half_len, half_len)
                who = piece ^ (index % 2) if sliding else piece ^ index
                if who == 0:
                    origin = source.at[layer, pl.ds(first_row, n_rows)]
                elif who == 1:
                    origin = partner_hbm.at[kind, layer]
                else:
                    origin = far[2].at[kind] if who == 3 else far[kind].at[0]
                found.append(pltpu.make_async_copy(origin, buffer.at[:, :, place], in_sem.at[kind * 4 + piece]))
        return found

    variants = 2 if sliding else 4
    which = me % variants

    def each_variant(act):
        for index in range(variants):
            @pl.when(which == index)
            def _():
                for copy in cache_copies(index):
                    act(copy)

    unit_copies = []
    if sliding:
        for half in range(2):
            for kind in range(2):
                unit_copies.append(pltpu.make_async_copy(
                    far[0].at[(chip + half) % 2, layer, kind], units_ref.at[half, kind], in_sem.at[8 + half * 2 + kind]))

    n_sem = [0]

    def weight_copy(source, target, first, size):
        rows = pl.ds(first, size)
        copy = pltpu.make_async_copy(source.at[layer, rows], target.at[rows], weight_sem.at[n_sem[0]])
        n_sem[0] += 1
        return copy

    k_len = model // K_STEPS
    down_cuts = [(first, min(DOWN_ROWS, hidden - first)) for first in range(0, hidden, DOWN_ROWS)]
    proj_copies = [weight_copy(wq_hbm, wq_ref, 0, model), weight_copy(wk_hbm, wk_ref, 0, dim), weight_copy(wv_hbm, wv_ref, 0, dim)]
    up_copies = [[weight_copy(wg_hbm, wg_ref, part * k_len, k_len), weight_copy(wu_hbm, wu_ref, part * k_len, k_len)] for part in range(K_STEPS)]
    out_weight = weight_copy(wo_hbm, wo_ref, 0, q_width)
    down_copies = [weight_copy(wd_hbm, wd_ref, first, size) for first, size in down_cuts]

    def start(copies):
        for copy in copies:
            copy.start()

    def wait(copies):
        for copy in copies:
            copy.wait()

    lane = lax.broadcasted_iota(jnp.int32, (dim, LANES), 1)
    if fused:
        here = lax.axis_index("tp")
        barrier = pltpu.get_barrier_semaphore()
        for flip in range(1, n_tp):
            pl.semaphore_signal(barrier, inc=1, device_id={"tp": here ^ flip}, device_id_type=MESH_ID)
    start(proj_copies)
    each_variant(lambda copy: copy.start())
    start(unit_copies)
    if fused:
        pl.semaphore_wait(barrier, n_tp - 1)
        shares = []
        for flip in range(1, n_tp):
            shares.append(pltpu.make_async_remote_copy(
                src_ref=part_ref, dst_ref=slots.at[here], send_sem=send_sem.at[flip - 1], recv_sem=recv_sem.at[flip - 1],
                device_id={"tp": here ^ flip}, device_id_type=MESH_ID))
        start(shares)
        for copies in up_copies:
            start(copies)
        start([out_weight])
        start(down_copies)
        slots[here] = part_ref[...]
    else:
        for copies in up_copies[:2]:
            start(copies)
    if fused:
        each_variant(lambda copy: copy.wait())
        wait(unit_copies)
        for row in range(n_rows):
            edge = edges[row]
            for unit in range(keys_ref.shape[-1] // LANES):
                slot = lane + unit * LANES
                cols = slice(unit * LANES, (unit + 1) * LANES)
                half = unit // HALF_UNITS
                if sliding:
                    begin, _, base = listed[row][half]
                    keep = jnp.logical_xor(slot < edge, chip == 0)
                    place = jnp.clip(base + unit - begin, 0, MAX_UNITS - 1)
                elif unit < 2 * HALF_UNITS:
                    continue
                else:
                    keep = slot < edge
                for kind, buffer in enumerate(buffers):
                    if not sliding:
                        remote = jnp.zeros((dim, LANES), buffer.dtype)
                    else:
                        remote = units_ref[half, kind, place]
                    buffer[row, :, cols] = jnp.where(keep, buffer[row, :, cols], remote)
        wait(shares)
        total = slots[0]
        for index in range(1, n_tp):
            total = total + slots[index]
        rows32 = (h_ref[...].astype(jnp.float32) + total).astype(jnp.bfloat16).astype(jnp.float32)
        h_out[...] = rows32
    else:
        rows32 = h_ref[...].astype(jnp.float32)
    centered = rows32 - jnp.mean(rows32, axis=-1, keepdims=True)
    variance = jnp.mean(centered * centered, axis=-1, keepdims=True)
    scaled = centered * lax.rsqrt(variance + NORM_EPS)
    normed = scaled * gain_ref[layer:layer + 1].astype(jnp.float32)
    normed = jnp.concatenate([normed, jnp.zeros((PAD - n_rows, model), jnp.float32)], axis=0).astype(jnp.bfloat16)

    nt = (((1,), (1,)), ((), ()))
    wait(proj_copies)
    query = jnp.dot(normed, wq_ref[...], preferred_element_type=jnp.float32)[:n_rows]
    k_new = lax.dot_general(wk_ref[...], normed, nt, preferred_element_type=jnp.float32)
    v_new = lax.dot_general(wv_ref[...], normed, nt, preferred_element_type=jnp.float32)
    if sliding:
        q_lane = lax.broadcasted_iota(jnp.int32, query.shape, 1)
        swapped = jnp.where(q_lane % dim < dim // 2, pltpu.roll(query, q_width - dim // 2, 1), pltpu.roll(query, dim // 2, 1))
        query = query * cq_ref[...] + swapped * sq_ref[...]
        first = k_new[:dim // 2]
        second = k_new[dim // 2:]
        cosine = ck_ref[...]
        sine = sk_ref[...]
        k_new = jnp.concatenate([first * cosine - second * sine, second * cosine + first * sine], axis=0)
    k_new = k_new.astype(jnp.bfloat16).astype(jnp.float32)
    v_new = v_new.astype(jnp.bfloat16).astype(jnp.float32)
    spread = [jnp.broadcast_to(query[r:r + 1], (heads, q_width)) for r in range(n_rows)]
    spread = jnp.concatenate(spread, axis=0)
    at_row = lax.broadcasted_iota(jnp.int32, spread.shape, 0)
    at_col = lax.broadcasted_iota(jnp.int32, spread.shape, 1)
    own_head = at_col // dim == at_row % heads
    masked = jnp.where(own_head, spread, 0.0).astype(jnp.bfloat16)
    pick_row = lax.broadcasted_iota(jnp.int32, (dim, q_width), 0)
    pick_col = lax.broadcasted_iota(jnp.int32, (dim, q_width), 1)
    pick = jnp.where(pick_col % dim == pick_row, 1.0, 0.0).astype(jnp.bfloat16)
    head_q = lax.dot_general(masked, pick, nt, preferred_element_type=jnp.float32).astype(jnp.bfloat16)

    column = lax.broadcasted_iota(jnp.int32, (dim, PAD), 1)
    if fused:
        for row in range(n_rows):
            edge = edges[row]
            for buffer, new in zip(buffers, (k_new, v_new)):
                picked = jnp.sum(jnp.where(column == row, new, 0.0), axis=1, keepdims=True)
                tile = jnp.broadcast_to(picked, (dim, LANES)).astype(buffer.dtype)
                for unit in range(keys_ref.shape[-1] // LANES):
                    if not sliding and unit < 2 * HALF_UNITS:
                        continue
                    cols = slice(unit * LANES, (unit + 1) * LANES)
                    buffer[row, :, cols] = jnp.where(lane + unit * LANES == edge, tile, buffer[row, :, cols])
    else:
        start(up_copies[2])
        each_variant(lambda copy: copy.wait())
        wait(unit_copies)
        for row in range(n_rows):
            edge = edges[row]
            border = edge // LANES
            cols = pl.ds(pl.multiple_of(border * LANES, LANES), LANES)
            slot = lane + border * LANES
            before = [buffer[row, :, cols] for buffer in buffers]
            if sliding:
                for half in range(2):
                    begin, count, base = listed[row][half]

                    def place_unit(unit, carry, half=half, begin=begin, base=base):
                        to = pl.ds(pl.multiple_of(unit * LANES, LANES), LANES)
                        for kind, buffer in enumerate(buffers):
                            buffer[row, :, to] = units_ref[half, kind, base + unit - begin]
                        return carry

                    lax.fori_loop(begin, begin + count, place_unit, 0)
                border_half = border // HALF_UNITS
                border_base = jnp.where(border_half == 0, listed[row][0][2] - listed[row][0][0], listed[row][1][2] - listed[row][1][0])
                border_place = jnp.clip(border_base + border, 0, MAX_UNITS - 1)
                keep = jnp.logical_xor(slot < edge, chip == 0)
            else:
                def clear_unit(unit, carry):
                    to = pl.ds(pl.multiple_of(unit * LANES, LANES), LANES)
                    for buffer in buffers:
                        buffer[row, :, to] = jnp.zeros((dim, LANES), buffer.dtype)
                    return carry

                lax.fori_loop(border + 1, 4 * HALF_UNITS, clear_unit, 0)
                keep = slot < edge
            for kind, (buffer, new) in enumerate(zip(buffers, (k_new, v_new))):
                picked = jnp.sum(jnp.where(column == row, new, 0.0), axis=1, keepdims=True)
                if sliding:
                    remote = units_ref[border_half, kind, border_place].astype(jnp.float32)
                else:
                    remote = jnp.zeros((dim, LANES), jnp.float32)
                merged = jnp.where(keep, before[kind].astype(jnp.float32), remote)
                merged = jnp.where(slot == edge, jnp.broadcast_to(picked, (dim, LANES)), merged)
                buffer[row, :, cols] = merged.astype(buffer.dtype)
        start(up_copies[3])
    out_copies = []
    for kind, (buffer, kept) in enumerate(zip(buffers, (keys_hbm, values_hbm))):
        target = kept.at[0] if layer == 0 else kept
        out_copies.append(pltpu.make_async_copy(buffer, target, out_sem.at[kind]))
    start(out_copies)
    mixed = []
    for row in range(n_rows):
        edge = edges[row]
        scores = jnp.dot(head_q[heads * row:heads * (row + 1)], keys_ref[row], preferred_element_type=jnp.float32) * dim ** -0.5
        if not sliding:
            position = lax.broadcasted_iota(jnp.int32, scores.shape, 1)
            scores = jnp.where(position <= edge, scores, -1e30)
        top = jnp.max(scores, axis=-1, keepdims=True)
        raised = jnp.exp(scores - top)
        weights = (raised / jnp.sum(raised, axis=-1, keepdims=True)).astype(jnp.bfloat16)
        mixed.append(lax.dot_general(weights, values_ref[row], nt, preferred_element_type=jnp.float32))
    both = jnp.concatenate(mixed, axis=0).astype(jnp.bfloat16)
    wide = jnp.dot(both, pick, preferred_element_type=jnp.float32)
    wide = jnp.where(own_head, wide, 0.0).astype(jnp.bfloat16)

    if not fused:
        start([out_weight])
        start(down_copies)
    gate = jnp.zeros((PAD, hidden), jnp.float32)
    raise_ = jnp.zeros((PAD, hidden), jnp.float32)
    for part in range(K_STEPS):
        wait(up_copies[part])
        rows = slice(part * k_len, (part + 1) * k_len)
        gate = gate + jnp.dot(normed[:, rows], wg_ref[rows], preferred_element_type=jnp.float32)
        raise_ = raise_ + jnp.dot(normed[:, rows], wu_ref[rows], preferred_element_type=jnp.float32)
    active = (gate * jax.nn.sigmoid(gate) * raise_).astype(jnp.bfloat16)

    wait([out_weight])
    product = jnp.dot(wide, wo_ref[...], preferred_element_type=jnp.float32)
    sums = jnp.concatenate([jnp.sum(product[heads * r:heads * (r + 1)], axis=0, keepdims=True) for r in range(n_rows)], axis=0)
    total = jnp.zeros((PAD, model), jnp.float32)
    for copy, (first, size) in zip(down_copies, down_cuts):
        copy.wait()
        total = total + jnp.dot(active[:, first:first + size], wd_ref[first:first + size], preferred_element_type=jnp.float32)
    if final:
        end_ref[...] = sums + total[:n_rows]
        wait(out_copies)
        ends = []
        for flip in range(1, n_tp):
            ends.append(pltpu.make_async_remote_copy(
                src_ref=end_ref, dst_ref=end_slots.at[here], send_sem=end_send.at[flip - 1], recv_sem=end_recv.at[flip - 1],
                device_id={"tp": here ^ flip}, device_id_type=MESH_ID))
        start(ends)
        end_slots[here] = end_ref[...]
        wait(ends)
        total = end_slots[0]
        for index in range(1, n_tp):
            total = total + end_slots[index]
        out_ref[...] = (rows32 + total).astype(out_ref.dtype)
    else:
        out_ref[...] = sums + total[:n_rows]
        wait(out_copies)


def chain_kernel(n_layers, n_tp, lengths_ref, h_ref, gain_ref, cq_ref, sq_ref, ck_ref, sk_ref, wq_hbm, wk_hbm, wv_hbm, wg_hbm, wu_hbm, wd_hbm,
                 wo_hbm, k_hbm, v_hbm, partner_hbm, got_hbm, out_ref, h_out, *refs):
    kept = refs[:2 * n_layers]
    (wq_ref, wk_ref, wv_ref, wg_ref, wu_ref, wd_ref, wo_ref, keys_ref, values_ref, units_ref, part_ref, slots,
     weight_sem, in_sem, unit_sem, out_sem, send_sem, recv_sem) = refs[2 * n_layers:]
    n_rows, model = h_ref.shape
    dim = wk_ref.shape[0]
    q_width = wq_ref.shape[1]
    hidden = wg_ref.shape[1]
    heads = q_width // dim
    half_len = k_hbm.shape[-1]
    me = lax.axis_index("sp")
    here = lax.axis_index("tp")
    chip = me // 2
    core = me % 2
    first_row = me * n_rows
    k_len = model // K_STEPS
    nt = (((1,), (1,)), ((), ()))
    down_cuts = [(first, min(DOWN_ROWS, hidden - first)) for first in range(0, hidden, DOWN_ROWS)]
    edges = [lengths_ref[first_row + row] - WINDOW for row in range(n_rows)]
    listed = [[None] * 2 for _ in range(n_rows)]
    for half in range(2):
        rows, _ = list_of(lengths_ref, chip, half)
        for row in range(n_rows):
            listed[row][half] = [jnp.where(core == 0, one, two) for one, two in zip(rows[row], rows[n_rows + row])]

    def start(copies):
        for copy in copies:
            copy.start()

    def wait(copies):
        for copy in copies:
            copy.wait()

    def cache_copies(layer, index):
        found = []
        for kind, (source, buffer) in enumerate(((k_hbm, keys_ref), (v_hbm, values_ref))):
            for piece in range(2):
                place = pl.ds(piece * half_len, half_len)
                origin = source.at[layer, pl.ds(first_row, n_rows)] if piece == index else partner_hbm.at[kind, layer]
                found.append(pltpu.make_async_copy(origin, buffer.at[layer, :, :, place], in_sem.at[layer, kind * 2 + piece]))
        return found

    def each_core(layer, act):
        for index in range(2):
            @pl.when(core == index)
            def _():
                for copy in cache_copies(layer, index):
                    act(copy)

    def unit_copies(layer):
        return [pltpu.make_async_copy(got_hbm.at[(chip + half) % 2, layer, kind], units_ref.at[half, kind], unit_sem.at[layer, half * 2 + kind])
                for half in range(2) for kind in range(2)]

    plans = []
    for layer in range(n_layers):
        count = [0]

        def cut(source, target, first, size, layer=layer, count=count):
            rows = pl.ds(first, size)
            copy = pltpu.make_async_copy(source.at[layer, rows], target.at[rows], weight_sem.at[layer, count[0]])
            count[0] += 1
            return copy

        proj = [cut(wq_hbm, wq_ref, 0, model), cut(wk_hbm, wk_ref, 0, dim), cut(wv_hbm, wv_ref, 0, dim)]
        up = [[cut(wg_hbm, wg_ref, p * k_len, k_len), cut(wu_hbm, wu_ref, p * k_len, k_len)] for p in range(K_STEPS)]
        out_weight = cut(wo_hbm, wo_ref, 0, q_width)
        down = [cut(wd_hbm, wd_ref, first, size) for first, size in down_cuts]
        plans.append((proj, up, out_weight, down))

    barrier = pltpu.get_barrier_semaphore()
    for flip in range(1, n_tp):
        pl.semaphore_signal(barrier, inc=1, device_id={"tp": here ^ flip}, device_id_type=MESH_ID)
    start(plans[0][0])
    each_core(0, lambda copy: copy.start())
    start(unit_copies(0))
    for copies in plans[0][1]:
        start(copies)
    start([plans[0][2]])
    start(plans[0][3])
    for layer in range(1, n_layers):
        each_core(layer, lambda copy: copy.start())
    pl.semaphore_wait(barrier, n_tp - 1)

    lane = lax.broadcasted_iota(jnp.int32, (dim, LANES), 1)
    column = lax.broadcasted_iota(jnp.int32, (dim, PAD), 1)
    pick_row = lax.broadcasted_iota(jnp.int32, (dim, q_width), 0)
    pick_col = lax.broadcasted_iota(jnp.int32, (dim, q_width), 1)
    n_units = 2 * HALF_UNITS
    for layer in range(n_layers):
        proj, up, out_weight, down = plans[layer]
        buffers = (keys_ref.at[layer], values_ref.at[layer])
        shares = []
        if layer > 0:
            for flip in range(1, n_tp):
                shares.append(pltpu.make_async_remote_copy(
                    src_ref=part_ref.at[layer - 1], dst_ref=slots.at[layer - 1, here], send_sem=send_sem.at[layer - 1, flip - 1],
                    recv_sem=recv_sem.at[layer - 1, flip - 1], device_id={"tp": here ^ flip}, device_id_type=MESH_ID))
            start(shares)
            for copies in up:
                start(copies)
            start([out_weight])
            start(down)
            slots[layer - 1, here] = part_ref[layer - 1]
        each_core(layer, lambda copy: copy.wait())
        wait(unit_copies(layer))
        for row in range(n_rows):
            for unit in range(n_units):
                slot = lane + unit * LANES
                cols = slice(unit * LANES, (unit + 1) * LANES)
                half = unit // HALF_UNITS
                begin, _, base = listed[row][half]
                keep = jnp.logical_xor(slot < edges[row], chip == 0)
                place = jnp.clip(base + unit - begin, 0, MAX_UNITS - 1)
                for kind, buffer in enumerate(buffers):
                    buffer[row, :, cols] = jnp.where(keep, buffer[row, :, cols], units_ref[half, kind, place])
        if layer + 1 < n_layers:
            start(unit_copies(layer + 1))
        if layer > 0:
            wait(shares)
            total = slots[layer - 1, 0]
            for index in range(1, n_tp):
                total = total + slots[layer - 1, index]
            before = h_ref[...].astype(jnp.float32) if layer == 1 else h_out[...]
            rows32 = (before + total).astype(jnp.bfloat16).astype(jnp.float32)
            h_out[...] = rows32
        else:
            rows32 = h_ref[...].astype(jnp.float32)
        centered = rows32 - jnp.mean(rows32, axis=-1, keepdims=True)
        variance = jnp.mean(centered * centered, axis=-1, keepdims=True)
        scaled = centered * lax.rsqrt(variance + NORM_EPS)
        normed = scaled * gain_ref[layer:layer + 1].astype(jnp.float32)
        normed = jnp.concatenate([normed, jnp.zeros((PAD - n_rows, model), jnp.float32)], axis=0).astype(jnp.bfloat16)

        wait(proj)
        query = jnp.dot(normed, wq_ref[...], preferred_element_type=jnp.float32)[:n_rows]
        k_new = lax.dot_general(wk_ref[...], normed, nt, preferred_element_type=jnp.float32)
        v_new = lax.dot_general(wv_ref[...], normed, nt, preferred_element_type=jnp.float32)
        if layer + 1 < n_layers:
            start(plans[layer + 1][0])
        q_lane = lax.broadcasted_iota(jnp.int32, query.shape, 1)
        swapped = jnp.where(q_lane % dim < dim // 2, pltpu.roll(query, q_width - dim // 2, 1), pltpu.roll(query, dim // 2, 1))
        query = query * cq_ref[...] + swapped * sq_ref[...]
        upper = k_new[:dim // 2]
        lower = k_new[dim // 2:]
        cosine = ck_ref[...]
        sine = sk_ref[...]
        k_new = jnp.concatenate([upper * cosine - lower * sine, lower * cosine + upper * sine], axis=0)
        k_new = k_new.astype(jnp.bfloat16).astype(jnp.float32)
        v_new = v_new.astype(jnp.bfloat16).astype(jnp.float32)
        spread = jnp.concatenate([jnp.broadcast_to(query[r:r + 1], (heads, q_width)) for r in range(n_rows)], axis=0)
        at_row = lax.broadcasted_iota(jnp.int32, spread.shape, 0)
        at_col = lax.broadcasted_iota(jnp.int32, spread.shape, 1)
        own_head = at_col // dim == at_row % heads
        masked = jnp.where(own_head, spread, 0.0).astype(jnp.bfloat16)
        pick = jnp.where(pick_col % dim == pick_row, 1.0, 0.0).astype(jnp.bfloat16)
        head_q = lax.dot_general(masked, pick, nt, preferred_element_type=jnp.float32).astype(jnp.bfloat16)
        for row in range(n_rows):
            for buffer, new in zip(buffers, (k_new, v_new)):
                picked = jnp.sum(jnp.where(column == row, new, 0.0), axis=1, keepdims=True)
                tile = jnp.broadcast_to(picked, (dim, LANES)).astype(buffer.dtype)
                for unit in range(n_units):
                    cols = slice(unit * LANES, (unit + 1) * LANES)
                    buffer[row, :, cols] = jnp.where(lane + unit * LANES == edges[row], tile, buffer[row, :, cols])
        out_copies = []
        for kind, buffer in enumerate(buffers):
            out_copies.append(pltpu.make_async_copy(buffer, kept[2 * layer + kind], out_sem.at[layer, kind]))
        start(out_copies)
        mixed = []
        for row in range(n_rows):
            scores = jnp.dot(head_q[heads * row:heads * (row + 1)], keys_ref[layer, row], preferred_element_type=jnp.float32) * dim ** -0.5
            top = jnp.max(scores, axis=-1, keepdims=True)
            raised = jnp.exp(scores - top)
            weights = (raised / jnp.sum(raised, axis=-1, keepdims=True)).astype(jnp.bfloat16)
            mixed.append(lax.dot_general(weights, values_ref[layer, row], nt, preferred_element_type=jnp.float32))
        both = jnp.concatenate(mixed, axis=0).astype(jnp.bfloat16)
        wide = jnp.dot(both, pick, preferred_element_type=jnp.float32)
        wide = jnp.where(own_head, wide, 0.0).astype(jnp.bfloat16)

        gate = jnp.zeros((PAD, hidden), jnp.float32)
        raise_ = jnp.zeros((PAD, hidden), jnp.float32)
        for p in range(K_STEPS):
            wait(up[p])
            rows = slice(p * k_len, (p + 1) * k_len)
            gate = gate + jnp.dot(normed[:, rows], wg_ref[rows], preferred_element_type=jnp.float32)
            raise_ = raise_ + jnp.dot(normed[:, rows], wu_ref[rows], preferred_element_type=jnp.float32)
        active = (gate * jax.nn.sigmoid(gate) * raise_).astype(jnp.bfloat16)
        wait([out_weight])
        product = jnp.dot(wide, wo_ref[...], preferred_element_type=jnp.float32)
        sums = jnp.concatenate([jnp.sum(product[heads * r:heads * (r + 1)], axis=0, keepdims=True) for r in range(n_rows)], axis=0)
        total = jnp.zeros((PAD, model), jnp.float32)
        for copy, (first, size) in zip(down, down_cuts):
            copy.wait()
            total = total + jnp.dot(active[:, first:first + size], wd_ref[first:first + size], preferred_element_type=jnp.float32)
        if layer + 1 < n_layers:
            part_ref[layer] = sums + total[:n_rows]
        else:
            out_ref[...] = sums + total[:n_rows]
        wait(out_copies)


def chain_call(n_layers, n_tp, lengths, h, gain, tables, w_query, wk_t, wv_t, w_out, w_gate, w_up, w_down, k_t, v_t, partner, got):
    n_rows, model = h.shape
    q_width = w_query.shape[2]
    dim = wk_t.shape[1]
    hidden = w_gate.shape[2]
    total = 2 * k_t.shape[-1]
    in_vmem = pl.BlockSpec(memory_space=pltpu.VMEM)
    anywhere = pl.BlockSpec(memory_space=pl.ANY)
    args = [lengths, h, gain, *tables, w_query, wk_t, wv_t, w_gate, w_up, w_down, w_out, k_t, v_t, partner, got]
    row_shape = jax.ShapeDtypeStruct((n_rows, model), jnp.float32)
    kept_shape = jax.ShapeDtypeStruct((n_rows, dim, total), k_t.dtype)
    n_weight = 4 + 2 * K_STEPS + -(-hidden // DOWN_ROWS)
    dma = pltpu.SemaphoreType.DMA
    return pl.pallas_call(
        functools.partial(chain_kernel, n_layers, n_tp),
        in_specs=[pl.BlockSpec(memory_space=pltpu.SMEM)] + [in_vmem] * 6 + [anywhere] * 11,
        out_specs=(in_vmem, in_vmem) + (anywhere,) * (2 * n_layers),
        out_shape=(row_shape, row_shape) + (kept_shape,) * (2 * n_layers),
        scratch_shapes=[
            pltpu.VMEM((model, q_width), jnp.bfloat16),
            pltpu.VMEM((dim, model), jnp.bfloat16),
            pltpu.VMEM((dim, model), jnp.bfloat16),
            pltpu.VMEM((model, hidden), jnp.bfloat16),
            pltpu.VMEM((model, hidden), jnp.bfloat16),
            pltpu.VMEM((hidden, model), jnp.bfloat16),
            pltpu.VMEM((q_width, model), jnp.bfloat16),
            pltpu.VMEM((n_layers, n_rows, dim, total), jnp.bfloat16),
            pltpu.VMEM((n_layers, n_rows, dim, total), jnp.bfloat16),
            pltpu.VMEM((2, 2, MAX_UNITS, dim, LANES), jnp.bfloat16),
            pltpu.VMEM((n_layers - 1, n_rows, model), jnp.float32),
            pltpu.VMEM((n_layers - 1, n_tp, n_rows, model), jnp.float32),
            dma((n_layers, n_weight)), dma((n_layers, 4)), dma((n_layers, 4)), dma((n_layers, 2)),
            dma((n_layers - 1, n_tp - 1)), dma((n_layers - 1, n_tp - 1)),
        ],
        compiler_params=pltpu.CompilerParams(vmem_limit_bytes=VMEM_GRANT, collective_id=40, has_side_effects=True),
        name="window_chain",
    )(*args)


def layer_call(layer, sliding, lengths, h, gain, tables, w_query, wk_t, wv_t, w_out, w_gate, w_up, w_down, k_t, v_t, partner, far, part=None, n_tp=0):
    n_rows, model = h.shape
    q_width = w_query.shape[2]
    dim = wk_t.shape[1]
    hidden = w_gate.shape[2]
    half_len = k_t.shape[-1]
    in_vmem = pl.BlockSpec(memory_space=pltpu.VMEM)
    anywhere = pl.BlockSpec(memory_space=pl.ANY)
    total = (2 if sliding else 4) * half_len
    kept = (3, n_rows, dim, total) if layer == 0 else (n_rows, dim, total)
    kept_shape = jax.ShapeDtypeStruct(kept, k_t.dtype)
    args = [lengths, h, gain, *tables, w_query, wk_t, wv_t, w_gate, w_up, w_down, w_out, k_t, v_t, partner, *far]
    in_specs = [pl.BlockSpec(memory_space=pltpu.SMEM)] + [in_vmem] * 6 + [anywhere] * (10 + len(far))
    fused = part is not None
    if fused:
        args.append(part)
        in_specs.append(in_vmem)
    n_small = 2 if fused else 1
    weight_bytes = 2 * (2 * model * q_width + 2 * dim * model + 3 * model * hidden)
    units = (2, 2, MAX_UNITS, dim, LANES) if sliding else (8, LANES)
    n_weight = 4 + 2 * K_STEPS + -(-hidden // DOWN_ROWS)
    row_shape = jax.ShapeDtypeStruct((n_rows, model), jnp.float32)
    first_shape = row_shape
    if fused:
        remote = [pltpu.VMEM((n_tp, n_rows, model), jnp.float32), pltpu.SemaphoreType.DMA((n_tp - 1,)), pltpu.SemaphoreType.DMA((n_tp - 1,))]
        if not sliding:
            remote = remote + [pltpu.VMEM((n_rows, model), jnp.float32)] + remote
            first_shape = jax.ShapeDtypeStruct((n_rows, model), jnp.bfloat16)
        params = pltpu.CompilerParams(vmem_limit_bytes=VMEM_GRANT, collective_id=40 + layer, has_side_effects=True)
    else:
        remote = []
        params = pltpu.CompilerParams(vmem_limit_bytes=VMEM_GRANT)
    return pl.pallas_call(
        functools.partial(layer_kernel, layer, sliding, len(far), n_tp if fused else 0),
        in_specs=in_specs, out_specs=(in_vmem,) * n_small + (anywhere, anywhere),
        scratch_shapes=[
            pltpu.VMEM((model, q_width), jnp.bfloat16),
            pltpu.VMEM((dim, model), jnp.bfloat16),
            pltpu.VMEM((dim, model), jnp.bfloat16),
            pltpu.VMEM((model, hidden), jnp.bfloat16),
            pltpu.VMEM((model, hidden), jnp.bfloat16),
            pltpu.VMEM((hidden, model), jnp.bfloat16),
            pltpu.VMEM((q_width, model), jnp.bfloat16),
            pltpu.VMEM((n_rows, dim, total), jnp.bfloat16),
            pltpu.VMEM((n_rows, dim, total), jnp.bfloat16),
            pltpu.VMEM(units, jnp.bfloat16),
            pltpu.SemaphoreType.DMA((n_weight,)),
            pltpu.SemaphoreType.DMA((12,)),
            pltpu.SemaphoreType.DMA((2,)),
        ] + remote,
        out_shape=(first_shape, row_shape)[:n_small] + (kept_shape, kept_shape),
        compiler_params=params,
        cost_estimate=pl.CostEstimate(flops=PAD * weight_bytes, bytes_accessed=weight_bytes, transcendentals=0),
    )(*args)


def rotary_tables(positions, dim, heads):
    half = dim // 2
    inv_freq = 1.0 / (float(ROPE_BASE) ** (np.arange(half) * 2.0 / dim))
    wide = np.tile(inv_freq, 2 * heads).astype(np.float32)
    sign = np.tile(np.repeat([-1.0, 1.0], half), heads).astype(np.float32)
    turn = positions.astype(jnp.float32)[:, None] * wide[None, :]
    padded = jnp.pad(positions, (0, PAD - positions.shape[0])).astype(jnp.float32)
    turn_t = inv_freq.astype(np.float32)[:, None] * padded[None, :]
    return jnp.cos(turn), jnp.sin(turn) * sign[None, :], jnp.cos(turn_t), jnp.sin(turn_t)


LANES = 128
HALF_UNITS = 16
CHIP_ROWS = 4
MAX_UNITS = CHIP_ROWS * HALF_UNITS
HEAVY_LEVELS = (28, 36, 40, 44, 46, 48, 50, 52, 54, 56, 58, 60, 62, 64)
LIGHT_LEVELS = (8, 16, 20, 24, 26, 28, 30, 32, 34, 36, 38, 40, 44, 48, 56, 64)


def row_units(edge, half, from_upper):
    low = half * HALF_UNITS
    upper_end = jnp.clip((edge + LANES - 1) // LANES, low, low + HALF_UNITS)
    lower_start = jnp.clip((edge + 1) // LANES, low, low + HALF_UNITS)
    start = jnp.where(from_upper, low, lower_start)
    count = jnp.where(from_upper, upper_end - low, low + HALF_UNITS - lower_start)
    return start, count


def list_of(lengths_ref, chip, half):
    base = jnp.int32(0)
    found = []
    for row in range(CHIP_ROWS):
        start, count = row_units(lengths_ref[CHIP_ROWS * chip + row] - WINDOW, half, chip == 0)
        found.append((start, count, base))
        base = base + count
    return found, base


def pack_kernel(n_packed, lengths_ref, other_ref, k_ref, v_ref, out_ref, level_ref, across_ref, diagonal_ref):
    me = lax.axis_index("sp")
    core = me % 2
    chip = me // 2
    layer = pl.program_id(0)

    @pl.when(layer == 0)
    def _():
        for place, (levels, swap) in enumerate(((HEAVY_LEVELS, 0), (LIGHT_LEVELS, 1))):
            need = jnp.int32(0)
            for ref in (lengths_ref, other_ref):
                for target in range(2):
                    need = jnp.maximum(need, list_of(ref, target, target ^ swap)[1])
            index = jnp.int32(0)
            for level in levels[:-1]:
                index = index + jnp.where(need > level, 1, 0)
            level_ref[place] = index

    rows, _ = list_of(lengths_ref, 1 - chip, core)
    for row, (start, count, base) in enumerate(rows):
        first = start - core * HALF_UNITS
        for unit in range(HALF_UNITS):
            @pl.when(jnp.logical_and(layer < n_packed, jnp.logical_and(unit >= first, unit < first + count)))
            def _():
                place = base + unit - first
                cols = pl.ds(unit * LANES, LANES)
                out_ref[0, 0, place] = k_ref[0, row, :, cols]
                out_ref[0, 1, place] = v_ref[0, row, :, cols]

    @pl.when(layer == n_packed)
    def _():
        pair = CHIP_ROWS // 2
        across_ref[0] = v_ref[0, pl.ds(pair * core, pair)]
        for kind, ref in enumerate((k_ref, v_ref)):
            diagonal_ref[kind] = ref[0, pl.ds(pair * (1 - core), pair)]


def pack_call(lengths, other, k_t, v_t, n_layers):
    dim, half_len = k_t.shape[2:]
    whole_shape = (2, CHIP_ROWS // 2, dim, half_len)
    single_shape = (1,) + whole_shape[1:]
    whole = pl.BlockSpec(whole_shape, lambda l: (0, 0, 0, 0))
    single = pl.BlockSpec(single_shape, lambda l: (0, 0, 0, 0))
    block = pl.BlockSpec((1, CHIP_ROWS, dim, half_len), lambda l: (l, 1 - lax.axis_index("sp") // 2, 0, 0))
    small = pl.BlockSpec(memory_space=pltpu.SMEM)
    return pl.pallas_call(
        functools.partial(pack_kernel, n_layers),
        grid=(n_layers + 1,), in_specs=[small, small, block, block],
        out_specs=(pl.BlockSpec((1, 2, MAX_UNITS, dim, LANES), lambda l: (jnp.minimum(l, n_layers - 1), 0, 0, 0, 0)), small, single, whole),
        out_shape=(
            jax.ShapeDtypeStruct((n_layers, 2, MAX_UNITS, dim, LANES), k_t.dtype), jax.ShapeDtypeStruct((2,), jnp.int32),
            jax.ShapeDtypeStruct(single_shape, k_t.dtype), jax.ShapeDtypeStruct(whole_shape, k_t.dtype)),
        compiler_params=pltpu.CompilerParams(dimension_semantics=("arbitrary",), vmem_limit_bytes=VMEM_GRANT),
        name="pack_units",
    )(lengths, other, k_t, v_t)


def send_kernel(heavy, n_units, packed_ref, k_ref, v_ref, *rest):
    if heavy:
        got_ref, partner_ref, send_sem, recv_sem, fsend_sem, frecv_sem, psend_sem, precv_sem = rest
        phase = 0
    else:
        _, got_ref, send_sem, recv_sem, fsend_sem, frecv_sem = rest
        phase = 1
    me = lax.axis_index("sp")
    middle = jnp.logical_or(me == 1, me == 2)
    sender = middle if heavy else jnp.logical_not(middle)
    across = (me + 2) % 4
    partner = me + 1 - 2 * (me % 2)
    n_layers = packed_ref.shape[0]
    barrier = pltpu.get_barrier_semaphore()
    for peer in (across, partner):
        pl.semaphore_signal(barrier, inc=1, device_id={"sp": peer}, device_id_type=MESH_ID)
    pl.semaphore_wait(barrier, 2)
    direct = []
    onward = []
    for layer in range(n_layers):
        for kind in range(2):
            index = layer * 2 + kind
            part = pl.ds(0, n_units)
            target = got_ref.at[phase, layer, kind, part]
            direct.append(pltpu.make_async_remote_copy(
                src_ref=packed_ref.at[layer, kind, part], dst_ref=target, send_sem=send_sem.at[index], recv_sem=recv_sem.at[index],
                device_id={"sp": across}, device_id_type=MESH_ID))
            onward.append(pltpu.make_async_remote_copy(
                src_ref=target, dst_ref=target, send_sem=fsend_sem.at[index], recv_sem=frecv_sem.at[index],
                device_id={"sp": partner}, device_id_type=MESH_ID))

    @pl.when(sender)
    def _():
        for copy in direct:
            copy.start()

    shares = []
    if heavy:
        rows = partner_ref.shape[2]
        for kind, source in enumerate((k_ref, v_ref)):
            for layer in range(source.shape[0]):
                index = layer * 2 + kind
                shares.append(pltpu.make_async_remote_copy(
                    src_ref=source.at[layer, pl.ds(rows * partner, rows)], dst_ref=partner_ref.at[kind, layer],
                    send_sem=psend_sem.at[index], recv_sem=precv_sem.at[index],
                    device_id={"sp": partner}, device_id_type=MESH_ID))
        for copy in shares:
            copy.start()

    @pl.when(jnp.logical_not(sender))
    def _():
        for near, far in zip(direct, onward):
            near.wait_recv()
            far.start()
        for far in onward:
            far.wait_send()

    @pl.when(sender)
    def _():
        for near, far in zip(direct, onward):
            near.wait_send()
            far.wait_recv()

    for copy in shares:
        copy.wait()


def send_call(heavy, n_units, slot, packed, k_t, v_t, got=None):
    n_layers = packed.shape[0]
    n_copies = 2 * n_layers
    anywhere = pl.BlockSpec(memory_space=pl.ANY)
    got_shape = jax.ShapeDtypeStruct((2,) + packed.shape, packed.dtype)
    sems = [pltpu.SemaphoreType.DMA((n_copies,)) for _ in range(4)]
    if heavy:
        args = (packed, k_t, v_t)
        rows = k_t.shape[1] // 4
        out_shape = (got_shape, jax.ShapeDtypeStruct((2, k_t.shape[0], rows) + k_t.shape[2:], k_t.dtype))
        sems += [pltpu.SemaphoreType.DMA((2 * k_t.shape[0],)) for _ in range(2)]
        aliases = {}
        out_specs = (anywhere, anywhere)
    else:
        args = (packed, k_t, v_t, got)
        out_shape = got_shape
        aliases = {3: 0}
        out_specs = anywhere
    return pl.pallas_call(
        functools.partial(send_kernel, heavy, n_units),
        out_shape=out_shape, in_specs=[anywhere] * len(args), out_specs=out_specs, scratch_shapes=sems,
        input_output_aliases=aliases,
        compiler_params=pltpu.CompilerParams(collective_id=slot, has_side_effects=True),
    )(*args)


def gather_kernel(n_window, *refs):
    n_in = 2 * n_window + 2
    sources, targets = refs[:n_in], refs[n_in:n_in + 4]
    windows, keys, values, in_sem, out_sem = refs[n_in + 4:]
    moves = []
    for place, source in enumerate(sources):
        if place < 2 * n_window:
            held, target = windows.at[place], targets[place % 2].at[place // 2]
        else:
            held, target = (keys, values)[place % 2], targets[2 + place % 2]
        moves.append((pltpu.make_async_copy(source, held, in_sem.at[place]), pltpu.make_async_copy(held, target, out_sem.at[place])))
    for bring, _ in moves:
        bring.start()
    for bring, send in moves:
        bring.wait()
        send.start()
    for _, send in moves:
        send.wait()


def gather_call(windows, globals_):
    n_window = len(windows) // 2
    anywhere = pl.BlockSpec(memory_space=pl.ANY)
    args = list(windows) + list(globals_)
    window = windows[0]
    whole = globals_[0]
    stacked = jax.ShapeDtypeStruct((n_window,) + window.shape, window.dtype)
    whole_shape = jax.ShapeDtypeStruct(whole.shape, whole.dtype)
    return pl.pallas_call(
        functools.partial(gather_kernel, n_window),
        in_specs=[anywhere] * len(args), out_specs=(anywhere,) * 4,
        out_shape=(stacked, stacked, whole_shape, whole_shape),
        scratch_shapes=[
            pltpu.VMEM((2 * n_window,) + window.shape, window.dtype), pltpu.VMEM(whole.shape, whole.dtype), pltpu.VMEM(whole.shape, whole.dtype),
            pltpu.SemaphoreType.DMA((len(args),)), pltpu.SemaphoreType.DMA((len(args),))],
        compiler_params=pltpu.CompilerParams(vmem_limit_bytes=VMEM_GRANT),
        name="gather_rows",
    )(*args)


def solution(mesh):
    cache_spec = P(None, "dp", "tp", "sp", None)
    row_spec = P(("dp", "sp"), None)
    col_spec = P(None, None, "tp")
    inner_spec = P(None, "tp", None)
    window_spec = P(None, ("dp", "sp"), "tp", None, None)
    global_spec = P(("dp", "sp"), "tp", None, None)
    in_specs = (cache_spec, cache_spec, P("dp"), row_spec, P(None, None), col_spec, col_spec, col_spec, inner_spec, col_spec, col_spec, inner_spec)
    out_specs = (row_spec, window_spec, window_spec, global_spec, global_spec)

    def inner_step(k_cache, v_cache, lengths, hidden, ln_gain, w_query, w_key, w_value, w_out, w_gate, w_up, w_down):
        n_layers = w_query.shape[0]
        rows_dev = hidden.shape[0]
        head_dim = k_cache.shape[-1]
        n_tp = mesh.shape["tp"]
        me = lax.axis_index("sp")
        my_lengths = lax.dynamic_slice_in_dim(lengths, me * rows_dev, rows_dev)
        k_t = k_cache[:, :, 0].swapaxes(-1, -2)
        v_t = v_cache[:, :, 0].swapaxes(-1, -2)
        last = n_layers - 1

        other = lax.ppermute(lengths, "dp", [(0, 1), (1, 0)])
        first = lax.dynamic_slice(k_t, (last, (me ^ 2) * rows_dev, 0, 0), (1, rows_dev) + k_t.shape[2:])
        early = lax.ppermute(first, "sp", [(i, i ^ 2) for i in range(4)])
        packed, levels, *whole_rows = pack_call(lengths, other, k_t, v_t, n_layers - 1)
        heavy_calls = [functools.partial(send_call, True, n, 1 + i) for i, n in enumerate(HEAVY_LEVELS)]
        light_calls = [functools.partial(send_call, False, n, 1 + len(HEAVY_LEVELS) + i) for i, n in enumerate(LIGHT_LEVELS)]
        got, partner = lax.switch(levels[0], heavy_calls, packed, k_t, v_t)
        got = lax.switch(levels[1], light_calls, packed, k_t, v_t, got)
        got, *whole_rows = lax.optimization_barrier((got, *whole_rows))
        whole_got = [lax.ppermute(rows, "sp", [(i, i ^ flip) for i in range(4)]) for flip, rows in zip((2, 3), whole_rows)]

        tables = rotary_tables(my_lengths, head_dim, w_query.shape[2] // head_dim)
        weights = (w_query, w_key.swapaxes(1, 2), w_value.swapaxes(1, 2), w_out, w_gate, w_up, w_down)
        part, residual, *windows = chain_call(last, n_tp, lengths, hidden, ln_gain, tables, *weights, k_t, v_t, partner, got)
        part, _, *kept = layer_call(last, False, lengths, residual, ln_gain, tables, *weights, k_t, v_t, partner, [early, *whole_got], part, n_tp)

        def back(rows_t):
            return rows_t.swapaxes(-1, -2)

        win_k, win_v, all_k, all_v = gather_call(windows, kept)
        return part, back(win_k)[:, :, None], back(win_v)[:, :, None], back(all_k)[:, None], back(all_v)[:, None]

    return jax.shard_map(inner_step, mesh=mesh, in_specs=in_specs, out_specs=out_specs, check_vma=False)
```
